256 devices in a mesh: gx: 4 (over x), gy: 8 (over z), gz: 8 (over y, core).
Axes of the slice: x: 4, y: 4, z: 8, core: 2. Of those that a mesh axis runs over, the one named last changes fastest.
Arguments:
- right_side: float32 [128, 256, 1024], P('gx', 'gy', 'gz'), may hold values from -1 to 1
- z_faces: float32 [1024], P('gz'), may hold values from 0.5 to 2, as said below
- xy_coupling: float32 [5], replicated, as said below
- block_inverse: float32 [5, 1024, 128], P(None, 'gz'), as said below
Outputs:
- solution: float32 [128, 256, 1024], P('gx', 'gy', 'gz')
- residual: float32 [128, 256, 1024], P('gx', 'gy', 'gz')
The draws below stay inside these ranges and needn't reach their ends.
Inputs may be any that keep to these rules, and one draw needn't show every extreme that they name: z_faces is positive. xy_coupling[l] lies between 2.9 * 4^-l / 128^2 and 5.5 * 4^-l / 128^2. block_inverse[l] holds, block by block, the inverses of the 128 x 128 diagonal blocks of M_l built from z_faces and xy_coupling[l].
All inputs are finite; a program needn't handle non-finite values.
Results may differ from the reference program's by a relative error of at most 0.028.
Values sent between devices are 32-bit elements; how exact they have to be, the bound alone decides.
No kernel may reach another device: no remote copies, remote signals or barrier semaphores. Data moves between devices by JAX's collectives and lax.ppermute only.
A program may use at most 128 MiB of HBM per device.

```python
import jax
import jax.numpy as jnp
from jax import lax

CZ = 128
LEVELS = 5
SWEEPS = 2
NX = 128
NY = 256
NZ = 1024


def coefficient_set(key):
    face_key = jax.random.fold_in(key, 101)
    level_key = jax.random.fold_in(key, 202)
    face_values = jnp.exp(jax.random.uniform(face_key, (NZ,), jnp.float32, jnp.log(0.5), jnp.log(2.0)))
    spread = jnp.exp(jax.random.uniform(level_key, (LEVELS,), jnp.float32, -0.3, 0.3))
    lateral = 4.0 / (CZ * CZ) * spread * 0.25 ** jnp.arange(LEVELS).astype(jnp.float32)
    return (face_values, lateral)


def draw_right_side(key, part):
    rough_key = jax.random.fold_in(key, 303)
    amplitude = 0.03 * (256.0 / NZ) ** 1.5
    rough = jnp.clip(jax.random.normal(rough_key, (NX, NY, NZ), jnp.float32), -4.0, 4.0)
    field = amplitude * rough
    return field.astype(jnp.float32)


def draw_z_faces(key, part):
    return coefficient_set(key)[0].astype(jnp.float32)


def draw_xy_coupling(key, part):
    return coefficient_set(key)[1].astype(jnp.float32)


def draw_block_inverse(key, part):
    face_values, lateral = coefficient_set(key)
    blocks_count = NZ // CZ
    up_values = jnp.concatenate([face_values[1:], jnp.ones((1,), jnp.float32)])
    down_rows = face_values.reshape(blocks_count, CZ)
    up_rows = up_values.reshape(blocks_count, CZ)
    identity = jnp.eye(CZ, dtype=jnp.float32)
    upper_shift = jnp.eye(CZ, k=1, dtype=jnp.float32)
    coupling = up_rows[:, :, None] * upper_shift
    base_matrix = (down_rows + up_rows)[:, :, None] * identity - coupling - jnp.swapaxes(coupling, 1, 2)
    matrices = base_matrix[None] + (4.0 * lateral)[:, None, None, None] * identity
    return jnp.linalg.inv(matrices).reshape(LEVELS, NZ, CZ).astype(jnp.float32)


def setup_inputs(seed: int = 0) -> dict:
    streams_of = jax.random.split(jax.random.key(seed), 5)
    right_side = draw_right_side(jax.random.fold_in(streams_of[4], 71), 0)
    z_faces = draw_z_faces(jax.random.fold_in(streams_of[4], 71), 0)
    xy_coupling = draw_xy_coupling(jax.random.fold_in(streams_of[4], 71), 0)
    block_inverse = draw_block_inverse(jax.random.fold_in(streams_of[4], 71), 0)
    return {"right_side": right_side, "z_faces": z_faces, "xy_coupling": xy_coupling, "block_inverse": block_inverse}


damping = 0.8
highest = lax.Precision.HIGHEST

def interface_setup(corner_aa, corner_ab, corner_ba, corner_bb, couplings):
    determinant = corner_aa * corner_bb - corner_ab * corner_ba
    corner_inverse = jnp.stack([jnp.stack([corner_bb, -corner_ab], -1), jnp.stack([-corner_ba, corner_aa], -1)], -2) / determinant[:, None, None]
    blocks_count = corner_aa.shape[0]
    identity = jnp.eye(blocks_count, dtype=corner_inverse.dtype)
    diagonal_part = jnp.einsum('kab,kl->kalb', corner_inverse, identity, precision=highest).reshape(2 * blocks_count, 2 * blocks_count)
    link_values = jnp.zeros((2 * blocks_count - 1,), corner_inverse.dtype).at[1::2].set(-couplings)
    schur_matrix = diagonal_part + jnp.diag(link_values, 1) + jnp.diag(link_values, -1)
    return (corner_inverse, diagonal_part, jnp.linalg.cholesky(schur_matrix))

def level_setup(block_inverse, z_faces, level):
    block_len = block_inverse.shape[2]
    blocks_count = z_faces.shape[0] // block_len
    inverse_blocks = block_inverse[level].reshape(blocks_count, block_len, block_len)
    last_cell = block_len - 1
    couplings = z_faces.reshape(blocks_count, block_len)[1:, 0]
    corner_inverse, diagonal_part, factor = interface_setup(inverse_blocks[:, 0, 0], inverse_blocks[:, 0, last_cell], inverse_blocks[:, last_cell, 0], inverse_blocks[:, last_cell, last_cell], couplings)
    return (inverse_blocks, corner_inverse, factor, couplings)

def line_solve(source, inverse_blocks, corner_inverse, factor, couplings):
    first_extent, second_extent, depth = source.shape
    blocks_count, block_len = (inverse_blocks.shape[0], inverse_blocks.shape[1])
    blocked = source.reshape(first_extent, second_extent, blocks_count, block_len)
    local_part = jnp.einsum('xykj,kij->xyki', blocked, inverse_blocks, precision=highest)
    end_values = jnp.stack([local_part[..., 0], local_part[..., block_len - 1]], -1)
    reduced_source = jnp.einsum('kab,xykb->kaxy', corner_inverse, end_values, precision=highest).reshape(2 * blocks_count, first_extent * second_extent)
    forward = lax.linalg.triangular_solve(factor, reduced_source, left_side=True, lower=True)
    interfaces = lax.linalg.triangular_solve(factor, forward, left_side=True, lower=True, transpose_a=True)
    interfaces = interfaces.reshape(blocks_count, 2, first_extent, second_extent).transpose(2, 3, 0, 1)
    zero_plane = jnp.zeros((first_extent, second_extent, 1), local_part.dtype)
    below_last = jnp.concatenate([zero_plane, interfaces[:, :, :-1, 1]], 2)
    above_first = jnp.concatenate([interfaces[:, :, 1:, 0], zero_plane], 2)
    zero_single = jnp.zeros((1,), couplings.dtype)
    down_coupling = jnp.concatenate([zero_single, couplings])
    up_coupling = jnp.concatenate([couplings, zero_single])
    result = local_part + (down_coupling * below_last)[..., None] * inverse_blocks[:, :, 0] + (up_coupling * above_first)[..., None] * inverse_blocks[:, :, block_len - 1]
    return result.reshape(first_extent, second_extent, depth)

def apply_operator(iterate, lateral_weight, down_faces, up_faces):
    padded = jnp.pad(iterate, 1)
    lateral = padded[:-2, 1:-1, 1:-1] + padded[2:, 1:-1, 1:-1] + padded[1:-1, :-2, 1:-1] + padded[1:-1, 2:, 1:-1]
    return lateral_weight * (4.0 * iterate - lateral) + down_faces * (iterate - padded[1:-1, 1:-1, :-2]) + up_faces * (iterate - padded[1:-1, 1:-1, 2:])

def restrict(field):
    first_extent, second_extent, depth = field.shape
    return field.reshape(first_extent // 2, 2, second_extent // 2, 2, depth).sum(axis=(1, 3)) * 0.25

def prolong(padded):
    first_extent = padded.shape[0] - 2
    second_extent = padded.shape[1] - 2
    depth = padded.shape[2]
    even_rows = 0.75 * padded[1:-1] + 0.25 * padded[:-2]
    odd_rows = 0.75 * padded[1:-1] + 0.25 * padded[2:]
    widened = jnp.stack([even_rows, odd_rows], 1).reshape(2 * first_extent, second_extent + 2, depth)
    even_rows = 0.75 * widened[:, 1:-1] + 0.25 * widened[:, :-2]
    odd_rows = 0.75 * widened[:, 1:-1] + 0.25 * widened[:, 2:]
    return jnp.stack([even_rows, odd_rows], 2).reshape(2 * first_extent, 2 * second_extent, depth)

def reference(right_side, z_faces, xy_coupling, block_inverse):
    up_faces = jnp.concatenate([z_faces[1:], jnp.ones((1,), z_faces.dtype)])
    setups = [level_setup(block_inverse, z_faces, level) for level in range(LEVELS)]

    def operator(iterate, level):
        return apply_operator(iterate, xy_coupling[level], z_faces, up_faces)

    def smooth(source, level):
        return line_solve(source, *setups[level])

    def multigrid_cycle(source, level):
        iterate = damping * smooth(source, level)
        for sweep in range(SWEEPS - 1):
            iterate = iterate + damping * smooth(source - operator(iterate, level), level)
        if level == LEVELS - 1:
            return iterate
        coarse = multigrid_cycle(restrict(source - operator(iterate, level)), level + 1)
        iterate = iterate + prolong(jnp.pad(coarse, ((1, 1), (1, 1), (0, 0))))
        for sweep in range(SWEEPS):
            iterate = iterate + damping * smooth(source - operator(iterate, level), level)
        return iterate
    solution = multigrid_cycle(right_side, 0)
    return (solution, right_side - operator(solution, 0))
```

```python
import functools

import jax
import jax.numpy as jnp
from jax import lax
from jax.experimental import pallas as pl
from jax.experimental.pallas import tpu as pltpu
from jax.sharding import PartitionSpec as P

LEVELS = 5
POWERS = 4
HIGHEST = lax.Precision.HIGHEST
F32 = jnp.float32
VMEM_LIMIT = 56 * 1024 * 1024


def contract(a, b, da, db):
    return lax.dot_general(
        a, b, (((da,), (db,)), ((), ())), precision=HIGHEST, preferred_element_type=F32
    )


def nn(a, b):
    return contract(a, b, 1, 0)


def nt(a, b):
    return contract(a, b, 1, 1)


def tn(a, b):
    return contract(a, b, 0, 0)


def rows(lo, hi, fn, step=4):
    full = (hi - lo) // step
    if full:
        def group(k, carry):
            for q in range(step):
                fn(lo + k * step + q)
            return carry

        lax.fori_loop(0, full, group, 0)
    for i in range(lo + full * step, hi):
        fn(i)


def sublane_index(length):
    return lax.broadcasted_iota(jnp.int32, (length, 128), 0)


def shifted(v, zero_ends):
    n = v.shape[0]
    low, high = pltpu.roll(v, 1, 0), pltpu.roll(v, n - 1, 0)
    if zero_ends:
        at = sublane_index(n)
        low = jnp.where(at > 0, low, 0.0)
        high = jnp.where(at < n - 1, high, 0.0)
    return low, high


class Window:
    def __init__(self, shape, origin=None, grid=None):
        self.x, self.y = shape
        self.whole = origin is None
        if not self.whole:
            self.x0, y0 = origin
            self.nx, ny = grid
            at = sublane_index(self.y) + y0
            self.in_y = jnp.where((at >= 0) & (at < ny), 1.0, 0.0).astype(F32)

    def mask(self, i, v):
        if self.whole:
            return v
        at = self.x0 + i
        inside = jnp.where((at >= 0) & (at < self.nx), 1.0, 0.0).astype(F32)
        return v * (self.in_y * inside)

    def around(self, ref, i):
        low, high = shifted(ref[i], self.whole)
        total = low + high
        if self.whole:
            below = ref[jnp.maximum(i - 1, 0)] * jnp.where(i > 0, 1.0, 0.0).astype(F32)
            above = ref[jnp.minimum(i + 1, self.x - 1)] * jnp.where(i < self.x - 1, 1.0, 0.0).astype(F32)
            return total + (below + above)
        return total + (ref[i - 1] + ref[i + 1])

    def span(self, trim):
        return (0, self.x) if self.whole else (trim, self.x - trim)


def line_powers(field, ends, power_ref, link_ref, count, out_refs):
    for j in range(count):
        value = nt(field, power_ref[j]) + tn(ends, link_ref[j])
        out_refs[j][...] = value.reshape(out_refs[j].shape)


def smoothed_residual(win, field_ref, x1, x2, t, out, trim):
    lo, hi = win.span(trim - 1)

    def inner(i):
        t[i] = 0.32 * x1[i] + win.mask(i, 0.64 * win.around(x2, i))

    rows(lo, hi, inner)
    lo, hi = win.span(trim)

    def outer(i):
        out[i] = 0.04 * field_ref[i] + win.around(t, i)

    rows(lo, hi, outer)


def horner(win, xs, weights, t0, t1, trim):
    src = xs[-1]
    scale = weights[-1]
    buffers = (t0, t1)
    for n, j in enumerate(range(len(xs) - 2, 0, -1)):
        dst = buffers[n % 2]
        lo, hi = win.span(trim - j)

        def one(i, src=src, dst=dst, j=j, scale=scale):
            dst[i] = weights[j] * xs[j][i] + win.mask(i, scale * win.around(src, i))

        rows(lo, hi, one)
        src, scale = dst, 1.0
    return src, scale


def restrict(src, scratch, out, x_at, y_at):
    count_x, count_y = out.shape[0], out.shape[1]
    for i in range(count_x):
        scratch[i] = src[x_at + 2 * i] + src[x_at + 2 * i + 1]
    for i in range(count_x):
        even = scratch[i, pl.ds(y_at, count_y, stride=2), :]
        odd = scratch[i, pl.ds(y_at + 1, count_y, stride=2), :]
        out[i] = (even + odd) * 0.25


def prolong(src, src_whole, out, win, x_from, y_from, count_x, count_y):
    last = src.shape[0] - 1
    for i in range(count_x):
        at = x_from + i
        centre = src[at]
        below = src[at - 1] if at > 0 else jnp.zeros_like(centre)
        above = src[at + 1] if at < last else jnp.zeros_like(centre)
        for odd, other in ((0, below), (1, above)):
            v = 0.75 * centre + 0.25 * other
            low, high = shifted(v, src_whole)
            for parity, side in ((0, low), (1, high)):
                w = 0.75 * v + 0.25 * side
                out[2 * i + odd, pl.ds(parity, count_y, stride=2), :] = w[y_from : y_from + count_y]
    if not win.whole:
        rows(0, 2 * count_x, lambda i: out.__setitem__(i, win.mask(i, out[i])))


def send(out_ref, value):
    for m in range(out_ref.shape[0]):
        out_ref[m] = value


def powers_kernel(g_ref, e_ref, zf_ref, power_ref, ends_ref, link_ref, up_ref, table_ref):
    levels, n = g_ref.shape[0], g_ref.shape[1]
    table_ref[...] = jnp.zeros_like(table_ref)
    link_ref[...] = jnp.zeros_like(link_ref)
    for level in range(levels):
        e = e_ref[level]
        inverse_e = 1.0 / jnp.full((1, n), e, F32)
        one = g_ref[level] * e
        two = nn(one, one)
        three = nn(two, one)
        four = nn(two, two)
        ends = []
        for j, value in enumerate((one, two, three, four)):
            power_ref[level, j] = value
            for s, row in enumerate((value[0:1], value[n - 1 : n])):
                ends_ref[level, 2 * j + s : 2 * j + s + 1] = row
                table_ref[0, 2 * j + s, level : level + 1] = row
                ends.append(row)
        for j in range(POWERS):
            for i in range(j + 1):
                for t in range(2):
                    link_ref[level, j, 2 * i + t : 2 * i + t + 1] = ends[2 * (j - i) + t] * inverse_e
        table_ref[0, 9, level : level + 1] = inverse_e
    table_ref[0, 8] = jnp.broadcast_to(zf_ref[...], (8, n))
    for m in range(1, table_ref.shape[0]):
        table_ref[m] = table_ref[0]
    at = lax.broadcasted_iota(jnp.int32, (1, n), 1)
    up_ref[...] = jnp.zeros_like(up_ref)
    up_ref[0:4] = ends_ref[0, 0:4]
    up_ref[4:5] = jnp.where(at == 0, 1.0, 0.0).astype(F32)
    up_ref[5:6] = jnp.where(at == n - 1, 1.0, 0.0).astype(F32)


def coupling_kernel(where_ref, table_ref, e_ref, zf_ref, om_ref, om_up_ref, m_ref, m_link_ref, held):
    blocks, n = table_ref.shape[0], table_ref.shape[3]
    k_own = where_ref[2]
    wide = (8, n)
    lane = lax.broadcasted_iota(jnp.int32, wide, 1)
    inverse_e = table_ref[0, 9]

    def entry(m, row, column):
        at = 0 if column == 0 else n - 1
        return jnp.broadcast_to(table_ref[m, row][:, at : at + 1], wide)

    corner = [
        [
            [[entry(m, 2 * i + s, t) * inverse_e for t in range(2)] for s in range(2)]
            for m in range(blocks)
        ]
        for i in range(POWERS)
    ]
    face = [entry(m, 8, 0) for m in range(blocks)]

    gain_v, gain_d, gain_p, gain_g = [corner[0][0][1][1]], [None], [None], [None]
    for k in range(1, blocks):
        (a, b), (c, d) = corner[0][k]
        g = face[k]
        gv = g * g * gain_v[k - 1]
        dk = 1.0 / (1.0 - a * gv)
        gain_d.append(dk)
        gain_p.append(dk * b)
        gain_g.append(gv)
        gain_v.append(d + c * gv * gain_p[k])

    def solve(low, high):
        u, pu = [high[0]], [None]
        for k in range(1, blocks):
            (a, b), (c, d) = corner[0][k]
            gu = face[k] * u[k - 1]
            pu.append(gain_d[k] * (low[k] + a * gu))
            u.append(high[k] + c * (gu + gain_g[k] * pu[k]))
        zero = jnp.zeros(wide, F32)
        alpha, beta = [zero] * blocks, [zero] * blocks
        for k in range(blocks - 1, 0, -1):
            p = pu[k] + gain_p[k] * beta[k]
            beta[k - 1] = face[k] * p
            alpha[k] = face[k] * (u[k - 1] + gain_v[k - 1] * beta[k - 1])
        return alpha, beta

    unit = [
        [jnp.where(lane == 8 * m + s, 1.0, 0.0).astype(F32) for m in range(blocks)] for s in range(2)
    ]
    response = [solve(unit[0], unit[1])]
    for i in range(1, POWERS):
        source = [[None] * blocks, [None] * blocks]
        for m in range(blocks):
            for s in range(2):
                total = None
                for q in range(i):
                    c = corner[i - q][m][s]
                    term = c[0] * response[q][0][m] + c[1] * response[q][1][m]
                    total = term if total is None else total + term
                source[s][m] = total
        response.append(solve(source[0], source[1]))
    for i in range(POWERS):
        for t in range(2):
            for m in range(blocks):
                held[m, 2 * i + t] = response[i][t][m]
    om_ref[...] = jnp.zeros_like(om_ref)
    for i in range(POWERS):
        for t in range(2):
            total = held[k_own, 2 * i + t]
            for j in range(1, i + 1):
                total = total + pltpu.roll(held[k_own, 2 * (i - j) + t], 2 * j, 1)
            for level in range(LEVELS):
                om_ref[level, 2 * i + t : 2 * i + t + 1] = total[level : level + 1]
    om_up_ref[...] = om_ref[0]
    lane = lane[0:1]
    om_up_ref[4:5] = jnp.where((lane == 8 * (k_own - 1) + 5) & (k_own > 0), 1.0, 0.0).astype(F32)
    om_up_ref[5:6] = jnp.where((lane == 8 * (k_own + 1) + 4) & (k_own < blocks - 1), 1.0, 0.0).astype(F32)
    om_up_ref[6:8] = jnp.zeros((2, n), F32)

    above = jnp.minimum(k_own + 1, blocks - 1)
    top = table_ref[above, 8][0:1, 0:1]
    top = jnp.where(jnp.full((1, 1), k_own, jnp.int32) < blocks - 1, top, 1.0)
    down = zf_ref[...]
    up = jnp.where(lane == n - 1, jnp.broadcast_to(top, (1, n)), pltpu.roll(down, n - 1, 1))
    row = lax.broadcasted_iota(jnp.int32, (n, n), 0)
    column = lax.broadcasted_iota(jnp.int32, (n, n), 1)
    down_all, up_all = jnp.broadcast_to(down, (n, n)), jnp.broadcast_to(up, (n, n))
    m_ref[...] = jnp.where(
        row == column,
        down_all + up_all + 4.0 * e_ref[0],
        jnp.where(row == column - 1, -down_all, jnp.where(row == column + 1, -up_all, 0.0)),
    )
    m_link_ref[...] = jnp.zeros_like(m_link_ref)
    m_link_ref[4:5] = jnp.where(lane == 0, -down, 0.0)
    m_link_ref[5:6] = jnp.where(lane == n - 1, -up, 0.0)


def flat(ref):
    return ref[...].reshape(ref.shape[0] * ref.shape[1], ref.shape[2])


def ends_kernel(f_ref, v_ref, out_ref):
    send(out_ref, nt(v_ref[...], flat(f_ref)))


def ends_from(om_ref, got_ref):
    return nn(om_ref[:, : got_ref.shape[0]], got_ref[...])


def down_kernel(halo, grid, where_ref, f_ref, got_ref, om_ref, power_ref, link_ref, out_ref, x1, x2, t, r, pair):
    hx, hy = halo
    sx, sy = f_ref.shape[0] - 2 * hx, f_ref.shape[1] - 2 * hy
    win = Window(f_ref.shape[:2], (where_ref[0] * sx - hx, where_ref[1] * sy - hy), grid)
    ends = ends_from(om_ref, got_ref)
    line_powers(flat(f_ref), ends, power_ref, link_ref, 2, (x1, x2))
    smoothed_residual(win, f_ref, x1, x2, t, r, hx)
    restrict(r, pair, out_ref, hx, hy)


KNOWN = (0.9984, 0.9728, 0.8192, 0.4096)
TWICE = (0.0016, 0.0256, 0.1536, 0.4096, 0.4096)


def known_kernel(
    halo, trim, grid, twice, where_ref, e_ref, f_ref, got_ref, om_ref, power_ref, link_ref, *rest
):
    hx, hy = halo
    level = 0 if twice else 1
    outs, (x1, x2, x3, x4, t0, t1) = rest[:-6], rest[-6:]
    sx, sy = f_ref.shape[0] - 2 * hx, f_ref.shape[1] - 2 * hy
    win = Window(f_ref.shape[:2], (where_ref[0] * sx - hx, where_ref[1] * sy - hy), grid)
    ends = ends_from(om_ref, got_ref)
    xs = (x1, x2, x3, x4)
    line_powers(flat(f_ref), ends, power_ref, link_ref, POWERS, xs)
    inverse_e = 1.0 / jnp.full((f_ref.shape[1], 128), e_ref[level], F32)
    src, scale = horner(win, xs, KNOWN, t0, t1, trim)
    lo, hi = win.span(trim)
    if twice:
        known_out, twice_out = outs

        def known(i):
            v = (KNOWN[0] * x1[i] + scale * win.around(src, i)) * inverse_e
            known_out[i - hx] = v[hy : hy + sy]

        rows(lo, hi, known)
        src2, scale2 = horner(win, (f_ref,) + xs, TWICE, t0, t1, trim)

        def again(i):
            v = TWICE[0] * f_ref[i] + scale2 * win.around(src2, i)
            twice_out[i - hx] = v[hy : hy + sy]

        rows(lo, hi, again)
    else:
        (known_out,) = outs
        known_out[...] = jnp.zeros_like(known_out)

        def known(i):
            v = (KNOWN[0] * x1[i] + scale * win.around(src, i)) * inverse_e
            known_out[i] = win.mask(i, v)

        rows(lo, hi, known)


def spread_kernel(parts_ref, v_ref, f_ref, out_ref):
    many, sx, sy = parts_ref.shape[:3]
    across = f_ref.shape[1] // sy
    for p in range(many):
        ix, iy = p // across, p % across
        f_ref[ix * sx : (ix + 1) * sx, iy * sy : (iy + 1) * sy] = parts_ref[p]
    send(out_ref, nt(v_ref[...], flat(f_ref)))


def whole_down_kernel(
    level, region, where_ref, e_ref, f_ref, got_ref, om_ref, power_ref, link_ref, v_ref,
    coarse_ref, out_ref, known_ref, x1, x2, x3, x4, t0, t1, pair, *padded
):
    win = Window(f_ref.shape[:2])
    ends = ends_from(om_ref, got_ref)
    xs = (x1, x2, x3, x4)
    line_powers(flat(f_ref), ends, power_ref, link_ref, POWERS, xs)
    smoothed_residual(win, f_ref, x1, x2, t0, t1, 2)
    restrict(t1, pair, coarse_ref, 0, 0)
    send(out_ref, nt(v_ref[...], flat(coarse_ref)))
    inverse_e = 1.0 / jnp.full((f_ref.shape[1], 128), e_ref[level], F32)
    src, scale = horner(win, xs, KNOWN, t0, t1, 4)
    if region is None:
        def known(i):
            known_ref[i] = (KNOWN[0] * x1[i] + scale * win.around(src, i)) * inverse_e

        rows(0, win.x, known)
    else:
        (pad,) = padded
        margin = region
        clear_edges(pad, margin)

        def known(i):
            v = (KNOWN[0] * x1[i] + scale * win.around(src, i)) * inverse_e
            pad[i + margin, margin : margin + win.y] = v

        rows(0, win.x, known)
        cut(where_ref, pad, known_ref, margin)


def clear_edges(pad, margin):
    x, y = pad.shape[:2]
    zero_rows = jnp.zeros((margin, y, 128), F32)
    zero_cols = jnp.zeros((x, margin, 128), F32)
    pad[0:margin] = zero_rows
    pad[x - margin : x] = zero_rows
    pad[:, 0:margin] = zero_cols
    pad[:, y - margin : y] = zero_cols


def cut(where_ref, pad, out_ref, margin):
    sx, sy = out_ref.shape[0] - 2 * margin, out_ref.shape[1] - 2 * margin
    x_at = where_ref[0] * sx
    y_at = pl.multiple_of(where_ref[1] * sy, 8)

    def one(i):
        out_ref[i] = pad[x_at + i, pl.ds(y_at, out_ref.shape[1]), :]

    rows(0, out_ref.shape[0], one)


def bottom_kernel(e_ref, f_ref, got_ref, om_ref, power_ref, link_ref, v_ref, w_ref, out_ref, x1, x2, c):
    win = Window(f_ref.shape[:2])
    ends = ends_from(om_ref, got_ref)
    line_powers(flat(f_ref), ends, power_ref, link_ref, 2, (x1, x2))
    inverse_e = 1.0 / jnp.full((f_ref.shape[1], 128), e_ref[LEVELS - 1], F32)

    def one(i):
        c[i] = (0.96 * x1[i] + 0.64 * win.around(x2, i)) * inverse_e

    rows(0, win.x, one)
    prolong(c, True, w_ref, Window(w_ref.shape[:2]), 0, 0, win.x, win.y)
    send(out_ref, nt(v_ref[...], flat(w_ref)))


def corrected(win, w_ref, known_ref, x1, x2, t, c, trim):
    smoothed_residual(win, w_ref, x1, x2, t, c, trim)
    lo, hi = win.span(trim)

    def add(i):
        c[i] = win.mask(i, c[i] + known_ref[i])

    rows(lo, hi, add)


def whole_up_kernel(
    margin, where_ref, w_ref, known_ref, got_ref, om_ref, power_ref, link_ref, v_ref,
    fine_ref, out_ref, x1, x2, t, c, fine, pad
):
    win = Window(w_ref.shape[:2])
    ends = ends_from(om_ref, got_ref)
    line_powers(flat(w_ref), ends, power_ref, link_ref, 2, (x1, x2))
    corrected(win, w_ref, known_ref, x1, x2, t, c, 2)
    prolong(c, True, fine, Window(fine.shape[:2]), 0, 0, win.x, win.y)
    clear_edges(pad, margin)

    def place(i):
        pad[i + margin, margin : margin + fine.shape[1]] = fine[i]

    rows(0, fine.shape[0], place)
    cut(where_ref, pad, fine_ref, margin)
    send(out_ref, nt(v_ref[...], flat(fine_ref)))


def up_kernel(
    halo, fine_halo, grid, where_ref, w_ref, known_ref, got_ref, om_ref, power_ref, link_ref, v_ref,
    fine_ref, out_ref, x1, x2, t, c
):
    hx, hy = halo
    fx, fy = fine_halo
    sx, sy = w_ref.shape[0] - 2 * hx, w_ref.shape[1] - 2 * hy
    ix, iy = where_ref[0], where_ref[1]
    win = Window(w_ref.shape[:2], (ix * sx - hx, iy * sy - hy), grid)
    fine_win = Window(
        fine_ref.shape[:2], (2 * ix * sx - fx, 2 * iy * sy - fy), (2 * grid[0], 2 * grid[1])
    )
    ends = ends_from(om_ref, got_ref)
    line_powers(flat(w_ref), ends, power_ref, link_ref, 2, (x1, x2))
    c[...] = jnp.zeros_like(c)
    corrected(win, w_ref, known_ref, x1, x2, t, c, 2)
    odd = fx % 2
    count_x = (fine_ref.shape[0] + 2 * odd) // 2
    if odd:
        x_from = hx - (fx + 1) // 2
        prolong_odd(c, fine_ref, fine_win, x_from, hy - fy // 2, count_x, fine_ref.shape[1] // 2)
    else:
        prolong(c, False, fine_ref, fine_win, hx - fx // 2, hy - fy // 2, count_x, fine_ref.shape[1] // 2)
    send(out_ref, nt(v_ref[...], flat(fine_ref)))


def prolong_odd(src, out, win, x_from, y_from, count_x, count_y):
    for i in range(count_x):
        at = x_from + i
        for odd, other in ((0, at - 1), (1, at + 1)):
            row = 2 * i + odd - 1
            if row < 0 or row >= out.shape[0]:
                continue
            v = 0.75 * src[at] + 0.25 * src[other]
            low, high = shifted(v, False)
            for parity, side in ((0, low), (1, high)):
                w = 0.75 * v + 0.25 * side
                out[row, pl.ds(parity, count_y, stride=2), :] = w[y_from : y_from + count_y]
    rows(0, out.shape[0], lambda i: out.__setitem__(i, win.mask(i, out[i])))


def final_kernel(
    halo, grid, where_ref, e_ref, w_ref, known_ref, twice_ref, got_ref, om_ref, power_ref, link_ref,
    m_ref, m_link_ref, u_ref, r_ref, x1, x2, xm, t0, t1
):
    hx, hy = halo
    sx, sy = w_ref.shape[0] - 2 * hx, w_ref.shape[1] - 2 * hy
    win = Window(w_ref.shape[:2], (where_ref[0] * sx - hx, where_ref[1] * sy - hy), grid)
    ends = ends_from(om_ref, got_ref)
    field = flat(w_ref)
    line_powers(field, ends, power_ref, link_ref, 2, (x1, x2))
    xm[...] = (nt(field, m_ref[...]) + tn(ends, m_link_ref[...])).reshape(xm.shape)
    e = e_ref[0]

    def first(i):
        t0[i] = win.mask(i, win.around(x2, i))

    lo, hi = win.span(hx - 2)
    rows(lo, hi, first)

    def second(i):
        t1[i] = (0.32 * e) * x1[i] - (0.64 * e) * t0[i]

    rows(lo, hi, second)
    lo, hi = win.span(hx - 1)

    def fourth(i):
        x2[i] = (0.28 * e) * w_ref[i] + win.mask(i, win.around(t1, i))

    rows(lo, hi, fourth)

    def fifth(i):
        t0[i] = 0.32 * x1[i] + 0.64 * t0[i]

    rows(lo, hi, fifth)
    lo, hi = win.span(hx)

    def last(i):
        at = i - hx
        u = 0.04 * w_ref[i] + win.around(t0, i)
        u_ref[at] = known_ref[at] + u[hy : hy + sy]
        r = 0.04 * xm[i] + win.around(x2, i)
        r_ref[at] = twice_ref[at] - r[hy : hy + sy]

    rows(lo, hi, last)


def call(kernel, outs, scratch, smem, *args, flops=0):
    specs = [
        pl.BlockSpec(memory_space=pltpu.SMEM if k in smem else pltpu.VMEM) for k in range(len(args))
    ]
    out_specs = [pl.BlockSpec(memory_space=pltpu.VMEM) for _ in outs]
    return pl.pallas_call(
        kernel,
        out_shape=[jax.ShapeDtypeStruct(s, F32) for s in outs],
        in_specs=specs,
        out_specs=out_specs,
        scratch_shapes=[pltpu.VMEM(s, F32) for s in scratch],
        compiler_params=pltpu.CompilerParams(vmem_limit_bytes=VMEM_LIMIT),
        cost_estimate=pl.CostEstimate(flops=int(flops) or 1000000, bytes_accessed=1000000, transcendentals=0),
    )(*args)


def exchange(copies, axes="gz"):
    got = lax.all_to_all(copies, axes, 0, 0, tiled=True)
    return got


def stacked(copies):
    got = exchange(copies)
    return got.reshape(got.shape[0] * got.shape[1], got.shape[2])


def with_halo(value, width_x, width_y):
    def both(v, axis, dim, width):
        size, length = lax.axis_size(axis), v.shape[dim]
        up = [(i, i + 1) for i in range(size - 1)]
        last = lax.slice_in_dim(v, length - width, length, axis=dim)
        first = lax.slice_in_dim(v, 0, width, axis=dim)
        low = lax.ppermute(last, axis, up)
        high = lax.ppermute(first, axis, [(b, a) for a, b in up])
        return jnp.concatenate([low, v, high], axis=dim)

    return both(both(value, "gy", 1, width_y), "gx", 0, width_x)


def body(right_side, z_faces, xy_coupling, block_inverse):
    part = functools.partial
    gx, gy, gz = (lax.axis_size(a) for a in ("gx", "gy", "gz"))
    n = z_faces.shape[0]
    where = jnp.stack([lax.axis_index(a) for a in ("gx", "gy", "gz")]).astype(jnp.int32)
    sx, sy = right_side.shape[0], right_side.shape[1]
    grids = [(gx * (sx >> l), gy * (sy >> l)) for l in range(LEVELS)]
    e = xy_coupling
    faces = z_faces.reshape(1, n)

    power, ends, link, ends_up, table = call(
        powers_kernel,
        [(LEVELS, POWERS, n, n), (LEVELS, 8, n), (LEVELS, POWERS, 8, n), (8, n), (gz, 10, 8, n)],
        [],
        (1,),
        block_inverse, e, faces,
    )
    table = exchange(table)
    om, om_up, m_matrix, m_link = call(
        coupling_kernel,
        [(LEVELS, 8, n), (8, n), (n, n), (8, n)],
        [(gz, 8, 8, n)],
        (0, 2),
        where, table, e, faces,
    )

    h0 = (4, 4)
    ext0 = (sx + 8, sy + 8)
    f0 = with_halo(right_side, 4, 4)
    lines0 = ext0[0] * ext0[1]
    (copies,) = call(ends_kernel, [(gz, 8, lines0)], [], (), f0, ends[0])
    got0 = stacked(copies)
    cube0 = ext0 + (n,)
    (f1,) = call(
        part(down_kernel, h0, grids[0]),
        [(sx // 2, sy // 2, n)],
        [cube0, cube0, cube0, cube0, (sx // 2, ext0[1], n)],
        (0,),
        where, f0, got0, om[0], power[0], link[0],
    )
    known0, twice0 = call(
        part(known_kernel, h0, 4, grids[0], True),
        [(sx, sy, n), (sx, sy, n)],
        [cube0] * 6,
        (0, 1),
        where, e, f0, got0, om[0], power[0], link[0],
        flops=20000000000,
    )

    s1x, s1y = sx // 2, sy // 2
    h1 = (5, 8)
    ext1 = (s1x + 10, s1y + 16)
    cube1 = ext1 + (n,)
    f1 = with_halo(f1, 5, 8)
    (copies,) = call(ends_kernel, [(gz, 8, ext1[0] * ext1[1])], [], (), f1, ends[1])
    got1 = stacked(copies)
    s2x, s2y = s1x // 2, s1y // 2
    (f2,) = call(
        part(down_kernel, h1, grids[1]),
        [(s2x, s2y, n)],
        [cube1, cube1, cube1, cube1, (s2x, ext1[1], n)],
        (0,),
        where, f1, got1, om[1], power[1], link[1],
    )
    (known1,) = call(
        part(known_kernel, h1, 3, grids[1], False),
        [cube1],
        [cube1] * 6,
        (0, 1),
        where, e, f1, got1, om[1], power[1], link[1],
        flops=10000000000,
    )

    many = gx * gy
    parts = lax.all_to_all(
        jnp.broadcast_to(f2[None], (many, s2x, s2y, n)), ("gx", "gy"), 0, 0, tiled=True
    )
    cubes = [g + (n,) for g in grids]
    lines = [g[0] * g[1] for g in grids]
    f2, copies = call(spread_kernel, [cubes[2], (gz, 8, lines[2])], [], (), parts, ends[2])
    margin = 8
    region = (s2x + 2 * margin, s2y + 2 * margin, n)
    padded = (grids[2][0] + 2 * margin, grids[2][1] + 2 * margin, n)
    f3, copies, known2 = call(
        part(whole_down_kernel, 2, margin),
        [cubes[3], (gz, 8, lines[3]), region],
        [cubes[2]] * 6 + [(grids[3][0], grids[2][1], n), padded],
        (0, 1),
        where, e, f2, stacked(copies), om[2], power[2], link[2], ends[3],
    )
    f4, copies, known3 = call(
        part(whole_down_kernel, 3, None),
        [cubes[4], (gz, 8, lines[4]), cubes[3]],
        [cubes[3]] * 6 + [(grids[4][0], grids[3][1], n)],
        (0, 1),
        where, e, f3, stacked(copies), om[3], power[3], link[3], ends[4],
    )
    w3, copies = call(
        bottom_kernel,
        [cubes[3], (gz, 8, lines[3])],
        [cubes[4]] * 3,
        (0,),
        e, f4, stacked(copies), om[4], power[4], link[4], ends[3],
    )
    w2, copies = call(
        part(whole_up_kernel, margin),
        [region, (gz, 8, region[0] * region[1])],
        [cubes[3]] * 4 + [cubes[2], padded],
        (0,),
        where, w3, known3, stacked(copies), om[3], power[3], link[3], ends[2],
    )

    w1, copies = call(
        part(up_kernel, (margin, margin), h1, grids[2]),
        [cube1, (gz, 8, ext1[0] * ext1[1])],
        [region] * 4,
        (0,),
        where, w2, known2, stacked(copies), om[2], power[2], link[2], ends[1],
    )
    w0, copies = call(
        part(up_kernel, h1, h0, grids[1]),
        [cube0, (gz, 8, lines0)],
        [cube1] * 4,
        (0,),
        where, w1, known1, stacked(copies), om[1], power[1], link[1], ends_up,
    )
    u, r = call(
        part(final_kernel, h0, grids[0]),
        [(sx, sy, n), (sx, sy, n)],
        [cube0] * 5,
        (0, 1),
        where, e, w0, known0, twice0, stacked(copies), om_up, power[0], link[0], m_matrix, m_link,
    )
    return u, r


def solution(mesh):
    return jax.shard_map(
        body,
        mesh=mesh,
        in_specs=(P("gx", "gy", "gz"), P("gz"), P(), P(None, "gz", None)),
        out_specs=(P("gx", "gy", "gz"), P("gx", "gy", "gz")),
        check_vma=False,
    )
```

```python
import functools

import jax
import jax.numpy as jnp
from jax import lax
from jax.experimental import pallas as pl
from jax.experimental.pallas import tpu as pltpu
from jax.sharding import PartitionSpec as P

LEVELS = 5
POWERS = 4
HIGHEST = lax.Precision.HIGHEST
F32 = jnp.float32
VMEM_LIMIT = 56 * 1024 * 1024


def contract(a, b, da, db):
    return lax.dot_general(
        a, b, (((da,), (db,)), ((), ())), precision=HIGHEST, preferred_element_type=F32
    )


def exact_nn(a, b):
    return contract(a, b, 1, 0)


def exact_nt(a, b):
    return contract(a, b, 1, 1)


def exact_tn(a, b):
    return contract(a, b, 0, 0)


def halves(a):
    if isinstance(a, tuple):
        return a
    high = a.astype(jnp.bfloat16)
    return high, (a - high.astype(F32)).astype(jnp.bfloat16)


def product(a, b, da, db):
    (ah, al), (bh, bl) = halves(a), halves(b)

    def dot(x, y):
        return lax.dot_general(x, y, (((da,), (db,)), ((), ())), preferred_element_type=F32)

    return dot(ah, bh) + (dot(ah, bl) + dot(al, bh))


def nn(a, b):
    return product(a, b, 1, 0)


def nt(a, b):
    return product(a, b, 1, 1)


def tn(a, b):
    return product(a, b, 0, 0)


def rows(lo, hi, fn, step=4):
    full = (hi - lo) // step
    if full:
        def group(k, carry):
            for q in range(step):
                fn(lo + k * step + q)
            return carry

        lax.fori_loop(0, full, group, 0)
    for i in range(lo + full * step, hi):
        fn(i)


def sublane_index(length):
    return lax.broadcasted_iota(jnp.int32, (length, 128), 0)


def shifted(v, zero_ends):
    n = v.shape[0]
    low, high = pltpu.roll(v, 1, 0), pltpu.roll(v, n - 1, 0)
    if zero_ends:
        at = sublane_index(n)
        low = jnp.where(at > 0, low, 0.0)
        high = jnp.where(at < n - 1, high, 0.0)
    return low, high


class Window:
    def __init__(self, shape, origin=None, grid=None):
        self.x, self.y = shape
        self.whole = origin is None
        self.lo, self.hi = (0, self.y) if self.whole else (1, self.y - 1)
        if not self.whole:
            self.x0, y0 = origin
            self.nx, ny = grid
            at = sublane_index(self.y - 2) + (y0 + 1)
            self.in_y = jnp.where((at >= 0) & (at < ny), 1.0, 0.0).astype(F32)

    def get(self, ref, i):
        return ref[i, self.lo : self.hi]

    def put(self, ref, i, v):
        ref[i, self.lo : self.hi] = v

    def mask(self, i, v):
        if self.whole:
            return v
        at = self.x0 + i
        inside = jnp.where((at >= 0) & (at < self.nx), 1.0, 0.0).astype(F32)
        return v * (self.in_y * inside)

    def around(self, ref, i):
        if self.whole:
            low, high = shifted(ref[i], True)
            below = ref[jnp.maximum(i - 1, 0)] * jnp.where(i > 0, 1.0, 0.0).astype(F32)
            above = ref[jnp.minimum(i + 1, self.x - 1)] * jnp.where(i < self.x - 1, 1.0, 0.0).astype(F32)
            return (low + high) + (below + above)
        y = self.y
        return (ref[i, 0 : y - 2] + ref[i, 2:y]) + (ref[i - 1, 1 : y - 1] + ref[i + 1, 1 : y - 1])

    def span(self, trim):
        return (0, self.x) if self.whole else (trim, self.x - trim)

    def each(self, trim, out, fn):
        lo, hi = self.span(trim)
        rows(lo, hi, lambda i: self.put(out, i, fn(i)))


def line_powers(field, ends, power_ref, link_ref, count, out_refs, exact=False):
    if not exact:
        field, ends = halves(field), halves(ends)
    for j in range(count):
        if exact:
            value = exact_nt(field, power_ref[j]) + exact_tn(ends, link_ref[j])
        else:
            value = nt(field, power_ref[j]) + tn(ends, link_ref[j])
        out_refs[j][...] = value.reshape(out_refs[j].shape)


def smoothed_residual(win, field_ref, x1, x2, t, out, trim, masked=False, add=None):
    win.each(trim - 1, t, lambda i: 0.32 * win.get(x1, i) + win.mask(i, 0.64 * win.around(x2, i)))

    def outer(i):
        v = 0.04 * win.get(field_ref, i) + win.around(t, i)
        if add is not None:
            v = v + win.get(add, i)
        return win.mask(i, v) if masked else v

    win.each(trim, out, outer)


def horner(win, xs, weights, t0, t1, trim):
    src = xs[-1]
    scale = weights[-1]
    buffers = (t0, t1)
    for n, j in enumerate(range(len(xs) - 2, 0, -1)):
        dst = buffers[n % 2]

        def one(i, src=src, j=j, scale=scale):
            return weights[j] * win.get(xs[j], i) + win.mask(i, scale * win.around(src, i))

        win.each(trim - j, dst, one)
        src, scale = dst, 1.0
    return src, scale


def restrict(src, scratch, out, x_at, y_at):
    count_x, count_y = out.shape[0], out.shape[1]
    for i in range(count_x):
        scratch[i] = src[x_at + 2 * i] + src[x_at + 2 * i + 1]
    for i in range(count_x):
        even = scratch[i, pl.ds(y_at, count_y, stride=2), :]
        odd = scratch[i, pl.ds(y_at + 1, count_y, stride=2), :]
        out[i] = (even + odd) * 0.25


def prolong(src, src_whole, out, win, x_from, y_from, count_x, count_y):
    last = src.shape[0] - 1
    for i in range(count_x):
        at = x_from + i
        centre = src[at]
        below = src[at - 1] if at > 0 else jnp.zeros_like(centre)
        above = src[at + 1] if at < last else jnp.zeros_like(centre)
        for odd, other in ((0, below), (1, above)):
            v = 0.75 * centre + 0.25 * other
            low, high = shifted(v, src_whole)
            for parity, side in ((0, low), (1, high)):
                w = 0.75 * v + 0.25 * side
                out[2 * i + odd, pl.ds(parity, count_y, stride=2), :] = w[y_from : y_from + count_y]
    if not win.whole:
        win.each(0, out, lambda i: win.mask(i, win.get(out, i)))


def send(out_ref, value):
    for m in range(out_ref.shape[0]):
        out_ref[m] = value


def powers_kernel(g_ref, e_ref, zf_ref, *outs):
    levels, n = g_ref.shape[0], g_ref.shape[1]
    power_refs, ends_refs, link_refs = outs[0:levels], outs[levels : 2 * levels], outs[2 * levels : 3 * levels]
    up_ref, basis_ref, table_ref = outs[3 * levels :]
    table_ref[...] = jnp.zeros_like(table_ref)
    for level in range(levels):
        power_ref, ends_ref, link_ref = power_refs[level], ends_refs[level], link_refs[level]
        link_ref[...] = jnp.zeros_like(link_ref)
        e = e_ref[level]
        inverse_e = 1.0 / jnp.full((1, n), e, F32)
        one = g_ref[level] * e
        two = exact_nn(one, one)
        three = exact_nn(two, one)
        four = exact_nn(two, two)
        ends = []
        for j, value in enumerate((one, two, three, four)):
            power_ref[j] = value
            for s, row in enumerate((value[0:1], value[n - 1 : n])):
                ends_ref[2 * j + s : 2 * j + s + 1] = row
                table_ref[0, 2 * j + s, level : level + 1] = row
                ends.append(row)
        for j in range(POWERS):
            for i in range(j + 1):
                for t in range(2):
                    link_ref[j, 2 * i + t : 2 * i + t + 1] = ends[2 * (j - i) + t] * inverse_e
        table_ref[0, 9, level : level + 1] = inverse_e
    table_ref[0, 8] = jnp.broadcast_to(zf_ref[...], (8, n))
    zero = ends_refs[0][0:4] * (1.0 / jnp.full((4, n), e_ref[0], F32))
    basis_ref[0:4] = zero
    basis_ref[4:8] = exact_nn(zero, power_refs[1][0])
    basis_ref[8:12] = exact_nn(zero, power_refs[1][1])
    basis_ref[12:16] = ends_refs[1][0:4] * (1.0 / jnp.full((4, n), e_ref[1], F32))
    basis = jnp.concatenate([basis_ref[...], jnp.zeros((n - 16, n), F32)], 0)
    at = lax.broadcasted_iota(jnp.int32, (8, n), 1)
    table_ref[0, 10] = jnp.where(at < 4, exact_nt(ends_refs[1][...], basis), 0.0)
    table_ref[0, 11] = exact_nt(ends_refs[2][...], basis)
    for m in range(1, table_ref.shape[0]):
        table_ref[m] = table_ref[0]
    at = lax.broadcasted_iota(jnp.int32, (1, n), 1)
    up_ref[...] = jnp.zeros_like(up_ref)
    up_ref[0:4] = ends_refs[0][0:4]
    up_ref[4:5] = jnp.where(at == 0, 1.0, 0.0).astype(F32)
    up_ref[5:6] = jnp.where(at == n - 1, 1.0, 0.0).astype(F32)


def coupling_kernel(
    where_ref, table_ref, e_ref, zf_ref, basis_ref, om0, om1, om2, om3, om4, om_up_ref, m_ref, m_link_ref, mix_ref, w2_ref, held, full
):
    blocks, n = table_ref.shape[0], table_ref.shape[3]
    k_own = where_ref[2]
    wide = (8, n)
    lane = lax.broadcasted_iota(jnp.int32, wide, 1)
    inverse_e = table_ref[0, 9]

    def entry(m, row, column):
        at = 0 if column == 0 else n - 1
        return jnp.broadcast_to(table_ref[m, row][:, at : at + 1], wide)

    corner = [
        [
            [[entry(m, 2 * i + s, t) * inverse_e for t in range(2)] for s in range(2)]
            for m in range(blocks)
        ]
        for i in range(POWERS)
    ]
    face = [entry(m, 8, 0) for m in range(blocks)]

    gain_v, gain_d, gain_p, gain_g = [corner[0][0][1][1]], [None], [None], [None]
    for k in range(1, blocks):
        (a, b), (c, d) = corner[0][k]
        g = face[k]
        gv = g * g * gain_v[k - 1]
        dk = 1.0 / (1.0 - a * gv)
        gain_d.append(dk)
        gain_p.append(dk * b)
        gain_g.append(gv)
        gain_v.append(d + c * gv * gain_p[k])

    def solve(low, high):
        u, pu = [high[0]], [None]
        for k in range(1, blocks):
            (a, b), (c, d) = corner[0][k]
            gu = face[k] * u[k - 1]
            pu.append(gain_d[k] * (low[k] + a * gu))
            u.append(high[k] + c * (gu + gain_g[k] * pu[k]))
        zero = jnp.zeros(wide, F32)
        alpha, beta = [zero] * blocks, [zero] * blocks
        for k in range(blocks - 1, 0, -1):
            p = pu[k] + gain_p[k] * beta[k]
            beta[k - 1] = face[k] * p
            alpha[k] = face[k] * (u[k - 1] + gain_v[k - 1] * beta[k - 1])
        return alpha, beta

    unit = [
        [jnp.where(lane == 8 * m + s, 1.0, 0.0).astype(F32) for m in range(blocks)] for s in range(2)
    ]
    response = [solve(unit[0], unit[1])]
    for i in range(1, POWERS):
        source = [[None] * blocks, [None] * blocks]
        for m in range(blocks):
            for s in range(2):
                total = None
                for q in range(i):
                    c = corner[i - q][m][s]
                    term = c[0] * response[q][0][m] + c[1] * response[q][1][m]
                    total = term if total is None else total + term
                source[s][m] = total
        response.append(solve(source[0], source[1]))
    for i in range(POWERS):
        for t in range(2):
            for m in range(blocks):
                held[m, 2 * i + t] = response[i][t][m]
    om_refs = (om0, om1, om2, om3, om4)
    for i in range(POWERS):
        for t in range(2):
            total = held[k_own, 2 * i + t]
            for j in range(1, i + 1):
                total = total + pltpu.roll(held[k_own, 2 * (i - j) + t], 2 * j, 1)
            for level in range(LEVELS):
                om_refs[level][2 * i + t : 2 * i + t + 1] = total[level : level + 1]
    om_up_ref[...] = om0[...]

    def every(i, t, m):
        total = held[m, 2 * i + t]
        if i == 1:
            total = total + pltpu.roll(held[m, t], 2, 1)
        return total

    def matrix(slot, level, groups, own):
        full[...] = jnp.zeros_like(full)
        for start, i, scale in groups:
            for m in range(blocks):
                for t in range(2):
                    row = start + 2 * m + t
                    full[row : row + 1] = scale * every(i, t, m)[level : level + 1]
        if own is not None:
            full[own : own + 8] = om_refs[level][...]
        mix_ref[slot] = full[...].T

    matrix(0, 0, [(0, 0, 0.32)], 64)
    matrix(1, 0, [(0, 1, 0.64), (16, 0, 0.64)], None)
    matrix(2, 1, [(96, 0, 0.32)], None)
    matrix(3, 1, [(96, 1, 0.64), (112, 0, 0.64)], None)
    matrix(4, 1, [], 0)
    row = lax.broadcasted_iota(jnp.int32, (n, n), 0)
    column = lax.broadcasted_iota(jnp.int32, (n, n), 1)

    def spread(m):
        return jnp.where(
            (row < 16) & (column == (row >> 1) * 16 + 2 * m + (row & 1)), 1.0, 0.0
        ).astype(F32)

    def gathered(slot):
        full[...] = jnp.zeros_like(full)
        for m in range(blocks):
            full[8 * m : 8 * m + 8] = exact_nn(table_ref[m, slot], spread(m))
        return full[...]

    one = gathered(10).T

    def diagonal(shift, scale):
        return jnp.where((row < 32) & (column == row + shift), scale, 0.0).astype(F32)

    mix_ref[5] = diagonal(0, 0.04)
    mix_ref[6] = exact_nn(one, mix_ref[2]) + diagonal(32, 0.32)
    mix_ref[7] = exact_nn(one, mix_ref[3]) + diagonal(64, 0.64)
    mix_ref[8] = exact_nn(one, mix_ref[4])
    w2_ref[...] = exact_nn(om2[...], gathered(11))
    basis = jnp.concatenate([basis_ref[...], jnp.zeros((n - 16, n), F32)], 0)
    chosen = exact_tn(spread(k_own), basis)
    mix_ref[9] = jnp.where(row < 32, chosen, 0.0)
    mix_ref[10] = chosen
    lane = lane[0:1]
    om_up_ref[4:5] = jnp.where((lane == 8 * (k_own - 1) + 5) & (k_own > 0), 1.0, 0.0).astype(F32)
    om_up_ref[5:6] = jnp.where((lane == 8 * (k_own + 1) + 4) & (k_own < blocks - 1), 1.0, 0.0).astype(F32)
    om_up_ref[6:8] = jnp.zeros((2, n), F32)

    above = jnp.minimum(k_own + 1, blocks - 1)
    top = table_ref[above, 8][0:1, 0:1]
    top = jnp.where(jnp.full((1, 1), k_own, jnp.int32) < blocks - 1, top, 1.0)
    down = zf_ref[...]
    up = jnp.where(lane == n - 1, jnp.broadcast_to(top, (1, n)), pltpu.roll(down, n - 1, 1))
    down_all, up_all = jnp.broadcast_to(down, (n, n)), jnp.broadcast_to(up, (n, n))
    m_ref[...] = jnp.where(
        row == column,
        down_all + up_all + 4.0 * e_ref[0],
        jnp.where(row == column - 1, -down_all, jnp.where(row == column + 1, -up_all, 0.0)),
    )
    m_link_ref[...] = jnp.zeros_like(m_link_ref)
    m_link_ref[4:5] = jnp.where(lane == 0, -down, 0.0)
    m_link_ref[5:6] = jnp.where(lane == n - 1, -up, 0.0)


def flat(ref):
    return ref[...].reshape(ref.shape[0] * ref.shape[1], ref.shape[2])


def ends_from(om_ref, got_ref):
    return exact_nn(om_ref[:, : got_ref.shape[0]], got_ref[...])


def restrict_into(src, scratch, out, x_at, y_at, count_y, y_to):
    for i in range(out.shape[0]):
        scratch[i] = src[x_at + 2 * i] + src[x_at + 2 * i + 1]
    for i in range(out.shape[0]):
        even = scratch[i, pl.ds(y_at, count_y, stride=2), :]
        odd = scratch[i, pl.ds(y_at + 1, count_y, stride=2), :]
        out[i, y_to : y_to + count_y] = (even + odd) * 0.25


def padded_lanes(count):
    return (count + 127) // 128 * 128


def windows(where_ref, s0, s1, ext0, ext1, grids):
    h0 = tuple((a - b) // 2 for a, b in zip(ext0, s0))
    h1 = tuple((a - b) // 2 for a, b in zip(ext1, s1))
    ix, iy = where_ref[0], where_ref[1]
    win0 = Window(ext0, (ix * s0[0] - h0[0], iy * s0[1] - h0[1]), grids[0])
    win1 = Window(ext1, (ix * s1[0] - h1[0], iy * s1[1] - h1[1]), grids[1])
    return win0, win1, h0, h1


def local_down_kernel(
    s0, s1, grids, where_ref, f_ref, power0, power1, v0, v1, v2, out_ref, f1_ref, f2_ref,
    x1, x2, t, r, pair, y1, y2, t1, r1, pair1
):
    ext0, ext1 = f_ref.shape[:2], f1_ref.shape[:2]
    win0, win1, h0, h1 = windows(where_ref, s0, s1, ext0, ext1, grids)
    field = halves(flat(f_ref))
    lanes0 = ext0[0] * ext0[1]
    lanes1 = ext1[0] * ext1[1]
    at1 = padded_lanes(lanes0)
    at2 = at1 + padded_lanes(lanes1)
    many = out_ref.shape[0]
    out_ref[0, :, at1 - 128 : at1] = jnp.zeros((8, 128), F32)
    out_ref[0, :, at2 - 128 : at2] = jnp.zeros((8, 128), F32)
    out_ref[0, :, at2 : at2 + 128] = jnp.zeros((8, 128), F32)
    out_ref[0, :, 0:lanes0] = nt(v0[...], field)
    x1[...] = nt(field, power0[0]).reshape(x1.shape)
    x2[...] = nt(field, power0[1]).reshape(x2.shape)
    smoothed_residual(win0, f_ref, x1, x2, t, r, 2, masked=True)
    f1_ref[...] = jnp.zeros_like(f1_ref)
    count = (ext0[1] - 4) // 2
    restrict_into(r, pair, f1_ref, 2, 2, count, (ext1[1] - count) // 2)
    field = halves(flat(f1_ref))
    out_ref[0, :, at1 : at1 + lanes1] = nt(v1[...], field)
    y1[...] = nt(field, power1[0]).reshape(y1.shape)
    y2[...] = nt(field, power1[1]).reshape(y2.shape)
    smoothed_residual(win1, f1_ref, y1, y2, t1, r1, h1[0])
    restrict(r1, pair1, f2_ref, h1[0], h1[1])
    lines2 = f2_ref.shape[0] * f2_ref.shape[1]
    out_ref[0, :, at2 : at2 + lines2] = nt(v2[...], flat(f2_ref))
    for m in range(1, many):
        out_ref[m] = out_ref[0]


def joined_down_kernel(
    s0, s1, ext0, grids, where_ref, got_ref, f1_local, f2_local, mix_ref, om2_ref, w2_ref,
    f1_ref, own1_ref, parts_ref, d1, d2, f, pair, y, h1s, h2s, f2s, pair1, z
):
    ext1 = f1_local.shape[:2]
    win0, win1, h0, h1 = windows(where_ref, s0, s1, ext0, ext1, grids)
    lanes0 = ext0[0] * ext0[1]
    lanes1 = ext1[0] * ext1[1]
    at1 = padded_lanes(lanes0)
    at2 = at1 + padded_lanes(lanes1)
    got0 = halves(got_ref[:, 0:lanes0])
    rows_in = got_ref.shape[0]
    d1[...] = tn(got0, mix_ref[0, 0:rows_in]).reshape(d1.shape)
    d2[...] = tn(got0, mix_ref[1, 0:rows_in]).reshape(d2.shape)

    win0.each(1, d1, lambda i: win0.get(d1, i) + win0.mask(i, win0.around(d2, i)))
    win0.each(2, f, lambda i: win0.mask(i, win0.around(d1, i)))
    y[...] = jnp.zeros_like(y)
    count = (ext0[1] - 4) // 2
    restrict_into(f, pair, y, 2, 2, count, (ext1[1] - count) // 2)
    yf = halves(flat(y))
    f1_ref[...] = f1_local[...] + nn(yf, mix_ref[9]).reshape(f1_ref.shape)
    got1 = halves(got_ref[:, at1 : at1 + lanes1])
    own1_ref[...] = (tn(got1, mix_ref[4, 0:rows_in]) + nn(yf, mix_ref[8])).reshape(own1_ref.shape)
    h1s[...] = (tn(got1, mix_ref[2, 0:rows_in]) + nn(yf, mix_ref[6])).reshape(h1s.shape)
    h2s[...] = (tn(got1, mix_ref[3, 0:rows_in]) + nn(yf, mix_ref[7])).reshape(h2s.shape)
    f2s[...] = nn(yf, mix_ref[5]).reshape(f2s.shape)
    trim = h1[0]
    win1.each(trim - 1, h1s, lambda i: win1.get(h1s, i) + win1.mask(i, win1.around(h2s, i)))
    win1.each(trim, f2s, lambda i: win1.get(f2s, i) + win1.around(h1s, i))
    restrict(f2s, pair1, z, h1[0], h1[1])
    zf = flat(z)
    lines2 = zf.shape[0]
    side = z.shape[0]
    parts_ref[0, 0:side] = f2_local[...] + nn(zf, mix_ref[10]).reshape(z.shape)
    own2 = nn(om2_ref[:, 0:rows_in], got_ref[:, at2 : at2 + lines2]) + nt(w2_ref[...], zf)
    parts_ref[0, side] = jnp.zeros((8, 128), F32)
    parts_ref[0, side, :, 0:lines2] = own2
    for m in range(1, parts_ref.shape[0]):
        parts_ref[m] = parts_ref[0]


KNOWN = (0.9984, 0.9728, 0.8192, 0.4096)
TWICE = (0.0016, 0.0256, 0.1536, 0.4096, 0.4096)


def lane_powers(field, coefficients, lane0, power_ref, link_ref, count, out_refs, exact=False):
    n = field.shape[1]
    if not exact:
        field, coefficients = halves(field), halves(coefficients)
    one, two = (exact_nt, exact_nn) if exact else (nt, nn)
    for j in range(count):
        pieces = [link_ref[j], jnp.zeros((n - 8 - lane0, n), F32)]
        if lane0:
            pieces = [jnp.zeros((lane0, n), F32)] + pieces
        value = one(field, power_ref[j]) + two(coefficients, jnp.concatenate(pieces, 0))
        out_refs[j][...] = value.reshape(out_refs[j].shape)


def known_zero_kernel(
    s0, ext0, grid, where_ref, e_ref, f_ref, got_ref, mix_ref, power_ref, link_ref,
    known_out, twice_out, own, f, x1, x2, x3, x4, t0, t1
):
    hx, hy = (f.shape[0] - s0[0]) // 2, (f.shape[1] - s0[1]) // 2
    cx, cy = (ext0[0] - f.shape[0]) // 2, (ext0[1] - f.shape[1]) // 2
    win = Window(f.shape[:2], (where_ref[0] * s0[0] - hx, where_ref[1] * s0[1] - hy), grid)
    coefficients = tn(got_ref[:, 0 : ext0[0] * ext0[1]], mix_ref[0, 0 : got_ref.shape[0]])
    own[...] = coefficients.reshape(ext0 + (128,))[cx : cx + f.shape[0], cy : cy + f.shape[1]]
    f[...] = f_ref[cx : cx + f.shape[0], cy : cy + f.shape[1]]
    xs = (x1, x2, x3, x4)
    lane_powers(flat(f), flat(own), 64, power_ref, link_ref, POWERS, xs)
    inverse_e = 1.0 / jnp.full((win.hi - win.lo, 128), e_ref[0], F32)
    at = hy - win.lo
    src, scale = horner(win, xs, KNOWN, t0, t1, hx)
    lo, hi = win.span(hx)

    def known(i):
        v = (KNOWN[0] * win.get(x1, i) + scale * win.around(src, i)) * inverse_e
        known_out[i - hx] = v[at : at + s0[1]]

    rows(lo, hi, known)
    src2, scale2 = horner(win, (f,) + xs, TWICE, t0, t1, hx)

    def again(i):
        v = TWICE[0] * win.get(f, i) + scale2 * win.around(src2, i)
        twice_out[i - hx] = v[at : at + s0[1]]

    rows(lo, hi, again)


def known_one_kernel(
    s1, grid, where_ref, e_ref, f_ref, own_ref, power_ref, link_ref, known_out, x1, x2, x3, x4, t0, t1
):
    hx, hy = (f_ref.shape[0] - s1[0]) // 2, (f_ref.shape[1] - s1[1]) // 2
    win = Window(f_ref.shape[:2], (where_ref[0] * s1[0] - hx, where_ref[1] * s1[1] - hy), grid)
    xs = (x1, x2, x3, x4)
    lane_powers(flat(f_ref), flat(own_ref), 0, power_ref, link_ref, POWERS, xs, exact=True)
    inverse_e = 1.0 / jnp.full((win.hi - win.lo, 128), e_ref[1], F32)
    src, scale = horner(win, xs, KNOWN, t0, t1, 3)
    known_out[...] = jnp.zeros_like(known_out)

    def known(i):
        return win.mask(i, (KNOWN[0] * win.get(x1, i) + scale * win.around(src, i)) * inverse_e)

    win.each(3, known_out, known)


def known_two_kernel(
    across, down, grid, where_ref, e_ref, parts_ref, power_ref, link_ref, known_out,
    fp, ap, x1, x2, x3, x4, t0, t1
):
    side = parts_ref.shape[2]
    lines = side * side
    ix, iy = where_ref[0], where_ref[1]
    for p in range(9):
        jx, jy = ix + p // 3 - 1, iy + p % 3 - 1
        inside = (jx >= 0) & (jx < across) & (jy >= 0) & (jy < down)
        at = jnp.clip(jx, 0, across - 1) * down + jnp.clip(jy, 0, down - 1)
        scale = jnp.where(inside, 1.0, 0.0).astype(F32)
        fp[p * lines : (p + 1) * lines] = (parts_ref[at, 0:side] * scale).reshape(lines, 128)
        ap[:, p * lines : (p + 1) * lines] = (parts_ref[at, side] * scale)[:, 0:lines]
    xs = (x1, x2, x3, x4)
    for j in range(POWERS):
        value = exact_nt(fp[...], power_ref[j]) + exact_tn(ap[...], link_ref[j])
        for p in range(9):
            px, py = p // 3 * side, p % 3 * side
            piece = value[p * lines : (p + 1) * lines].reshape(side, side, 128)
            xs[j][px : px + side, py : py + side] = piece
    win = Window(x1.shape[:2], ((ix - 1) * side, (iy - 1) * side), grid)
    inverse_e = 1.0 / jnp.full((win.hi - win.lo, 128), e_ref[2], F32)
    src, scale = horner(win, xs, KNOWN, t0, t1, 3)
    known_out[...] = jnp.zeros_like(known_out)

    def known(i):
        return win.mask(i, (KNOWN[0] * win.get(x1, i) + scale * win.around(src, i)) * inverse_e)

    win.each(3, known_out, known)


def gathered_down_kernel(
    across, down, parts_ref, power_ref, link_ref, v_ref, coarse_ref, out_ref, f, fp, ap, x1, x2, t, r, pair
):
    many, side = parts_ref.shape[0], parts_ref.shape[2]
    lines = side * side
    for p in range(many):
        px, py = p // down * side, p % down * side
        part = parts_ref[p, 0:side]
        f[px : px + side, py : py + side] = part
        fp[p * lines : (p + 1) * lines] = part.reshape(lines, 128)
        ap[:, p * lines : (p + 1) * lines] = parts_ref[p, side][:, 0:lines]
    fields, coefficients = halves(fp[...]), halves(ap[...])
    for j, x in enumerate((x1, x2)):
        value = nt(fields, power_ref[j]) + tn(coefficients, link_ref[j])
        for p in range(many):
            px, py = p // down * side, p % down * side
            x[px : px + side, py : py + side] = value[p * lines : (p + 1) * lines].reshape(side, side, 128)
    win = Window(f.shape[:2])
    smoothed_residual(win, f, x1, x2, t, r, 2)
    restrict(r, pair, coarse_ref, 0, 0)
    send(out_ref, nt(v_ref[...], flat(coarse_ref)))


def whole_down_kernel(
    f_ref, got_ref, om_ref, power_ref, link_ref, v_ref, coarse_ref, out_ref, x1, x2, t, r, pair
):
    win = Window(f_ref.shape[:2])
    ends = ends_from(om_ref, got_ref)
    line_powers(flat(f_ref), ends, power_ref, link_ref, 2, (x1, x2))
    smoothed_residual(win, f_ref, x1, x2, t, r, 2)
    restrict(r, pair, coarse_ref, 0, 0)
    send(out_ref, nt(v_ref[...], flat(coarse_ref)))


def whole_known_kernel(
    level, e_ref, f_ref, got_ref, om_ref, power_ref, link_ref, known_ref, x1, x2, x3, x4, t0, t1
):
    win = Window(f_ref.shape[:2])
    ends = ends_from(om_ref, got_ref)
    xs = (x1, x2, x3, x4)
    line_powers(flat(f_ref), ends, power_ref, link_ref, POWERS, xs, exact=True)
    inverse_e = 1.0 / jnp.full((f_ref.shape[1], 128), e_ref[level], F32)
    src, scale = horner(win, xs, KNOWN, t0, t1, 4)

    def known(i):
        known_ref[i] = (KNOWN[0] * x1[i] + scale * win.around(src, i)) * inverse_e

    rows(0, win.x, known)


def clear_edges(pad, margin):
    x, y = pad.shape[:2]
    zero_rows = jnp.zeros((margin, y, 128), F32)
    zero_cols = jnp.zeros((x, margin, 128), F32)
    pad[0:margin] = zero_rows
    pad[x - margin : x] = zero_rows
    pad[:, 0:margin] = zero_cols
    pad[:, y - margin : y] = zero_cols


def cut(where_ref, pad, out_ref, margin):
    sx, sy = out_ref.shape[0] - 2 * margin, out_ref.shape[1] - 2 * margin
    x_at = where_ref[0] * sx
    y_at = pl.multiple_of(where_ref[1] * sy, 8)

    def one(i):
        out_ref[i] = pad[x_at + i, pl.ds(y_at, out_ref.shape[1]), :]

    rows(0, out_ref.shape[0], one)


def bottom_kernel(e_ref, f_ref, got_ref, om_ref, power_ref, link_ref, v_ref, w_ref, out_ref, x1, x2, c):
    win = Window(f_ref.shape[:2])
    ends = ends_from(om_ref, got_ref)
    line_powers(flat(f_ref), ends, power_ref, link_ref, 2, (x1, x2), exact=True)
    inverse_e = 1.0 / jnp.full((f_ref.shape[1], 128), e_ref[LEVELS - 1], F32)

    def one(i):
        c[i] = (0.96 * x1[i] + 0.64 * win.around(x2, i)) * inverse_e

    rows(0, win.x, one)
    prolong(c, True, w_ref, Window(w_ref.shape[:2]), 0, 0, win.x, win.y)
    send(out_ref, exact_nt(v_ref[...], flat(w_ref)))


def whole_up_kernel(
    margin, where_ref, w_ref, known_ref, got_ref, om_ref, power_ref, link_ref, v_ref,
    fine_ref, out_ref, x1, x2, t, c, fine, pad
):
    win = Window(w_ref.shape[:2])
    ends = ends_from(om_ref, got_ref)
    line_powers(flat(w_ref), ends, power_ref, link_ref, 2, (x1, x2), exact=True)
    smoothed_residual(win, w_ref, x1, x2, t, c, 2, masked=True, add=known_ref)
    prolong(c, True, fine, Window(fine.shape[:2]), 0, 0, win.x, win.y)
    clear_edges(pad, margin)

    def place(i):
        pad[i + margin, margin : margin + fine.shape[1]] = fine[i]

    rows(0, fine.shape[0], place)
    cut(where_ref, pad, fine_ref, margin)
    send(out_ref, exact_nt(v_ref[...], flat(fine_ref)))


def up_kernel(
    halo, fine_halo, grid, where_ref, w_ref, known_ref, got_ref, om_ref, power_ref, link_ref, v_ref,
    fine_ref, out_ref, x1, x2, t, c
):
    hx, hy = halo
    fx, fy = fine_halo
    sx, sy = w_ref.shape[0] - 2 * hx, w_ref.shape[1] - 2 * hy
    ix, iy = where_ref[0], where_ref[1]
    win = Window(w_ref.shape[:2], (ix * sx - hx, iy * sy - hy), grid)
    fine_win = Window(
        fine_ref.shape[:2], (2 * ix * sx - fx, 2 * iy * sy - fy), (2 * grid[0], 2 * grid[1])
    )
    ends = ends_from(om_ref, got_ref)
    line_powers(flat(w_ref), ends, power_ref, link_ref, 2, (x1, x2), exact=True)
    c[...] = jnp.zeros_like(c)
    smoothed_residual(win, w_ref, x1, x2, t, c, 2, masked=True, add=known_ref)
    odd = fx % 2
    count_x = (fine_ref.shape[0] + 2 * odd) // 2
    if odd:
        x_from = hx - (fx + 1) // 2
        prolong_odd(c, fine_ref, fine_win, x_from, hy - fy // 2, count_x, fine_ref.shape[1] // 2)
    else:
        prolong(c, False, fine_ref, fine_win, hx - fx // 2, hy - fy // 2, count_x, fine_ref.shape[1] // 2)
    send(out_ref, exact_nt(v_ref[...], flat(fine_ref)))


def prolong_odd(src, out, win, x_from, y_from, count_x, count_y):
    for i in range(count_x):
        at = x_from + i
        for odd, other in ((0, at - 1), (1, at + 1)):
            row = 2 * i + odd - 1
            if row < 0 or row >= out.shape[0]:
                continue
            v = 0.75 * src[at] + 0.25 * src[other]
            low, high = shifted(v, False)
            for parity, side in ((0, low), (1, high)):
                w = 0.75 * v + 0.25 * side
                out[row, pl.ds(parity, count_y, stride=2), :] = w[y_from : y_from + count_y]
    win.each(0, out, lambda i: win.mask(i, win.get(out, i)))


def final_kernel(
    halo, grid, where_ref, e_ref, w_ref, known_ref, twice_ref, got_ref, om_ref, power_ref, link_ref,
    m_ref, m_link_ref, u_ref, r_ref, x1, x2, xm, t0, t1
):
    hx, hy = halo
    sx, sy = w_ref.shape[0] - 2 * hx, w_ref.shape[1] - 2 * hy
    win = Window(w_ref.shape[:2], (where_ref[0] * sx - hx, where_ref[1] * sy - hy), grid)
    ends = ends_from(om_ref, got_ref)
    field = flat(w_ref)
    line_powers(field, ends, power_ref, link_ref, 2, (x1, x2), exact=True)
    xm[...] = (exact_nt(field, m_ref[...]) + exact_tn(ends, m_link_ref[...])).reshape(xm.shape)
    e = e_ref[0]

    lo, hi = win.span(hx - 2)

    def inner(i):
        one = 0.32 * win.get(x1, i)
        two = win.mask(i, 0.64 * win.around(x2, i))
        win.put(t0, i, one + two)
        win.put(t1, i, e * (one - two))

    rows(lo, hi, inner)
    win.each(hx - 1, x2, lambda i: (0.28 * e) * win.get(w_ref, i) + win.mask(i, win.around(t1, i)))
    lo, hi = win.span(hx)
    cut_y = hy - win.lo

    def last(i):
        u = 0.04 * win.get(w_ref, i) + win.around(t0, i)
        u_ref[i - hx] = known_ref[i - hx] + u[cut_y : cut_y + sy]
        r = 0.04 * win.get(xm, i) + win.around(x2, i)
        r_ref[i - hx] = twice_ref[i - hx] - r[cut_y : cut_y + sy]

    rows(lo, hi, last)


def call(kernel, outs, scratch, smem, *args, flops=0):
    specs = [
        pl.BlockSpec(memory_space=pltpu.SMEM if k in smem else pltpu.VMEM) for k in range(len(args))
    ]
    out_specs = [pl.BlockSpec(memory_space=pltpu.VMEM) for _ in outs]
    return pl.pallas_call(
        kernel,
        out_shape=[jax.ShapeDtypeStruct(s, F32) for s in outs],
        in_specs=specs,
        out_specs=out_specs,
        scratch_shapes=[pltpu.VMEM(s, F32) for s in scratch],
        compiler_params=pltpu.CompilerParams(vmem_limit_bytes=VMEM_LIMIT),
        cost_estimate=pl.CostEstimate(flops=int(flops) or 1000000, bytes_accessed=1000000, transcendentals=0),
    )(*args)


def exchange(copies, axes="gz"):
    got = lax.all_to_all(copies, axes, 0, 0, tiled=True)
    return got


def stacked(copies):
    got = exchange(copies)
    return got.reshape(got.shape[0] * got.shape[1], got.shape[2])


def edges(v, axis, dim, width):
    size, length = lax.axis_size(axis), v.shape[dim]
    up = [(i, i + 1) for i in range(size - 1)]
    last = lax.slice_in_dim(v, length - width, length, axis=dim)
    first = lax.slice_in_dim(v, 0, width, axis=dim)
    return lax.ppermute(last, axis, up), lax.ppermute(first, axis, [(b, a) for a, b in up])


def halo_y(v, width):
    return edges(v, "gy", 1, width)


def halo_x(v, width):
    low, high = edges(v, "gx", 0, width)
    return jnp.concatenate([low, v, high], axis=0)


def body(right_side, z_faces, xy_coupling, block_inverse):
    part = functools.partial
    gx, gy, gz = (lax.axis_size(a) for a in ("gx", "gy", "gz"))
    n = z_faces.shape[0]
    where = jnp.stack([lax.axis_index(a) for a in ("gx", "gy", "gz")]).astype(jnp.int32)
    sx, sy = right_side.shape[0], right_side.shape[1]
    grids = [(gx * (sx >> l), gy * (sy >> l)) for l in range(LEVELS)]
    e = xy_coupling
    faces = z_faces.reshape(1, n)

    setup = call(
        powers_kernel,
        [(POWERS, n, n)] * LEVELS + [(8, n)] * LEVELS + [(POWERS, 8, n)] * LEVELS + [(8, n), (16, n), (gz, 12, 8, n)],
        [],
        (1,),
        block_inverse, e, faces,
    )
    power, ends, link = (setup[k * LEVELS : (k + 1) * LEVELS] for k in range(3))
    ends_up, basis, table = setup[3 * LEVELS :]
    low, high, table = lax.optimization_barrier((*halo_y(right_side, 12), table))
    f0 = halo_x(jnp.concatenate([low, right_side, high], axis=1), 12)
    table = exchange(table)
    *om, om_up, m_matrix, m_link, mix, w2_map = call(
        coupling_kernel,
        [(8, n)] * LEVELS + [(8, n), (n, n), (8, n), (11, n, n), (8, n)],
        [(gz, 8, 8, n), (n, n)],
        (0, 2),
        where, table, e, faces, basis,
    )

    s0, s1, s2 = (sx, sy), (sx // 2, sy // 2), (sx // 4, sy // 4)
    ext0, ext1 = (sx + 24, sy + 24), (sx // 2 + 10, sy // 2 + 16)
    cube0, cube1 = ext0 + (n,), ext1 + (n,)
    lines0, lines1 = ext0[0] * ext0[1], ext1[0] * ext1[1]
    lanes = padded_lanes(lines0) + padded_lanes(lines1) + padded_lanes(s2[0] * s2[1])
    copies, f1_local, f2_local = call(
        part(local_down_kernel, s0, s1, grids),
        [(gz, 8, lanes), cube1, s2 + (n,)],
        [cube0] * 4 + [(ext1[0], ext0[1], n)] + [cube1] * 4 + [(s2[0], ext1[1], n)],
        (0,),
        where, f0, power[0], power[1], ends[0], ends[1], ends[2],
    )
    got = stacked(copies)
    many = gx * gy
    f1, own1, parts = call(
        part(joined_down_kernel, s0, s1, ext0, grids),
        [cube1, cube1, (many, s2[0] + 1, s2[1], n)],
        [cube0] * 3 + [(ext1[0], ext0[1], n)] + [cube1] * 4 + [(s2[0], ext1[1], n), s2 + (n,)],
        (0,),
        where, got, f1_local, f2_local, mix, om[2], w2_map,
    )
    parts = lax.all_to_all(parts, ("gx", "gy"), 0, 0, tiled=True)
    inner0 = (sx + 8, sy + 8, n)
    known0, twice0 = call(
        part(known_zero_kernel, s0, ext0, grids[0]),
        [s0 + (n,), s0 + (n,)],
        [inner0] * 8,
        (0, 1),
        where, e, f0, got, mix, power[0], link[0],
        flops=20000000000,
    )
    (known1,) = call(
        part(known_one_kernel, s1, grids[1]),
        [cube1],
        [cube1] * 6,
        (0, 1),
        where, e, f1, own1, power[1], link[1],
        flops=10000000000,
    )
    parts, known0, twice0, known1 = lax.optimization_barrier((parts, known0, twice0, known1))

    cubes = [g + (n,) for g in grids]
    lines = [g[0] * g[1] for g in grids]
    margin = s2[0]
    region = (3 * s2[0], 3 * s2[1], n)
    padded = (grids[2][0] + 2 * margin, grids[2][1] + 2 * margin, n)
    f3, copies = call(
        part(gathered_down_kernel, gx, gy),
        [cubes[3], (gz, 8, lines[3])],
        [cubes[2], (lines[2], n), (8, lines[2])] + [cubes[2]] * 4 + [(grids[3][0], grids[2][1], n)],
        (),
        parts, power[2], link[2], ends[3],
    )
    got3 = stacked(copies)
    (known2,) = call(
        part(known_two_kernel, gx, gy, grids[2]),
        [region],
        [(region[0] * region[1], n), (8, region[0] * region[1])] + [region] * 6,
        (0, 1),
        where, e, parts, power[2], link[2],
        flops=8000000000,
    )
    got3, known2 = lax.optimization_barrier((got3, known2))
    f4, copies = call(
        whole_down_kernel,
        [cubes[4], (gz, 8, lines[4])],
        [cubes[3]] * 4 + [(grids[4][0], grids[3][1], n)],
        (),
        f3, got3, om[3], power[3], link[3], ends[4],
    )
    got4 = stacked(copies)
    (known3,) = call(
        part(whole_known_kernel, 3),
        [cubes[3]],
        [cubes[3]] * 6,
        (0,),
        e, f3, got3, om[3], power[3], link[3],
        flops=8000000000,
    )
    got4, known3 = lax.optimization_barrier((got4, known3))
    w3, copies = call(
        bottom_kernel,
        [cubes[3], (gz, 8, lines[3])],
        [cubes[4]] * 3,
        (0,),
        e, f4, got4, om[4], power[4], link[4], ends[3],
    )
    w2, copies = call(
        part(whole_up_kernel, margin),
        [region, (gz, 8, region[0] * region[1])],
        [cubes[3]] * 4 + [cubes[2], padded],
        (0,),
        where, w3, known3, stacked(copies), om[3], power[3], link[3], ends[2],
    )

    h0, h1 = (4, 4), (5, 8)
    cube0, lines0 = inner0, inner0[0] * inner0[1]
    w1, copies = call(
        part(up_kernel, (margin, margin), h1, grids[2]),
        [cube1, (gz, 8, lines1)],
        [region] * 4,
        (0,),
        where, w2, known2, stacked(copies), om[2], power[2], link[2], ends[1],
    )
    w0, copies = call(
        part(up_kernel, h1, h0, grids[1]),
        [cube0, (gz, 8, lines0)],
        [cube1] * 4,
        (0,),
        where, w1, known1, stacked(copies), om[1], power[1], link[1], ends_up,
    )
    u, r = call(
        part(final_kernel, h0, grids[0]),
        [(sx, sy, n), (sx, sy, n)],
        [cube0] * 5,
        (0, 1),
        where, e, w0, known0, twice0, stacked(copies), om_up, power[0], link[0], m_matrix, m_link,
    )
    return u, r


def solution(mesh):
    return jax.shard_map(
        body,
        mesh=mesh,
        in_specs=(P("gx", "gy", "gz"), P("gz"), P(), P(None, "gz", None)),
        out_specs=(P("gx", "gy", "gz"), P("gx", "gy", "gz")),
        check_vma=False,
    )
```

```python
import functools

import jax
import jax.numpy as jnp
from jax import lax
from jax.experimental import pallas as pl
from jax.experimental.pallas import tpu as pltpu
from jax.sharding import PartitionSpec as P

LEVELS = 5
POWERS = 4
HIGHEST = lax.Precision.HIGHEST
F32 = jnp.float32
VMEM_LIMIT = 56 * 1024 * 1024


def contract(a, b, da, db):
    return lax.dot_general(
        a, b, (((da,), (db,)), ((), ())), precision=HIGHEST, preferred_element_type=F32
    )


def exact_nn(a, b):
    return contract(a, b, 1, 0)


def exact_nt(a, b):
    return contract(a, b, 1, 1)


def exact_tn(a, b):
    return contract(a, b, 0, 0)


def halves(a):
    if isinstance(a, tuple):
        return a
    high = a.astype(jnp.bfloat16)
    return high, (a - high.astype(F32)).astype(jnp.bfloat16)


def product(a, b, da, db):
    (ah, al), (bh, bl) = halves(a), halves(b)

    def dot(x, y):
        return lax.dot_general(x, y, (((da,), (db,)), ((), ())), preferred_element_type=F32)

    return dot(ah, bh) + (dot(ah, bl) + dot(al, bh))


def nn(a, b):
    return product(a, b, 1, 0)


def nt(a, b):
    return product(a, b, 1, 1)


def tn(a, b):
    return product(a, b, 0, 0)


def rows(lo, hi, fn, step=4):
    full = (hi - lo) // step
    if full:
        def group(k, carry):
            for q in range(step):
                fn(lo + k * step + q)
            return carry

        lax.fori_loop(0, full, group, 0)
    for i in range(lo + full * step, hi):
        fn(i)


def sublane_index(length):
    return lax.broadcasted_iota(jnp.int32, (length, 128), 0)


def shifted(v, zero_ends):
    n = v.shape[0]
    low, high = pltpu.roll(v, 1, 0), pltpu.roll(v, n - 1, 0)
    if zero_ends:
        at = sublane_index(n)
        low = jnp.where(at > 0, low, 0.0)
        high = jnp.where(at < n - 1, high, 0.0)
    return low, high


class Window:
    def __init__(self, shape, origin=None, grid=None):
        self.x, self.y = shape
        self.whole = origin is None
        self.lo, self.hi = (0, self.y) if self.whole else (1, self.y - 1)
        if not self.whole:
            self.x0, y0 = origin
            self.nx, ny = grid
            at = sublane_index(self.y - 2) + (y0 + 1)
            self.in_y = jnp.where((at >= 0) & (at < ny), 1.0, 0.0).astype(F32)

    def get(self, ref, i):
        return ref[i, self.lo : self.hi]

    def put(self, ref, i, v):
        ref[i, self.lo : self.hi] = v

    def mask(self, i, v):
        if self.whole:
            return v
        at = self.x0 + i
        inside = jnp.where((at >= 0) & (at < self.nx), 1.0, 0.0).astype(F32)
        return v * (self.in_y * inside)

    def around(self, ref, i):
        if self.whole:
            low, high = shifted(ref[i], True)
            below = ref[jnp.maximum(i - 1, 0)] * jnp.where(i > 0, 1.0, 0.0).astype(F32)
            above = ref[jnp.minimum(i + 1, self.x - 1)] * jnp.where(i < self.x - 1, 1.0, 0.0).astype(F32)
            return (low + high) + (below + above)
        y = self.y
        return (ref[i, 0 : y - 2] + ref[i, 2:y]) + (ref[i - 1, 1 : y - 1] + ref[i + 1, 1 : y - 1])

    def span(self, trim):
        return (0, self.x) if self.whole else (trim, self.x - trim)

    def each(self, trim, out, fn):
        lo, hi = self.span(trim)
        rows(lo, hi, lambda i: self.put(out, i, fn(i)))


def line_powers(field, ends, power_ref, link_ref, count, out_refs, exact=False):
    if not exact:
        field, ends = halves(field), halves(ends)
    for j in range(count):
        if exact:
            value = exact_nt(field, power_ref[j]) + exact_tn(ends, link_ref[j])
        else:
            value = nt(field, power_ref[j]) + tn(ends, link_ref[j])
        out_refs[j][...] = value.reshape(out_refs[j].shape)


def smoothed_residual(win, field_ref, x1, x2, t, out, trim, masked=False, add=None):
    win.each(trim - 1, t, lambda i: 0.32 * win.get(x1, i) + win.mask(i, 0.64 * win.around(x2, i)))

    def outer(i):
        v = 0.04 * win.get(field_ref, i) + win.around(t, i)
        if add is not None:
            v = v + win.get(add, i)
        return win.mask(i, v) if masked else v

    win.each(trim, out, outer)


def horner(win, xs, weights, t0, t1, trim):
    src = xs[-1]
    scale = weights[-1]
    buffers = (t0, t1)
    for n, j in enumerate(range(len(xs) - 2, 0, -1)):
        dst = buffers[n % 2]

        def one(i, src=src, j=j, scale=scale):
            return weights[j] * win.get(xs[j], i) + win.mask(i, scale * win.around(src, i))

        win.each(trim - j, dst, one)
        src, scale = dst, 1.0
    return src, scale


def restrict(src, scratch, out, x_at, y_at):
    count_x, count_y = out.shape[0], out.shape[1]
    for i in range(count_x):
        scratch[i] = src[x_at + 2 * i] + src[x_at + 2 * i + 1]
    for i in range(count_x):
        even = scratch[i, pl.ds(y_at, count_y, stride=2), :]
        odd = scratch[i, pl.ds(y_at + 1, count_y, stride=2), :]
        out[i] = (even + odd) * 0.25


def prolong(src, src_whole, out, win, x_from, y_from, count_x, count_y):
    last = src.shape[0] - 1
    for i in range(count_x):
        at = x_from + i
        centre = src[at]
        below = src[at - 1] if at > 0 else jnp.zeros_like(centre)
        above = src[at + 1] if at < last else jnp.zeros_like(centre)
        for odd, other in ((0, below), (1, above)):
            v = 0.75 * centre + 0.25 * other
            low, high = shifted(v, src_whole)
            for parity, side in ((0, low), (1, high)):
                w = 0.75 * v + 0.25 * side
                out[2 * i + odd, pl.ds(parity, count_y, stride=2), :] = w[y_from : y_from + count_y]
    if not win.whole:
        win.each(0, out, lambda i: win.mask(i, win.get(out, i)))


def send(out_ref, value):
    for m in range(out_ref.shape[0]):
        out_ref[m] = value


def powers_kernel(g_ref, e_ref, zf_ref, *outs):
    levels, n = g_ref.shape[0], g_ref.shape[1]
    power_refs, ends_refs, link_refs = outs[0:levels], outs[levels : 2 * levels], outs[2 * levels : 3 * levels]
    up_ref, basis_ref, basis_up_ref, table_ref = outs[3 * levels :]
    table_ref[...] = jnp.zeros_like(table_ref)
    for level in range(levels):
        power_ref, ends_ref, link_ref = power_refs[level], ends_refs[level], link_refs[level]
        link_ref[...] = jnp.zeros_like(link_ref)
        e = e_ref[level]
        inverse_e = 1.0 / jnp.full((1, n), e, F32)
        one = g_ref[level] * e
        two = exact_nn(one, one)
        three = exact_nn(two, one)
        four = exact_nn(two, two)
        ends = []
        for j, value in enumerate((one, two, three, four)):
            power_ref[j] = value
            for s, row in enumerate((value[0:1], value[n - 1 : n])):
                ends_ref[2 * j + s : 2 * j + s + 1] = row
                table_ref[0, 2 * j + s, level : level + 1] = row
                ends.append(row)
        for j in range(POWERS):
            for i in range(j + 1):
                for t in range(2):
                    link_ref[j, 2 * i + t : 2 * i + t + 1] = ends[2 * (j - i) + t] * inverse_e
        table_ref[0, 9, level : level + 1] = inverse_e
    table_ref[0, 8] = jnp.broadcast_to(zf_ref[...], (8, n))
    def columns(level):
        return ends_refs[level][0:4] * (1.0 / jnp.full((4, n), e_ref[level], F32))

    zero = columns(0)
    basis_ref[0:4] = zero
    basis_ref[4:8] = exact_nn(zero, power_refs[1][0])
    basis_ref[8:12] = exact_nn(zero, power_refs[1][1])
    basis_ref[12:16] = columns(1)
    three = columns(3)
    two = [three, exact_nn(three, power_refs[2][0]), exact_nn(three, power_refs[2][1]), columns(2)]
    two = jnp.concatenate(two, 0)
    basis_up_ref[...] = jnp.zeros_like(basis_up_ref)
    basis_up_ref[0:16] = two
    basis_up_ref[16:32] = exact_nn(two, power_refs[1][0])
    basis_up_ref[32:48] = exact_nn(two, power_refs[1][1])
    basis_up_ref[48:52] = columns(1)
    at = lax.broadcasted_iota(jnp.int32, (1, n), 1)
    up_ref[...] = jnp.zeros_like(up_ref)
    up_ref[0:4] = ends_refs[0][0:4]
    up_ref[4:5] = jnp.where(at == 0, 1.0, 0.0).astype(F32)
    up_ref[5:6] = jnp.where(at == n - 1, 1.0, 0.0).astype(F32)


    full_basis = jnp.concatenate([basis_ref[...], jnp.zeros((n - 16, n), F32)], 0)
    at = lax.broadcasted_iota(jnp.int32, (8, n), 1)
    first = jnp.where(at < 4, exact_nt(ends_refs[1][...], full_basis), 0.0)
    second = exact_nt(ends_refs[2][...], full_basis)
    shifted_ends = jnp.concatenate([jnp.zeros((4, n), F32), ends_refs[2][0:4]], 0)
    third = jnp.where(at < 4, exact_nt(shifted_ends, basis_up_ref[...]), 0.0)
    fourth = jnp.where(at < 16, exact_nt(ends_refs[1][...], basis_up_ref[...]), 0.0)
    fifth = exact_nt(up_ref[...], basis_up_ref[...])
    total = first + pltpu.roll(second, 4, 1) + pltpu.roll(third, 20, 1)
    table_ref[0, 10] = total + pltpu.roll(fourth, 24, 1) + pltpu.roll(fifth, 40, 1)
    for m in range(1, table_ref.shape[0]):
        table_ref[m] = table_ref[0]


def coupling_kernel(
    where_ref, table_ref, e_ref, zf_ref, basis_ref, om0, om1, om2, om3, om4, om_up_ref, m_ref, m_link_ref, mix_ref, up_mix_ref, w2_ref, held, full
):
    blocks, n = table_ref.shape[0], table_ref.shape[3]
    k_own = where_ref[2]
    wide = (8, n)
    lane = lax.broadcasted_iota(jnp.int32, wide, 1)
    inverse_e = table_ref[0, 9]

    def entry(m, row, column):
        at = 0 if column == 0 else n - 1
        return jnp.broadcast_to(table_ref[m, row][:, at : at + 1], wide)

    corner = [
        [
            [[entry(m, 2 * i + s, t) * inverse_e for t in range(2)] for s in range(2)]
            for m in range(blocks)
        ]
        for i in range(POWERS)
    ]
    face = [entry(m, 8, 0) for m in range(blocks)]

    gain_v, gain_d, gain_p, gain_g = [corner[0][0][1][1]], [None], [None], [None]
    for k in range(1, blocks):
        (a, b), (c, d) = corner[0][k]
        g = face[k]
        gv = g * g * gain_v[k - 1]
        dk = 1.0 / (1.0 - a * gv)
        gain_d.append(dk)
        gain_p.append(dk * b)
        gain_g.append(gv)
        gain_v.append(d + c * gv * gain_p[k])

    def solve(low, high):
        u, pu = [high[0]], [None]
        for k in range(1, blocks):
            (a, b), (c, d) = corner[0][k]
            gu = face[k] * u[k - 1]
            pu.append(gain_d[k] * (low[k] + a * gu))
            u.append(high[k] + c * (gu + gain_g[k] * pu[k]))
        zero = jnp.zeros(wide, F32)
        alpha, beta = [zero] * blocks, [zero] * blocks
        for k in range(blocks - 1, 0, -1):
            p = pu[k] + gain_p[k] * beta[k]
            beta[k - 1] = face[k] * p
            alpha[k] = face[k] * (u[k - 1] + gain_v[k - 1] * beta[k - 1])
        return alpha, beta

    unit = [
        [jnp.where(lane == 8 * m + s, 1.0, 0.0).astype(F32) for m in range(blocks)] for s in range(2)
    ]
    response = [solve(unit[0], unit[1])]
    for i in range(1, POWERS):
        source = [[None] * blocks, [None] * blocks]
        for m in range(blocks):
            for s in range(2):
                total = None
                for q in range(i):
                    c = corner[i - q][m][s]
                    term = c[0] * response[q][0][m] + c[1] * response[q][1][m]
                    total = term if total is None else total + term
                source[s][m] = total
        response.append(solve(source[0], source[1]))
    for i in range(POWERS):
        for t in range(2):
            for m in range(blocks):
                held[m, 2 * i + t] = response[i][t][m]
    om_refs = (om0, om1, om2, om3, om4)
    for i in range(POWERS):
        for t in range(2):
            total = held[k_own, 2 * i + t]
            for j in range(1, i + 1):
                total = total + pltpu.roll(held[k_own, 2 * (i - j) + t], 2 * j, 1)
            for level in range(LEVELS):
                om_refs[level][2 * i + t : 2 * i + t + 1] = total[level : level + 1]
    om_up_ref[...] = om0[...]

    lane = lane[0:1]
    om_up_ref[4:5] = jnp.where((lane == 8 * (k_own - 1) + 5) & (k_own > 0), 1.0, 0.0).astype(F32)
    om_up_ref[5:6] = jnp.where((lane == 8 * (k_own + 1) + 4) & (k_own < blocks - 1), 1.0, 0.0).astype(F32)
    om_up_ref[6:8] = jnp.zeros((2, n), F32)

    row = lax.broadcasted_iota(jnp.int32, (n, n), 0)
    column = lax.broadcasted_iota(jnp.int32, (n, n), 1)

    def every(i, t, m, offset):
        total = held[m, 2 * i + t]
        if i == 1:
            total = total + pltpu.roll(held[m, t], 2, 1)
        return pltpu.roll(total, offset, 1) if offset else total

    def matrix(level, groups, own=None, offset=0):
        full[...] = jnp.zeros_like(full)
        for start, i, scale in groups:
            for m in range(blocks):
                for t in range(2):
                    at = start + 2 * m + t
                    full[at : at + 1] = scale * every(i, t, m, offset)[level : level + 1]
        if own is not None:
            full[own : own + 8] = om_refs[level][...]
        return full[...].T

    def gathered(offset, count):
        tiles = jnp.concatenate([table_ref[m, 10] for m in range(blocks)], 0)
        at = row - offset
        place = (at >= 0) & (at < count) & (at == (column >> 4) * 2 + (column & 1))
        value = exact_nn(tiles, jnp.where(place, 1.0, 0.0).astype(F32))
        high = 8 * blocks
        value = jnp.where((row[0:high] >> 3) == ((column[0:high] >> 1) & 7), value, 0.0)
        return jnp.concatenate([value, jnp.zeros((n - high, n), F32)], 0)

    def diagonal(shift, scale):
        return jnp.where((row < 32) & (column == row + shift), scale, 0.0).astype(F32)

    def rest(slot_ref, base, level, once, twice, table):
        slot_ref[base] = once
        slot_ref[base + 1] = twice
        slot_ref[base + 2] = diagonal(0, 0.04)
        slot_ref[base + 3] = exact_nn(table, once) + diagonal(32, 0.32)
        slot_ref[base + 4] = exact_nn(table, twice) + diagonal(64, 0.64)

    mix_ref[0] = matrix(0, [(0, 0, 0.32)], 64)
    mix_ref[1] = matrix(0, [(0, 1, 0.64), (16, 0, 0.64)])
    one = gathered(0, 4).T
    rest(mix_ref, 2, 1, matrix(1, [(96, 0, 0.32)]), matrix(1, [(96, 1, 0.64), (112, 0, 0.64)]), one)
    mix_ref[7] = matrix(1, [], 0)
    mix_ref[8] = exact_nn(one, mix_ref[7])
    w2_ref[...] = exact_nn(om2[...], gathered(4, 16))
    basis = jnp.concatenate([basis_ref[...], jnp.zeros((n - 16, n), F32)], 0)
    own_rows = jnp.where(
        (row < 16) & (column == (row >> 1) * 16 + 2 * k_own + (row & 1)), 1.0, 0.0
    ).astype(F32)
    chosen = exact_tn(own_rows, basis)
    mix_ref[9] = jnp.where(row < 32, chosen, 0.0)
    mix_ref[10] = chosen

    up_mix_ref[0] = matrix(3, [(0, 0, 0.32)])
    up_mix_ref[1] = matrix(3, [(0, 1, 0.64), (16, 0, 0.64)])
    once = matrix(2, [(96, 0, 0.32)], offset=4)
    twice = matrix(2, [(96, 1, 0.64), (112, 0, 0.64)], offset=4)
    rest(up_mix_ref, 2, 2, once, twice, gathered(20, 4).T)
    both = matrix(1, [(0, 0, 1.0), (16, 1, 1.0)])
    through = exact_nn(gathered(24, 16).T, both)
    up_rows = om_up_ref[...]
    for k, scale in enumerate((0.04, 0.32, 0.64)):
        full[...] = jnp.zeros_like(full)
        full[16 * k : 16 * k + 16] = scale * own_rows[0:16]
        full[64:72] = scale * exact_nn(up_rows, gathered(40 + 16 * k, 16))
        up_mix_ref[7 + k] = full[...].T
    last = exact_nn(up_rows, gathered(88, 4))
    wide_lane = lax.broadcasted_iota(jnp.int32, (8, n), 1)
    full[...] = jnp.zeros_like(full)
    for t in range(2):
        full[48 + t : 49 + t] = jnp.where(lane == 2 * k_own + t, 0.32, 0.0).astype(F32)
    full[64:72] = jnp.where(wide_lane < 16, 0.32 * last, 0.0)
    mixed = full[...].T
    up_mix_ref[8] = up_mix_ref[8] + exact_nn(through, mixed)
    up_mix_ref[10] = exact_nn(both, mixed)
    full[...] = jnp.zeros_like(full)
    for t in range(2):
        full[48 + t : 49 + t] = jnp.where(lane == 16 + 2 * k_own + t, 0.64, 0.0).astype(F32)
        full[50 + t : 51 + t] = jnp.where(lane == 2 * k_own + t, 0.64, 0.0).astype(F32)
    swapped = jnp.where(
        wide_lane < 16,
        pltpu.roll(last, n - 16, 1),
        jnp.where(wide_lane < 32, pltpu.roll(last, 16, 1), 0.0),
    )
    full[64:72] = 0.64 * swapped
    mixed = full[...].T
    up_mix_ref[9] = up_mix_ref[9] + exact_nn(through, mixed)
    up_mix_ref[11] = exact_nn(both, mixed)
    full[...] = jnp.zeros_like(full)
    full[64:72] = up_rows
    up_mix_ref[12] = full[...].T

    above = jnp.minimum(k_own + 1, blocks - 1)
    top = table_ref[above, 8][0:1, 0:1]
    top = jnp.where(jnp.full((1, 1), k_own, jnp.int32) < blocks - 1, top, 1.0)
    down = zf_ref[...]
    up = jnp.where(lane == n - 1, jnp.broadcast_to(top, (1, n)), pltpu.roll(down, n - 1, 1))
    down_all, up_all = jnp.broadcast_to(down, (n, n)), jnp.broadcast_to(up, (n, n))
    m_ref[...] = jnp.where(
        row == column,
        down_all + up_all + 4.0 * e_ref[0],
        jnp.where(row == column - 1, -down_all, jnp.where(row == column + 1, -up_all, 0.0)),
    )
    m_link_ref[...] = jnp.zeros_like(m_link_ref)
    m_link_ref[4:5] = jnp.where(lane == 0, -down, 0.0)
    m_link_ref[5:6] = jnp.where(lane == n - 1, -up, 0.0)


def flat(ref):
    return ref[...].reshape(ref.shape[0] * ref.shape[1], ref.shape[2])


def ends_from(om_ref, got_ref):
    return exact_nn(om_ref[:, : got_ref.shape[0]], got_ref[...])


def restrict_into(src, scratch, out, x_at, y_at, count_y, y_to):
    for i in range(out.shape[0]):
        scratch[i] = src[x_at + 2 * i] + src[x_at + 2 * i + 1]
    for i in range(out.shape[0]):
        even = scratch[i, pl.ds(y_at, count_y, stride=2), :]
        odd = scratch[i, pl.ds(y_at + 1, count_y, stride=2), :]
        out[i, y_to : y_to + count_y] = (even + odd) * 0.25


def padded_lanes(count):
    return (count + 127) // 128 * 128


def windows(where_ref, s0, s1, ext0, ext1, grids):
    h0 = tuple((a - b) // 2 for a, b in zip(ext0, s0))
    h1 = tuple((a - b) // 2 for a, b in zip(ext1, s1))
    ix, iy = where_ref[0], where_ref[1]
    win0 = Window(ext0, (ix * s0[0] - h0[0], iy * s0[1] - h0[1]), grids[0])
    win1 = Window(ext1, (ix * s1[0] - h1[0], iy * s1[1] - h1[1]), grids[1])
    return win0, win1, h0, h1


def local_down_kernel(
    s0, s1, grids, where_ref, f_ref, power0, power1, v0, v1, v2, out_ref, f1_ref, f2_ref,
    x1, x2, t, r, pair, y1, y2, t1, r1, pair1
):
    ext0, ext1 = f_ref.shape[:2], f1_ref.shape[:2]
    win0, win1, h0, h1 = windows(where_ref, s0, s1, ext0, ext1, grids)
    field = halves(flat(f_ref))
    lanes0 = ext0[0] * ext0[1]
    lanes1 = ext1[0] * ext1[1]
    at1 = padded_lanes(lanes0)
    at2 = at1 + padded_lanes(lanes1)
    many = out_ref.shape[0]
    out_ref[0, :, at1 - 128 : at1] = jnp.zeros((8, 128), F32)
    out_ref[0, :, at2 - 128 : at2] = jnp.zeros((8, 128), F32)
    out_ref[0, :, at2 : at2 + 128] = jnp.zeros((8, 128), F32)
    out_ref[0, :, 0:lanes0] = nt(v0[...], field)
    x1[...] = nt(field, power0[0]).reshape(x1.shape)
    x2[...] = nt(field, power0[1]).reshape(x2.shape)
    smoothed_residual(win0, f_ref, x1, x2, t, r, 2, masked=True)
    f1_ref[...] = jnp.zeros_like(f1_ref)
    count = (ext0[1] - 4) // 2
    restrict_into(r, pair, f1_ref, 2, 2, count, (ext1[1] - count) // 2)
    field = halves(flat(f1_ref))
    out_ref[0, :, at1 : at1 + lanes1] = nt(v1[...], field)
    y1[...] = nt(field, power1[0]).reshape(y1.shape)
    y2[...] = nt(field, power1[1]).reshape(y2.shape)
    smoothed_residual(win1, f1_ref, y1, y2, t1, r1, h1[0])
    restrict(r1, pair1, f2_ref, h1[0], h1[1])
    lines2 = f2_ref.shape[0] * f2_ref.shape[1]
    out_ref[0, :, at2 : at2 + lines2] = nt(v2[...], flat(f2_ref))
    for m in range(1, many):
        out_ref[m] = out_ref[0]


def joined_down_kernel(
    s0, s1, ext0, grids, where_ref, got_ref, f1_local, f2_local, mix_ref, om2_ref, w2_ref,
    f1_ref, own1_ref, parts_ref, d1, d2, f, pair, y, h1s, h2s, f2s, pair1, z
):
    ext1 = f1_local.shape[:2]
    win0, win1, h0, h1 = windows(where_ref, s0, s1, ext0, ext1, grids)
    lanes0 = ext0[0] * ext0[1]
    lanes1 = ext1[0] * ext1[1]
    at1 = padded_lanes(lanes0)
    at2 = at1 + padded_lanes(lanes1)
    got0 = halves(got_ref[:, 0:lanes0])
    rows_in = got_ref.shape[0]
    d1[...] = tn(got0, mix_ref[0, 0:rows_in]).reshape(d1.shape)
    d2[...] = tn(got0, mix_ref[1, 0:rows_in]).reshape(d2.shape)

    win0.each(1, d1, lambda i: win0.get(d1, i) + win0.mask(i, win0.around(d2, i)))
    win0.each(2, f, lambda i: win0.mask(i, win0.around(d1, i)))
    y[...] = jnp.zeros_like(y)
    count = (ext0[1] - 4) // 2
    restrict_into(f, pair, y, 2, 2, count, (ext1[1] - count) // 2)
    yf = halves(flat(y))
    f1_ref[...] = f1_local[...] + nn(yf, mix_ref[9]).reshape(f1_ref.shape)
    got1 = halves(got_ref[:, at1 : at1 + lanes1])
    own1_ref[...] = (tn(got1, mix_ref[7, 0:rows_in]) + nn(yf, mix_ref[8])).reshape(own1_ref.shape)
    h1s[...] = (tn(got1, mix_ref[2, 0:rows_in]) + nn(yf, mix_ref[5])).reshape(h1s.shape)
    h2s[...] = (tn(got1, mix_ref[3, 0:rows_in]) + nn(yf, mix_ref[6])).reshape(h2s.shape)
    f2s[...] = nn(yf, mix_ref[4]).reshape(f2s.shape)
    trim = h1[0]
    win1.each(trim - 1, h1s, lambda i: win1.get(h1s, i) + win1.mask(i, win1.around(h2s, i)))
    win1.each(trim, f2s, lambda i: win1.get(f2s, i) + win1.around(h1s, i))
    restrict(f2s, pair1, z, h1[0], h1[1])
    zf = flat(z)
    lines2 = zf.shape[0]
    side = z.shape[0]
    parts_ref[0, 0:side] = f2_local[...] + nn(zf, mix_ref[10]).reshape(z.shape)
    own2 = nn(om2_ref[:, 0:rows_in], got_ref[:, at2 : at2 + lines2]) + nt(w2_ref[...], zf)
    parts_ref[0, side] = jnp.zeros((8, 128), F32)
    parts_ref[0, side, :, 0:lines2] = own2
    for m in range(1, parts_ref.shape[0]):
        parts_ref[m] = parts_ref[0]


KNOWN = (0.9984, 0.9728, 0.8192, 0.4096)
TWICE = (0.0016, 0.0256, 0.1536, 0.4096, 0.4096)


def lane_powers(field, coefficients, lane0, power_ref, link_ref, count, out_refs, exact=False):
    n = field.shape[1]
    if not exact:
        field, coefficients = halves(field), halves(coefficients)
    one, two = (exact_nt, exact_nn) if exact else (nt, nn)
    for j in range(count):
        pieces = [link_ref[j], jnp.zeros((n - 8 - lane0, n), F32)]
        if lane0:
            pieces = [jnp.zeros((lane0, n), F32)] + pieces
        value = one(field, power_ref[j]) + two(coefficients, jnp.concatenate(pieces, 0))
        out_refs[j][...] = value.reshape(out_refs[j].shape)


def known_zero_kernel(
    s0, ext0, grid, where_ref, e_ref, f_ref, got_ref, mix_ref, power_ref, link_ref,
    known_out, twice_out, own, f, x1, x2, x3, x4, t0, t1
):
    hx, hy = (f.shape[0] - s0[0]) // 2, (f.shape[1] - s0[1]) // 2
    cx, cy = (ext0[0] - f.shape[0]) // 2, (ext0[1] - f.shape[1]) // 2
    win = Window(f.shape[:2], (where_ref[0] * s0[0] - hx, where_ref[1] * s0[1] - hy), grid)
    coefficients = tn(got_ref[:, 0 : ext0[0] * ext0[1]], mix_ref[0, 0 : got_ref.shape[0]])
    own[...] = coefficients.reshape(ext0 + (128,))[cx : cx + f.shape[0], cy : cy + f.shape[1]]
    f[...] = f_ref[cx : cx + f.shape[0], cy : cy + f.shape[1]]
    xs = (x1, x2, x3, x4)
    lane_powers(flat(f), flat(own), 64, power_ref, link_ref, POWERS, xs)
    inverse_e = 1.0 / jnp.full((win.hi - win.lo, 128), e_ref[0], F32)
    at = hy - win.lo
    src, scale = horner(win, xs, KNOWN, t0, t1, hx)
    lo, hi = win.span(hx)

    def known(i):
        v = (KNOWN[0] * win.get(x1, i) + scale * win.around(src, i)) * inverse_e
        known_out[i - hx] = v[at : at + s0[1]]

    rows(lo, hi, known)
    src2, scale2 = horner(win, (f,) + xs, TWICE, t0, t1, hx)

    def again(i):
        v = TWICE[0] * win.get(f, i) + scale2 * win.around(src2, i)
        twice_out[i - hx] = v[at : at + s0[1]]

    rows(lo, hi, again)


def known_one_kernel(
    s1, grid, where_ref, e_ref, f_ref, own_ref, power_ref, link_ref, known_out, x1, x2, x3, x4, t0, t1
):
    hx, hy = (f_ref.shape[0] - s1[0]) // 2, (f_ref.shape[1] - s1[1]) // 2
    win = Window(f_ref.shape[:2], (where_ref[0] * s1[0] - hx, where_ref[1] * s1[1] - hy), grid)
    xs = (x1, x2, x3, x4)
    lane_powers(flat(f_ref), flat(own_ref), 0, power_ref, link_ref, POWERS, xs, exact=True)
    inverse_e = 1.0 / jnp.full((win.hi - win.lo, 128), e_ref[1], F32)
    src, scale = horner(win, xs, KNOWN, t0, t1, 3)
    known_out[...] = jnp.zeros_like(known_out)

    def known(i):
        return win.mask(i, (KNOWN[0] * win.get(x1, i) + scale * win.around(src, i)) * inverse_e)

    win.each(3, known_out, known)


def known_two_kernel(
    across, down, grid, where_ref, e_ref, parts_ref, power_ref, link_ref, known_out,
    fp, ap, x1, x2, x3, x4, t0, t1
):
    side = parts_ref.shape[2]
    lines = side * side
    ix, iy = where_ref[0], where_ref[1]
    for p in range(9):
        jx, jy = ix + p // 3 - 1, iy + p % 3 - 1
        inside = (jx >= 0) & (jx < across) & (jy >= 0) & (jy < down)
        at = jnp.clip(jx, 0, across - 1) * down + jnp.clip(jy, 0, down - 1)
        scale = jnp.where(inside, 1.0, 0.0).astype(F32)
        fp[p * lines : (p + 1) * lines] = (parts_ref[at, 0:side] * scale).reshape(lines, 128)
        ap[:, p * lines : (p + 1) * lines] = (parts_ref[at, side] * scale)[:, 0:lines]
    xs = (x1, x2, x3, x4)
    for j in range(POWERS):
        value = exact_nt(fp[...], power_ref[j]) + exact_tn(ap[...], link_ref[j])
        for p in range(9):
            px, py = p // 3 * side, p % 3 * side
            piece = value[p * lines : (p + 1) * lines].reshape(side, side, 128)
            xs[j][px : px + side, py : py + side] = piece
    win = Window(x1.shape[:2], ((ix - 1) * side, (iy - 1) * side), grid)
    inverse_e = 1.0 / jnp.full((win.hi - win.lo, 128), e_ref[2], F32)
    src, scale = horner(win, xs, KNOWN, t0, t1, 3)
    known_out[...] = jnp.zeros_like(known_out)

    def known(i):
        return win.mask(i, (KNOWN[0] * win.get(x1, i) + scale * win.around(src, i)) * inverse_e)

    win.each(3, known_out, known)


def gathered_down_kernel(
    across, down, parts_ref, power_ref, link_ref, v_ref, coarse_ref, out_ref, f, fp, ap, x1, x2, t, r, pair
):
    many, side = parts_ref.shape[0], parts_ref.shape[2]
    lines = side * side
    for p in range(many):
        px, py = p // down * side, p % down * side
        part = parts_ref[p, 0:side]
        f[px : px + side, py : py + side] = part
        fp[p * lines : (p + 1) * lines] = part.reshape(lines, 128)
        ap[:, p * lines : (p + 1) * lines] = parts_ref[p, side][:, 0:lines]
    fields, coefficients = halves(fp[...]), halves(ap[...])
    for j, x in enumerate((x1, x2)):
        value = nt(fields, power_ref[j]) + tn(coefficients, link_ref[j])
        for p in range(many):
            px, py = p // down * side, p % down * side
            x[px : px + side, py : py + side] = value[p * lines : (p + 1) * lines].reshape(side, side, 128)
    win = Window(f.shape[:2])
    smoothed_residual(win, f, x1, x2, t, r, 2)
    restrict(r, pair, coarse_ref, 0, 0)
    send(out_ref, nt(v_ref[...], flat(coarse_ref)))


def whole_down_kernel(
    f_ref, got_ref, om_ref, power_ref, link_ref, v_ref, coarse_ref, out_ref, x1, x2, t, r, pair
):
    win = Window(f_ref.shape[:2])
    ends = ends_from(om_ref, got_ref)
    line_powers(flat(f_ref), ends, power_ref, link_ref, 2, (x1, x2))
    smoothed_residual(win, f_ref, x1, x2, t, r, 2)
    restrict(r, pair, coarse_ref, 0, 0)
    send(out_ref, nt(v_ref[...], flat(coarse_ref)))


def whole_known_kernel(
    level, e_ref, f_ref, got_ref, om_ref, power_ref, link_ref, known_ref, x1, x2, x3, x4, t0, t1
):
    win = Window(f_ref.shape[:2])
    ends = ends_from(om_ref, got_ref)
    xs = (x1, x2, x3, x4)
    line_powers(flat(f_ref), ends, power_ref, link_ref, POWERS, xs, exact=True)
    inverse_e = 1.0 / jnp.full((f_ref.shape[1], 128), e_ref[level], F32)
    src, scale = horner(win, xs, KNOWN, t0, t1, 4)

    def known(i):
        known_ref[i] = (KNOWN[0] * x1[i] + scale * win.around(src, i)) * inverse_e

    rows(0, win.x, known)


def clear_edges(pad, margin):
    x, y = pad.shape[:2]
    zero_rows = jnp.zeros((margin, y, 128), F32)
    zero_cols = jnp.zeros((x, margin, 128), F32)
    pad[0:margin] = zero_rows
    pad[x - margin : x] = zero_rows
    pad[:, 0:margin] = zero_cols
    pad[:, y - margin : y] = zero_cols


def cut(where_ref, pad, out_ref, margin):
    sx, sy = out_ref.shape[0] - 2 * margin, out_ref.shape[1] - 2 * margin
    x_at = where_ref[0] * sx
    y_at = pl.multiple_of(where_ref[1] * sy, 8)

    def one(i):
        out_ref[i] = pad[x_at + i, pl.ds(y_at, out_ref.shape[1]), :]

    rows(0, out_ref.shape[0], one)


UP_LANES = (1664, 896, 512)


def place_on_region(where_ref, fine, pad, out_ref, margin):
    clear_edges(pad, margin)

    def place(i):
        pad[i + margin, margin : margin + fine.shape[1]] = fine[i]

    rows(0, fine.shape[0], place)
    cut(where_ref, pad, out_ref, margin)


def up_windows(where_ref, s0, grids, region, ext1, ext0):
    s1, s2 = (s0[0] // 2, s0[1] // 2), (s0[0] // 4, s0[1] // 4)
    wins = []
    for level, (shape, s) in enumerate(((ext0, s0), (ext1, s1), (region, s2))):
        hx, hy = (shape[0] - s[0]) // 2, (shape[1] - s[1]) // 2
        wins.append(Window(shape, (where_ref[0] * s[0] - hx, where_ref[1] * s[1] - hy), grids[level]))
    return wins


def to_level_one(src, out, win):
    prolong_odd(src, out, win, 5, 4, (out.shape[0] + 2) // 2, out.shape[1] // 2)


def to_level_zero(src, out, win):
    prolong(src, False, out, win, 3, 6, out.shape[0] // 2, out.shape[1] // 2)


def local_up_kernel(
    s0, grids, margin, where_ref, e_ref, f_ref, got_ref, om_ref, power4, link4, known3, known2, known1,
    power3, power2, power1, v3, v2, v1, v0, out_ref, c1_ref,
    b1, b2, c4, w3, p1, p2, pt, c3, fine, pad, w2, q1, q2, qt, c2, w1, r1, r2, rt, w0
):
    win = Window(f_ref.shape[:2])
    ends = ends_from(om_ref, got_ref)
    line_powers(flat(f_ref), ends, power4, link4, 2, (b1, b2), exact=True)
    inverse_e = 1.0 / jnp.full((f_ref.shape[1], 128), e_ref[LEVELS - 1], F32)

    def one(i):
        c4[i] = (0.96 * b1[i] + 0.64 * win.around(b2, i)) * inverse_e

    rows(0, win.x, one)
    win3 = Window(w3.shape[:2])
    prolong(c4, True, w3, win3, 0, 0, win.x, win.y)
    win0, win1, win2 = up_windows(where_ref, s0, grids, w2.shape[:2], w1.shape[:2], w0.shape[:2])
    at1, at2 = UP_LANES[0], UP_LANES[0] + UP_LANES[1]
    out_ref[0] = jnp.zeros(out_ref.shape[1:], F32)

    def local(win, w, known, power, x1, x2, t, c):
        field = flat(w)
        x1[...] = exact_nt(field, power[0]).reshape(x1.shape)
        x2[...] = exact_nt(field, power[1]).reshape(x2.shape)
        c[...] = jnp.zeros_like(c)
        smoothed_residual(win, w, x1, x2, t, c, 2, masked=True, add=known)

    def words(v_ref, w, first_row, at):
        value = exact_nt(v_ref[...], flat(w))
        out_ref[0, first_row : first_row + 4, at : at + value.shape[1]] = value[0:4]

    words(v3, w3, 0, at2)
    local(win3, w3, known3, power3, p1, p2, pt, c3)
    prolong(c3, True, fine, Window(fine.shape[:2]), 0, 0, win3.x, win3.y)
    place_on_region(where_ref, fine, pad, w2, margin)
    words(v2, w2, 4, at1)
    local(win2, w2, known2, power2, q1, q2, qt, c2)
    to_level_one(c2, w1, win1)
    words(v1, w1, 0, at1)
    local(win1, w1, known1, power1, r1, r2, rt, c1_ref)
    to_level_zero(c1_ref, w0, win0)
    value = exact_nt(v0[...], flat(w0))
    out_ref[0, :, 0 : value.shape[1]] = value
    for m in range(1, out_ref.shape[0]):
        out_ref[m] = out_ref[0]


def finish_kernel(
    s0, grids, margin, where_ref, e_ref, got_ref, c1_local, known_ref, twice_ref, mix_ref, basis_ref,
    power_ref, link_ref, m_ref, m_link_ref, u_ref, r_ref,
    d1, d2, d3, fine, pad, y2, g1, g2, g3, y1, h1, h2, h3, c1, w, q, x1, x2, xm, t0, t1
):
    win0, win1, win2 = up_windows(where_ref, s0, grids, y2.shape[:2], y1.shape[:2], w.shape[:2])
    lines0, lines1 = w.shape[0] * w.shape[1], y1.shape[0] * y1.shape[1]
    lines2, lines3 = y2.shape[0] * y2.shape[1], d1.shape[0] * d1.shape[1]
    at1, at2 = UP_LANES[0], UP_LANES[0] + UP_LANES[1]
    k = got_ref.shape[0]

    got3 = halves(got_ref[:, at2 : at2 + lines3])
    d1[...] = tn(got3, mix_ref[0, 0:k]).reshape(d1.shape)
    d2[...] = tn(got3, mix_ref[1, 0:k]).reshape(d2.shape)
    win3 = Window(d1.shape[:2])
    win3.each(0, d1, lambda i: win3.get(d1, i) + win3.around(d2, i))
    win3.each(0, d3, lambda i: win3.around(d1, i))
    prolong(d3, True, fine, Window(fine.shape[:2]), 0, 0, win3.x, win3.y)
    place_on_region(where_ref, fine, pad, y2, margin)

    def coefficients(win, got, y, once, twice, maps, a1, a2, a3, trim):
        y, got = halves(flat(y)), halves(got)
        a1[...] = (tn(got, once[0:k]) + nn(y, maps[1])).reshape(a1.shape)
        a2[...] = (tn(got, twice[0:k]) + nn(y, maps[2])).reshape(a2.shape)
        a3[...] = nn(y, maps[0]).reshape(a3.shape)
        win.each(trim - 1, a1, lambda i: win.get(a1, i) + win.mask(i, win.around(a2, i)))
        win.each(trim, a3, lambda i: win.mask(i, win.get(a3, i) + win.around(a1, i)))

    maps = (mix_ref[4], mix_ref[5], mix_ref[6])
    got2 = got_ref[:, at1 : at1 + lines2]
    coefficients(win2, got2, y2, mix_ref[2], mix_ref[3], maps, g1, g2, g3, 2)
    to_level_one(g3, y1, win1)
    maps = (mix_ref[7], mix_ref[8], mix_ref[9])
    got1 = got_ref[:, at1 : at1 + lines1]
    coefficients(win1, got1, y1, mix_ref[10], mix_ref[11], maps, h1, h2, h3, 2)
    c1[...] = c1_local[...] + exact_nn(flat(h3), basis_ref[...]).reshape(c1.shape)
    to_level_zero(c1, w, win0)
    to_level_zero(h3, q, win0)
    q[...] = q[...] + tn(got_ref[:, 0:lines0], mix_ref[12, 0:k]).reshape(q.shape)

    hx, hy = (w.shape[0] - s0[0]) // 2, (w.shape[1] - s0[1]) // 2
    sy = s0[1]
    win = win0
    field, ends = flat(w), flat(q)
    lane_powers(field, ends, 64, power_ref, link_ref, 2, (x1, x2), exact=True)
    n = field.shape[1]
    m_link = jnp.concatenate([jnp.zeros((64, n), F32), m_link_ref[...], jnp.zeros((n - 72, n), F32)], 0)
    xm[...] = (exact_nt(field, m_ref[...]) + exact_nn(ends, m_link)).reshape(xm.shape)
    e = e_ref[0]
    w_ref = w

    lo, hi = win.span(hx - 2)

    def inner(i):
        one = 0.32 * win.get(x1, i)
        two = win.mask(i, 0.64 * win.around(x2, i))
        win.put(t0, i, one + two)
        win.put(t1, i, e * (one - two))

    rows(lo, hi, inner)
    win.each(hx - 1, x2, lambda i: (0.28 * e) * win.get(w_ref, i) + win.mask(i, win.around(t1, i)))
    lo, hi = win.span(hx)
    cut_y = hy - win.lo

    def last(i):
        u = 0.04 * win.get(w_ref, i) + win.around(t0, i)
        u_ref[i - hx] = known_ref[i - hx] + u[cut_y : cut_y + sy]
        r = 0.04 * win.get(xm, i) + win.around(x2, i)
        r_ref[i - hx] = twice_ref[i - hx] - r[cut_y : cut_y + sy]

    rows(lo, hi, last)


def prolong_odd(src, out, win, x_from, y_from, count_x, count_y):
    for i in range(count_x):
        at = x_from + i
        for odd, other in ((0, at - 1), (1, at + 1)):
            row = 2 * i + odd - 1
            if row < 0 or row >= out.shape[0]:
                continue
            v = 0.75 * src[at] + 0.25 * src[other]
            low, high = shifted(v, False)
            for parity, side in ((0, low), (1, high)):
                w = 0.75 * v + 0.25 * side
                out[row, pl.ds(parity, count_y, stride=2), :] = w[y_from : y_from + count_y]
    win.each(0, out, lambda i: win.mask(i, win.get(out, i)))


def call(kernel, outs, scratch, smem, *args, flops=0):
    specs = [
        pl.BlockSpec(memory_space=pltpu.SMEM if k in smem else pltpu.VMEM) for k in range(len(args))
    ]
    out_specs = [pl.BlockSpec(memory_space=pltpu.VMEM) for _ in outs]
    return pl.pallas_call(
        kernel,
        out_shape=[jax.ShapeDtypeStruct(s, F32) for s in outs],
        in_specs=specs,
        out_specs=out_specs,
        scratch_shapes=[pltpu.VMEM(s, F32) for s in scratch],
        compiler_params=pltpu.CompilerParams(vmem_limit_bytes=VMEM_LIMIT),
        cost_estimate=pl.CostEstimate(flops=int(flops) or 1000000, bytes_accessed=1000000, transcendentals=0),
    )(*args)


def exchange(copies, axes="gz"):
    got = lax.all_to_all(copies, axes, 0, 0, tiled=True)
    return got


def stacked(copies):
    got = exchange(copies)
    return got.reshape(got.shape[0] * got.shape[1], got.shape[2])


def edges(v, axis, dim, width):
    size, length = lax.axis_size(axis), v.shape[dim]
    up = [(i, i + 1) for i in range(size - 1)]
    last = lax.slice_in_dim(v, length - width, length, axis=dim)
    first = lax.slice_in_dim(v, 0, width, axis=dim)
    return lax.ppermute(last, axis, up), lax.ppermute(first, axis, [(b, a) for a, b in up])


def halo_y(v, width):
    return edges(v, "gy", 1, width)


def halo_x(v, width):
    low, high = edges(v, "gx", 0, width)
    return jnp.concatenate([low, v, high], axis=0)


def body(right_side, z_faces, xy_coupling, block_inverse):
    part = functools.partial
    gx, gy, gz = (lax.axis_size(a) for a in ("gx", "gy", "gz"))
    n = z_faces.shape[0]
    where = jnp.stack([lax.axis_index(a) for a in ("gx", "gy", "gz")]).astype(jnp.int32)
    sx, sy = right_side.shape[0], right_side.shape[1]
    grids = [(gx * (sx >> l), gy * (sy >> l)) for l in range(LEVELS)]
    e = xy_coupling
    faces = z_faces.reshape(1, n)

    setup = call(
        powers_kernel,
        [(POWERS, n, n)] * LEVELS + [(8, n)] * LEVELS + [(POWERS, 8, n)] * LEVELS + [(8, n), (16, n), (n, n), (gz, 11, 8, n)],
        [],
        (1,),
        block_inverse, e, faces,
    )
    power, ends, link = (setup[k * LEVELS : (k + 1) * LEVELS] for k in range(3))
    ends_up, basis, basis_up, table = setup[3 * LEVELS :]
    low, high, table = lax.optimization_barrier((*halo_y(right_side, 12), table))
    f0 = halo_x(jnp.concatenate([low, right_side, high], axis=1), 12)
    table = exchange(table)
    *om, om_up, m_matrix, m_link, mix, up_mix, w2_map = call(
        coupling_kernel,
        [(8, n)] * LEVELS + [(8, n), (n, n), (8, n), (11, n, n), (13, n, n), (8, n)],
        [(gz, 8, 8, n), (n, n)],
        (0, 2),
        where, table, e, faces, basis,
    )

    s0, s1, s2 = (sx, sy), (sx // 2, sy // 2), (sx // 4, sy // 4)
    ext0, ext1 = (sx + 24, sy + 24), (sx // 2 + 10, sy // 2 + 16)
    cube0, cube1 = ext0 + (n,), ext1 + (n,)
    lines0, lines1 = ext0[0] * ext0[1], ext1[0] * ext1[1]
    lanes = padded_lanes(lines0) + padded_lanes(lines1) + padded_lanes(s2[0] * s2[1])
    copies, f1_local, f2_local = call(
        part(local_down_kernel, s0, s1, grids),
        [(gz, 8, lanes), cube1, s2 + (n,)],
        [cube0] * 4 + [(ext1[0], ext0[1], n)] + [cube1] * 4 + [(s2[0], ext1[1], n)],
        (0,),
        where, f0, power[0], power[1], ends[0], ends[1], ends[2],
    )
    got = stacked(copies)
    many = gx * gy
    f1, own1, parts = call(
        part(joined_down_kernel, s0, s1, ext0, grids),
        [cube1, cube1, (many, s2[0] + 1, s2[1], n)],
        [cube0] * 3 + [(ext1[0], ext0[1], n)] + [cube1] * 4 + [(s2[0], ext1[1], n), s2 + (n,)],
        (0,),
        where, got, f1_local, f2_local, mix, om[2], w2_map,
    )
    parts = lax.all_to_all(parts, ("gx", "gy"), 0, 0, tiled=True)
    inner0 = (sx + 8, sy + 8, n)
    known0, twice0 = call(
        part(known_zero_kernel, s0, ext0, grids[0]),
        [s0 + (n,), s0 + (n,)],
        [inner0] * 8,
        (0, 1),
        where, e, f0, got, mix, power[0], link[0],
        flops=20000000000,
    )
    (known1,) = call(
        part(known_one_kernel, s1, grids[1]),
        [cube1],
        [cube1] * 6,
        (0, 1),
        where, e, f1, own1, power[1], link[1],
        flops=10000000000,
    )
    parts, known0, twice0, known1 = lax.optimization_barrier((parts, known0, twice0, known1))

    cubes = [g + (n,) for g in grids]
    lines = [g[0] * g[1] for g in grids]
    margin = s2[0]
    region = (3 * s2[0], 3 * s2[1], n)
    padded = (grids[2][0] + 2 * margin, grids[2][1] + 2 * margin, n)
    f3, copies = call(
        part(gathered_down_kernel, gx, gy),
        [cubes[3], (gz, 8, lines[3])],
        [cubes[2], (lines[2], n), (8, lines[2])] + [cubes[2]] * 4 + [(grids[3][0], grids[2][1], n)],
        (),
        parts, power[2], link[2], ends[3],
    )
    got3 = stacked(copies)
    (known2,) = call(
        part(known_two_kernel, gx, gy, grids[2]),
        [region],
        [(region[0] * region[1], n), (8, region[0] * region[1])] + [region] * 6,
        (0, 1),
        where, e, parts, power[2], link[2],
        flops=8000000000,
    )
    got3, known2 = lax.optimization_barrier((got3, known2))
    f4, copies = call(
        whole_down_kernel,
        [cubes[4], (gz, 8, lines[4])],
        [cubes[3]] * 4 + [(grids[4][0], grids[3][1], n)],
        (),
        f3, got3, om[3], power[3], link[3], ends[4],
    )
    got4 = stacked(copies)
    (known3,) = call(
        part(whole_known_kernel, 3),
        [cubes[3]],
        [cubes[3]] * 6,
        (0,),
        e, f3, got3, om[3], power[3], link[3],
        flops=8000000000,
    )
    got4, known3 = lax.optimization_barrier((got4, known3))

    copies, c1_local = call(
        part(local_up_kernel, s0, grids, margin),
        [(gz, 8, sum(UP_LANES)), cube1],
        [cubes[4]] * 3 + [cubes[3]] * 5 + [cubes[2], padded] + [region] * 5 + [cube1] * 4 + [inner0],
        (0, 1),
        where, e, f4, got4, om[4], power[4], link[4], known3, known2, known1,
        power[3], power[2], power[1], ends[3], ends[2], ends[1], ends_up,
    )
    u, r = call(
        part(finish_kernel, s0, grids, margin),
        [s0 + (n,), s0 + (n,)],
        [cubes[3]] * 3 + [cubes[2], padded] + [region] * 4 + [cube1] * 5 + [inner0] * 7,
        (0, 1),
        where, e, stacked(copies), c1_local, known0, twice0, up_mix, basis_up,
        power[0], link[0], m_matrix, m_link,
    )
    return u, r


def solution(mesh):
    return jax.shard_map(
        body,
        mesh=mesh,
        in_specs=(P("gx", "gy", "gz"), P("gz"), P(), P(None, "gz", None)),
        out_specs=(P("gx", "gy", "gz"), P("gx", "gy", "gz")),
        check_vma=False,
    )
```

```python
import functools

import jax
import jax.numpy as jnp
from jax import lax
from jax.experimental import pallas as pl
from jax.experimental.pallas import tpu as pltpu
from jax.sharding import PartitionSpec as P

LEVELS = 5
POWERS = 4
HIGHEST = lax.Precision.HIGHEST
F32 = jnp.float32
KNOWN = (0.9984, 0.9728, 0.8192, 0.4096)
TWICE = (0.0016, 0.0256, 0.1536, 0.4096, 0.4096)
VMEM_LIMIT = 56 * 1024 * 1024


def contract(a, b, da, db):
    return lax.dot_general(
        a, b, (((da,), (db,)), ((), ())), precision=HIGHEST, preferred_element_type=F32
    )


def exact_nn(a, b):
    return contract(a, b, 1, 0)


def exact_nt(a, b):
    return contract(a, b, 1, 1)


def exact_tn(a, b):
    return contract(a, b, 0, 0)


def halves(a):
    if isinstance(a, tuple):
        return a
    high = a.astype(jnp.bfloat16)
    return high, (a - high.astype(F32)).astype(jnp.bfloat16)


def product(a, b, da, db):
    (ah, al), (bh, bl) = halves(a), halves(b)

    def dot(x, y):
        return lax.dot_general(x, y, (((da,), (db,)), ((), ())), preferred_element_type=F32)

    return dot(ah, bh) + (dot(ah, bl) + dot(al, bh))


def nn(a, b):
    return product(a, b, 1, 0)


def nt(a, b):
    return product(a, b, 1, 1)


def tn(a, b):
    return product(a, b, 0, 0)


def rows(lo, hi, fn, step=8):
    full = (hi - lo) // step
    if full:
        def group(k, carry):
            for q in range(step):
                fn(lo + k * step + q)
            return carry

        lax.fori_loop(0, full, group, 0)
    for i in range(lo + full * step, hi):
        fn(i)


def sublane_index(length):
    return lax.broadcasted_iota(jnp.int32, (length, 128), 0)


def shifted(v, zero_ends):
    n = v.shape[0]
    low, high = pltpu.roll(v, 1, 0), pltpu.roll(v, n - 1, 0)
    if zero_ends:
        at = sublane_index(n)
        low = jnp.where(at > 0, low, 0.0)
        high = jnp.where(at < n - 1, high, 0.0)
    return low, high


class Window:
    def __init__(self, shape, origin=None, grid=None):
        self.x, self.y = shape
        self.whole = origin is None
        self.lo, self.hi = (0, self.y) if self.whole else (1, self.y - 1)
        if not self.whole:
            self.x0, y0 = origin
            self.nx, ny = grid
            at = sublane_index(self.y - 2) + (y0 + 1)
            self.in_y = jnp.where((at >= 0) & (at < ny), 1.0, 0.0).astype(F32)

    def get(self, ref, i):
        return ref[i, self.lo : self.hi]

    def put(self, ref, i, v):
        ref[i, self.lo : self.hi] = v

    def mask(self, i, v):
        if self.whole:
            return v
        at = self.x0 + i
        inside = jnp.where((at >= 0) & (at < self.nx), 1.0, 0.0).astype(F32)
        return v * (self.in_y * inside)

    def around(self, ref, i):
        if self.whole:
            low, high = shifted(ref[i], True)
            total = low + high
            if not (isinstance(i, int) and i == 0):
                total = total + ref[i - 1]
            if not (isinstance(i, int) and i == self.x - 1):
                total = total + ref[i + 1]
            return total
        y = self.y
        return (ref[i, 0 : y - 2] + ref[i, 2:y]) + (ref[i - 1, 1 : y - 1] + ref[i + 1, 1 : y - 1])

    def span(self, trim):
        return (0, self.x) if self.whole else (trim, self.x - trim)

    def loop(self, trim, fn):
        lo, hi = self.span(trim)
        if self.whole:
            fn(0)
            rows(lo + 1, hi - 1, fn)
            fn(hi - 1)
        else:
            rows(lo, hi, fn)

    def each(self, trim, out, fn):
        self.loop(trim, lambda i: self.put(out, i, fn(i)))


def line_powers(field, ends, power_ref, link_ref, count, out_refs, exact=False):
    if not exact:
        field, ends = halves(field), halves(ends)
    for j in range(count):
        if exact:
            value = exact_nt(field, power_ref[j]) + exact_tn(ends, link_ref[j])
        else:
            value = nt(field, power_ref[j]) + tn(ends, link_ref[j])
        out_refs[j][...] = value.reshape(out_refs[j].shape)


def smoothed_residual(win, field_ref, x1, x2, t, out, trim, masked=False, add=None):
    win.each(trim - 1, t, lambda i: 0.32 * win.get(x1, i) + win.mask(i, 0.64 * win.around(x2, i)))

    def outer(i):
        v = 0.04 * win.get(field_ref, i) + win.around(t, i)
        if add is not None:
            v = v + win.get(add, i)
        return win.mask(i, v) if masked else v

    win.each(trim, out, outer)


def horner(win, xs, weights, t0, t1, trim):
    src = xs[-1]
    scale = weights[-1]
    buffers = (t0, t1)
    for n, j in enumerate(range(len(xs) - 2, 0, -1)):
        dst = buffers[n % 2]

        def one(i, src=src, j=j, scale=scale):
            return weights[j] * win.get(xs[j], i) + win.mask(i, scale * win.around(src, i))

        win.each(trim - j, dst, one)
        src, scale = dst, 1.0
    return src, scale


def restrict(src, scratch, out, x_at, y_at):
    count_x, count_y = out.shape[0], out.shape[1]
    for i in range(count_x):
        scratch[i] = src[x_at + 2 * i] + src[x_at + 2 * i + 1]
    for i in range(count_x):
        even = scratch[i, pl.ds(y_at, count_y, stride=2), :]
        odd = scratch[i, pl.ds(y_at + 1, count_y, stride=2), :]
        out[i] = (even + odd) * 0.25


def prolong(src, src_whole, out, win, x_from, y_from, count_x, count_y):
    last = src.shape[0] - 1
    for i in range(count_x):
        at = x_from + i
        centre = src[at]
        below = src[at - 1] if at > 0 else jnp.zeros_like(centre)
        above = src[at + 1] if at < last else jnp.zeros_like(centre)
        for odd, other in ((0, below), (1, above)):
            v = 0.75 * centre + 0.25 * other
            low, high = shifted(v, src_whole)
            for parity, side in ((0, low), (1, high)):
                w = 0.75 * v + 0.25 * side
                out[2 * i + odd, pl.ds(parity, count_y, stride=2), :] = w[y_from : y_from + count_y]
    if not win.whole:
        win.each(0, out, lambda i: win.mask(i, win.get(out, i)))


def send(out_ref, value):
    for m in range(out_ref.shape[0]):
        out_ref[m] = value


def powers_kernel(g_ref, e_ref, zf_ref, *outs):
    levels, n = g_ref.shape[0], g_ref.shape[1]
    power_refs, ends_refs, link_refs = outs[0:levels], outs[levels : 2 * levels], outs[2 * levels : 3 * levels]
    up_ref, basis_ref, basis_up_ref, table_ref = outs[3 * levels :]
    table_ref[...] = jnp.zeros_like(table_ref)
    for level in range(levels):
        power_ref, ends_ref, link_ref = power_refs[level], ends_refs[level], link_refs[level]
        link_ref[...] = jnp.zeros_like(link_ref)
        e = e_ref[level]
        inverse_e = 1.0 / jnp.full((1, n), e, F32)
        one = g_ref[level] * e
        two = exact_nn(one, one)
        three = exact_nn(two, one)
        four = exact_nn(two, two)
        ends = []
        for j, value in enumerate((one, two, three, four)):
            power_ref[j] = value
            for s, row in enumerate((value[0:1], value[n - 1 : n])):
                ends_ref[2 * j + s : 2 * j + s + 1] = row
                table_ref[0, 2 * j + s, level : level + 1] = row
                ends.append(row)
        for j in range(POWERS):
            for i in range(j + 1):
                for t in range(2):
                    link_ref[j, 2 * i + t : 2 * i + t + 1] = ends[2 * (j - i) + t] * inverse_e
        table_ref[0, 9, level : level + 1] = inverse_e
    table_ref[0, 8] = jnp.broadcast_to(zf_ref[...], (8, n))
    def columns(level):
        return ends_refs[level][0:4] * (1.0 / jnp.full((4, n), e_ref[level], F32))

    zero = columns(0)
    basis_ref[0:4] = zero
    basis_ref[4:8] = exact_nn(zero, power_refs[1][0])
    basis_ref[8:12] = exact_nn(zero, power_refs[1][1])
    basis_ref[12:16] = columns(1)
    three = columns(3)
    two = [three, exact_nn(three, power_refs[2][0]), exact_nn(three, power_refs[2][1]), columns(2)]
    two = jnp.concatenate(two, 0)
    basis_up_ref[...] = jnp.zeros_like(basis_up_ref)
    basis_up_ref[0:16] = two
    basis_up_ref[16:32] = exact_nn(two, power_refs[1][0])
    basis_up_ref[32:48] = exact_nn(two, power_refs[1][1])
    basis_up_ref[48:52] = columns(1)
    at = lax.broadcasted_iota(jnp.int32, (1, n), 1)
    up_ref[...] = jnp.zeros_like(up_ref)
    up_ref[0:4] = ends_refs[0][0:4]
    up_ref[4:5] = jnp.where(at == 0, 1.0, 0.0).astype(F32)
    up_ref[5:6] = jnp.where(at == n - 1, 1.0, 0.0).astype(F32)


    full_basis = jnp.concatenate([basis_ref[...], jnp.zeros((n - 16, n), F32)], 0)
    at = lax.broadcasted_iota(jnp.int32, (8, n), 1)
    first = jnp.where(at < 4, exact_nt(ends_refs[1][...], full_basis), 0.0)
    second = exact_nt(ends_refs[2][...], full_basis)
    shifted_ends = jnp.concatenate([jnp.zeros((4, n), F32), ends_refs[2][0:4]], 0)
    third = jnp.where(at < 4, exact_nt(shifted_ends, basis_up_ref[...]), 0.0)
    fourth = jnp.where(at < 16, exact_nt(ends_refs[1][...], basis_up_ref[...]), 0.0)
    fifth = exact_nt(up_ref[...], basis_up_ref[...])
    total = first + pltpu.roll(second, 4, 1) + pltpu.roll(third, 20, 1)
    sixth = jnp.where(at < 4, exact_nt(ends_refs[4][...], basis_up_ref[...]), 0.0)
    total = total + pltpu.roll(fourth, 24, 1) + pltpu.roll(fifth, 40, 1)
    table_ref[0, 10] = total + pltpu.roll(sixth, 92, 1)
    for m in range(1, table_ref.shape[0]):
        table_ref[m] = table_ref[0]


def coupling_kernel(
    where_ref, table_ref, e_ref, zf_ref, basis_ref, basis_up_ref, om0, om1, om2, om3, om4, om_up_ref, m_ref, m_link_ref, mix_ref, up_mix_ref, w2_ref, w4_ref, held, full
):
    blocks, n = table_ref.shape[0], table_ref.shape[3]
    k_own = where_ref[2]
    wide = (8, n)
    lane = lax.broadcasted_iota(jnp.int32, wide, 1)
    inverse_e = table_ref[0, 9]

    def entry(m, row, column):
        at = 0 if column == 0 else n - 1
        return jnp.broadcast_to(table_ref[m, row][:, at : at + 1], wide)

    corner = [
        [
            [[entry(m, 2 * i + s, t) * inverse_e for t in range(2)] for s in range(2)]
            for m in range(blocks)
        ]
        for i in range(POWERS)
    ]
    face = [entry(m, 8, 0) for m in range(blocks)]

    gain_v, gain_d, gain_p, gain_g = [corner[0][0][1][1]], [None], [None], [None]
    for k in range(1, blocks):
        (a, b), (c, d) = corner[0][k]
        g = face[k]
        gv = g * g * gain_v[k - 1]
        dk = 1.0 / (1.0 - a * gv)
        gain_d.append(dk)
        gain_p.append(dk * b)
        gain_g.append(gv)
        gain_v.append(d + c * gv * gain_p[k])

    def solve(low, high):
        u, pu = [high[0]], [None]
        for k in range(1, blocks):
            (a, b), (c, d) = corner[0][k]
            gu = face[k] * u[k - 1]
            pu.append(gain_d[k] * (low[k] + a * gu))
            u.append(high[k] + c * (gu + gain_g[k] * pu[k]))
        zero = jnp.zeros(wide, F32)
        alpha, beta = [zero] * blocks, [zero] * blocks
        for k in range(blocks - 1, 0, -1):
            p = pu[k] + gain_p[k] * beta[k]
            beta[k - 1] = face[k] * p
            alpha[k] = face[k] * (u[k - 1] + gain_v[k - 1] * beta[k - 1])
        return alpha, beta

    unit = [
        [jnp.where(lane == 8 * m + s, 1.0, 0.0).astype(F32) for m in range(blocks)] for s in range(2)
    ]
    response = [solve(unit[0], unit[1])]
    for i in range(1, POWERS):
        source = [[None] * blocks, [None] * blocks]
        for m in range(blocks):
            for s in range(2):
                total = None
                for q in range(i):
                    c = corner[i - q][m][s]
                    term = c[0] * response[q][0][m] + c[1] * response[q][1][m]
                    total = term if total is None else total + term
                source[s][m] = total
        response.append(solve(source[0], source[1]))
    for i in range(POWERS):
        for t in range(2):
            for m in range(blocks):
                held[m, 2 * i + t] = response[i][t][m]
    om_refs = (om0, om1, om2, om3, om4)
    for i in range(POWERS):
        for t in range(2):
            total = held[k_own, 2 * i + t]
            for j in range(1, i + 1):
                total = total + pltpu.roll(held[k_own, 2 * (i - j) + t], 2 * j, 1)
            for level in range(LEVELS):
                om_refs[level][2 * i + t : 2 * i + t + 1] = total[level : level + 1]
    om_up_ref[...] = om0[...]

    lane = lane[0:1]
    om_up_ref[4:5] = jnp.where((lane == 8 * (k_own - 1) + 5) & (k_own > 0), 1.0, 0.0).astype(F32)
    om_up_ref[5:6] = jnp.where((lane == 8 * (k_own + 1) + 4) & (k_own < blocks - 1), 1.0, 0.0).astype(F32)
    om_up_ref[6:8] = jnp.zeros((2, n), F32)

    row = lax.broadcasted_iota(jnp.int32, (n, n), 0)
    column = lax.broadcasted_iota(jnp.int32, (n, n), 1)

    def every(i, t, m, offset):
        total = held[m, 2 * i + t]
        if i == 1:
            total = total + pltpu.roll(held[m, t], 2, 1)
        return pltpu.roll(total, offset, 1) if offset else total

    def matrix(level, groups, own=None, offset=0):
        full[...] = jnp.zeros_like(full)
        for start, i, scale in groups:
            for m in range(blocks):
                for t in range(2):
                    at = start + 2 * m + t
                    full[at : at + 1] = scale * every(i, t, m, offset)[level : level + 1]
        if own is not None:
            full[own : own + 8] = om_refs[level][...]
        return full[...].T

    def gathered(offset, count):
        tiles = jnp.concatenate([table_ref[m, 10] for m in range(blocks)], 0)
        at = row - offset
        place = (at >= 0) & (at < count) & (at == (column >> 4) * 2 + (column & 1))
        value = exact_nn(tiles, jnp.where(place, 1.0, 0.0).astype(F32))
        high = 8 * blocks
        value = jnp.where((row[0:high] >> 3) == ((column[0:high] >> 1) & 7), value, 0.0)
        return jnp.concatenate([value, jnp.zeros((n - high, n), F32)], 0)

    def diagonal(shift, scale):
        return jnp.where((row < 32) & (column == row + shift), scale, 0.0).astype(F32)

    def rest(slot_ref, base, level, once, twice, table):
        slot_ref[base] = once
        slot_ref[base + 1] = twice
        slot_ref[base + 2] = diagonal(0, 0.04)
        slot_ref[base + 3] = exact_nn(table, once) + diagonal(32, 0.32)
        slot_ref[base + 4] = exact_nn(table, twice) + diagonal(64, 0.64)

    mix_ref[0] = matrix(0, [(0, 0, 0.32)], 64)
    mix_ref[1] = matrix(0, [(0, 1, 0.64), (16, 0, 0.64)])
    one = gathered(0, 4).T
    rest(mix_ref, 2, 1, matrix(1, [(96, 0, 0.32)]), matrix(1, [(96, 1, 0.64), (112, 0, 0.64)]), one)
    mix_ref[7] = matrix(1, [], 0)
    mix_ref[8] = exact_nn(one, mix_ref[7])
    w2_ref[...] = exact_nn(om2[...], gathered(4, 16))
    basis = jnp.concatenate([basis_ref[...], jnp.zeros((n - 16, n), F32)], 0)
    own_rows = jnp.where(
        (row < 16) & (column == (row >> 1) * 16 + 2 * k_own + (row & 1)), 1.0, 0.0
    ).astype(F32)
    chosen = exact_tn(own_rows, basis)
    mix_ref[9] = jnp.where(row < 32, chosen, 0.0)
    mix_ref[10] = chosen

    up_mix_ref[0] = matrix(3, [(0, 0, 0.32)])
    up_mix_ref[1] = matrix(3, [(0, 1, 0.64), (16, 0, 0.64)])
    once = matrix(2, [(96, 0, 0.32)], offset=4)
    twice = matrix(2, [(96, 1, 0.64), (112, 0, 0.64)], offset=4)
    rest(up_mix_ref, 2, 2, once, twice, gathered(20, 4).T)
    both = matrix(1, [(0, 0, 1.0), (16, 1, 1.0)])
    through = exact_nn(gathered(24, 16).T, both)
    up_rows = om_up_ref[...]
    for k, scale in enumerate((0.04, 0.32, 0.64)):
        full[...] = jnp.zeros_like(full)
        full[16 * k : 16 * k + 16] = scale * own_rows[0:16]
        full[64:72] = scale * exact_nn(up_rows, gathered(40 + 16 * k, 16))
        up_mix_ref[7 + k] = full[...].T
    last = exact_nn(up_rows, gathered(88, 4))
    wide_lane = lax.broadcasted_iota(jnp.int32, (8, n), 1)
    full[...] = jnp.zeros_like(full)
    for t in range(2):
        full[48 + t : 49 + t] = jnp.where(lane == 2 * k_own + t, 0.32, 0.0).astype(F32)
    full[64:72] = jnp.where(wide_lane < 16, 0.32 * last, 0.0)
    mixed = full[...].T
    up_mix_ref[8] = up_mix_ref[8] + exact_nn(through, mixed)
    up_mix_ref[10] = exact_nn(both, mixed)
    full[...] = jnp.zeros_like(full)
    for t in range(2):
        full[48 + t : 49 + t] = jnp.where(lane == 16 + 2 * k_own + t, 0.64, 0.0).astype(F32)
        full[50 + t : 51 + t] = jnp.where(lane == 2 * k_own + t, 0.64, 0.0).astype(F32)
    swapped = jnp.where(
        wide_lane < 16,
        pltpu.roll(last, n - 16, 1),
        jnp.where(wide_lane < 32, pltpu.roll(last, 16, 1), 0.0),
    )
    full[64:72] = 0.64 * swapped
    mixed = full[...].T
    up_mix_ref[9] = up_mix_ref[9] + exact_nn(through, mixed)
    up_mix_ref[11] = exact_nn(both, mixed)
    full[...] = jnp.zeros_like(full)
    full[64:72] = up_rows
    up_mix_ref[12] = full[...].T
    up_mix_ref[13] = jnp.where(row < 32, exact_tn(own_rows, basis_up_ref[...]), 0.0)
    w4_ref[...] = exact_nn(om4[...], gathered(92, 4))
    for q in range(POWERS):
        full[...] = jnp.zeros_like(full)
        for b in range(q + 1):
            full[2 * b : 2 * b + 2] = KNOWN[q] * om3[2 * (q - b) : 2 * (q - b) + 2]
        up_mix_ref[14 + q] = full[...].T

    above = jnp.minimum(k_own + 1, blocks - 1)
    top = table_ref[above, 8][0:1, 0:1]
    top = jnp.where(jnp.full((1, 1), k_own, jnp.int32) < blocks - 1, top, 1.0)
    down = zf_ref[...]
    up = jnp.where(lane == n - 1, jnp.broadcast_to(top, (1, n)), pltpu.roll(down, n - 1, 1))
    down_all, up_all = jnp.broadcast_to(down, (n, n)), jnp.broadcast_to(up, (n, n))
    m_ref[...] = jnp.where(
        row == column,
        down_all + up_all + 4.0 * e_ref[0],
        jnp.where(row == column - 1, -down_all, jnp.where(row == column + 1, -up_all, 0.0)),
    )
    m_link_ref[...] = jnp.zeros_like(m_link_ref)
    m_link_ref[4:5] = jnp.where(lane == 0, -down, 0.0)
    m_link_ref[5:6] = jnp.where(lane == n - 1, -up, 0.0)


def flat(ref):
    return ref[...].reshape(ref.shape[0] * ref.shape[1], ref.shape[2])


def ends_from(om_ref, got_ref):
    return exact_nn(om_ref[:, : got_ref.shape[0]], got_ref[...])


def restrict_into(src, scratch, out, x_at, y_at, count_y, y_to):
    for i in range(out.shape[0]):
        scratch[i] = src[x_at + 2 * i] + src[x_at + 2 * i + 1]
    for i in range(out.shape[0]):
        even = scratch[i, pl.ds(y_at, count_y, stride=2), :]
        odd = scratch[i, pl.ds(y_at + 1, count_y, stride=2), :]
        out[i, y_to : y_to + count_y] = (even + odd) * 0.25


def padded_lanes(count):
    return (count + 127) // 128 * 128


def windows(where_ref, s0, s1, ext0, ext1, grids):
    h0 = tuple((a - b) // 2 for a, b in zip(ext0, s0))
    h1 = tuple((a - b) // 2 for a, b in zip(ext1, s1))
    ix, iy = where_ref[0], where_ref[1]
    win0 = Window(ext0, (ix * s0[0] - h0[0], iy * s0[1] - h0[1]), grids[0])
    win1 = Window(ext1, (ix * s1[0] - h1[0], iy * s1[1] - h1[1]), grids[1])
    return win0, win1, h0, h1


def local_down_kernel(
    s0, s1, grids, where_ref, f_ref, power0, power1, v0, v1, v2, out_ref, f1_ref, f2_ref,
    x1, x2, t, r, pair, y1, y2, t1, r1, pair1
):
    ext0, ext1 = f_ref.shape[:2], f1_ref.shape[:2]
    win0, win1, h0, h1 = windows(where_ref, s0, s1, ext0, ext1, grids)
    field = halves(flat(f_ref))
    lanes0 = ext0[0] * ext0[1]
    lanes1 = ext1[0] * ext1[1]
    at1 = padded_lanes(lanes0)
    at2 = at1 + padded_lanes(lanes1)
    many = out_ref.shape[0]
    out_ref[0, :, at1 - 128 : at1] = jnp.zeros((8, 128), F32)
    out_ref[0, :, at2 - 128 : at2] = jnp.zeros((8, 128), F32)
    out_ref[0, :, at2 : at2 + 128] = jnp.zeros((8, 128), F32)
    out_ref[0, :, 0:lanes0] = nt(v0[...], field)
    x1[...] = nt(field, power0[0]).reshape(x1.shape)
    x2[...] = nt(field, power0[1]).reshape(x2.shape)
    smoothed_residual(win0, f_ref, x1, x2, t, r, 2, masked=True)
    f1_ref[...] = jnp.zeros_like(f1_ref)
    count = (ext0[1] - 4) // 2
    restrict_into(r, pair, f1_ref, 2, 2, count, (ext1[1] - count) // 2)
    field = halves(flat(f1_ref))
    out_ref[0, :, at1 : at1 + lanes1] = nt(v1[...], field)
    y1[...] = nt(field, power1[0]).reshape(y1.shape)
    y2[...] = nt(field, power1[1]).reshape(y2.shape)
    smoothed_residual(win1, f1_ref, y1, y2, t1, r1, h1[0])
    restrict(r1, pair1, f2_ref, h1[0], h1[1])
    lines2 = f2_ref.shape[0] * f2_ref.shape[1]
    out_ref[0, :, at2 : at2 + lines2] = nt(v2[...], flat(f2_ref))
    for m in range(1, many):
        out_ref[m] = out_ref[0]


def joined_down_kernel(
    s0, s1, ext0, grids, where_ref, got_ref, f1_local, f2_local, mix_ref, om2_ref, w2_ref,
    f1_ref, own1_ref, parts_ref, d1, d2, f, pair, y, h1s, h2s, f2s, pair1, z
):
    ext1 = f1_local.shape[:2]
    win0, win1, h0, h1 = windows(where_ref, s0, s1, ext0, ext1, grids)
    lanes0 = ext0[0] * ext0[1]
    lanes1 = ext1[0] * ext1[1]
    at1 = padded_lanes(lanes0)
    at2 = at1 + padded_lanes(lanes1)
    got0 = halves(got_ref[:, 0:lanes0])
    rows_in = got_ref.shape[0]
    d1[...] = tn(got0, mix_ref[0, 0:rows_in]).reshape(d1.shape)
    d2[...] = tn(got0, mix_ref[1, 0:rows_in]).reshape(d2.shape)

    win0.each(1, d1, lambda i: win0.get(d1, i) + win0.mask(i, win0.around(d2, i)))
    win0.each(2, f, lambda i: win0.mask(i, win0.around(d1, i)))
    y[...] = jnp.zeros_like(y)
    count = (ext0[1] - 4) // 2
    restrict_into(f, pair, y, 2, 2, count, (ext1[1] - count) // 2)
    yf = halves(flat(y))
    f1_ref[...] = f1_local[...] + nn(yf, mix_ref[9]).reshape(f1_ref.shape)
    got1 = halves(got_ref[:, at1 : at1 + lanes1])
    own1_ref[...] = (tn(got1, mix_ref[7, 0:rows_in]) + nn(yf, mix_ref[8])).reshape(own1_ref.shape)
    h1s[...] = (tn(got1, mix_ref[2, 0:rows_in]) + nn(yf, mix_ref[5])).reshape(h1s.shape)
    h2s[...] = (tn(got1, mix_ref[3, 0:rows_in]) + nn(yf, mix_ref[6])).reshape(h2s.shape)
    f2s[...] = nn(yf, mix_ref[4]).reshape(f2s.shape)
    trim = h1[0]
    win1.each(trim - 1, h1s, lambda i: win1.get(h1s, i) + win1.mask(i, win1.around(h2s, i)))
    win1.each(trim, f2s, lambda i: win1.get(f2s, i) + win1.around(h1s, i))
    restrict(f2s, pair1, z, h1[0], h1[1])
    zf = flat(z)
    lines2 = zf.shape[0]
    side = z.shape[0]
    parts_ref[0, 0:side] = f2_local[...] + nn(zf, mix_ref[10]).reshape(z.shape)
    own2 = nn(om2_ref[:, 0:rows_in], got_ref[:, at2 : at2 + lines2]) + nt(w2_ref[...], zf)
    parts_ref[0, side] = jnp.zeros((8, 128), F32)
    parts_ref[0, side, :, 0:lines2] = own2
    for m in range(1, parts_ref.shape[0]):
        parts_ref[m] = parts_ref[0]


def lane_powers(field, coefficients, lane0, power_ref, link_ref, count, out_refs, exact=False):
    n = field.shape[1]
    if not exact:
        field, coefficients = halves(field), halves(coefficients)
    one, two = (exact_nt, exact_nn) if exact else (nt, nn)
    for j in range(count):
        pieces = [link_ref[j], jnp.zeros((n - 8 - lane0, n), F32)]
        if lane0:
            pieces = [jnp.zeros((lane0, n), F32)] + pieces
        value = one(field, power_ref[j]) + two(coefficients, jnp.concatenate(pieces, 0))
        out_refs[j][...] = value.reshape(out_refs[j].shape)


def known_zero_kernel(
    s0, ext0, grid, where_ref, e_ref, f_ref, got_ref, mix_ref, power_ref, link_ref,
    known_out, twice_out, own, f, x1, x2, x3, x4, t0, t1
):
    hx, hy = (f.shape[0] - s0[0]) // 2, (f.shape[1] - s0[1]) // 2
    cx, cy = (ext0[0] - f.shape[0]) // 2, (ext0[1] - f.shape[1]) // 2
    win = Window(f.shape[:2], (where_ref[0] * s0[0] - hx, where_ref[1] * s0[1] - hy), grid)
    coefficients = tn(got_ref[:, 0 : ext0[0] * ext0[1]], mix_ref[0, 0 : got_ref.shape[0]])
    own[...] = coefficients.reshape(ext0 + (128,))[cx : cx + f.shape[0], cy : cy + f.shape[1]]
    f[...] = f_ref[cx : cx + f.shape[0], cy : cy + f.shape[1]]
    xs = (x1, x2, x3, x4)
    lane_powers(flat(f), flat(own), 64, power_ref, link_ref, POWERS, xs)
    inverse_e = 1.0 / jnp.full((win.hi - win.lo, 128), e_ref[0], F32)
    at = hy - win.lo
    src, scale = horner(win, xs, KNOWN, t0, t1, hx)
    lo, hi = win.span(hx)

    def known(i):
        v = (KNOWN[0] * win.get(x1, i) + scale * win.around(src, i)) * inverse_e
        known_out[i - hx] = v[at : at + s0[1]]

    rows(lo, hi, known)
    src2, scale2 = horner(win, (f,) + xs, TWICE, t0, t1, hx)

    def again(i):
        v = TWICE[0] * win.get(f, i) + scale2 * win.around(src2, i)
        twice_out[i - hx] = v[at : at + s0[1]]

    rows(lo, hi, again)


def known_one_kernel(
    s1, grid, where_ref, e_ref, f_ref, own_ref, power_ref, link_ref, known_out, x1, x2, x3, x4, t0, t1
):
    hx, hy = (f_ref.shape[0] - s1[0]) // 2, (f_ref.shape[1] - s1[1]) // 2
    win = Window(f_ref.shape[:2], (where_ref[0] * s1[0] - hx, where_ref[1] * s1[1] - hy), grid)
    xs = (x1, x2, x3, x4)
    lane_powers(flat(f_ref), flat(own_ref), 0, power_ref, link_ref, POWERS, xs, exact=True)
    inverse_e = 1.0 / jnp.full((win.hi - win.lo, 128), e_ref[1], F32)
    src, scale = horner(win, xs, KNOWN, t0, t1, 3)
    known_out[...] = jnp.zeros_like(known_out)

    def known(i):
        return win.mask(i, (KNOWN[0] * win.get(x1, i) + scale * win.around(src, i)) * inverse_e)

    win.each(3, known_out, known)


def known_two_kernel(
    across, down, grid, where_ref, e_ref, parts_ref, power_ref, link_ref, known_out,
    fp, ap, x1, x2, x3, x4, t0, t1
):
    side = parts_ref.shape[2]
    lines = side * side
    ix, iy = where_ref[0], where_ref[1]
    for p in range(9):
        jx, jy = ix + p // 3 - 1, iy + p % 3 - 1
        inside = (jx >= 0) & (jx < across) & (jy >= 0) & (jy < down)
        at = jnp.clip(jx, 0, across - 1) * down + jnp.clip(jy, 0, down - 1)
        scale = jnp.where(inside, 1.0, 0.0).astype(F32)
        fp[p * lines : (p + 1) * lines] = (parts_ref[at, 0:side] * scale).reshape(lines, 128)
        ap[:, p * lines : (p + 1) * lines] = (parts_ref[at, side] * scale)[:, 0:lines]
    xs = (x1, x2, x3, x4)
    for j in range(POWERS):
        value = exact_nt(fp[...], power_ref[j]) + exact_tn(ap[...], link_ref[j])
        for p in range(9):
            px, py = p // 3 * side, p % 3 * side
            piece = value[p * lines : (p + 1) * lines].reshape(side, side, 128)
            xs[j][px : px + side, py : py + side] = piece
    win = Window(x1.shape[:2], ((ix - 1) * side, (iy - 1) * side), grid)
    inverse_e = 1.0 / jnp.full((win.hi - win.lo, 128), e_ref[2], F32)
    src, scale = horner(win, xs, KNOWN, t0, t1, 3)
    known_out[...] = jnp.zeros_like(known_out)

    def known(i):
        return win.mask(i, (KNOWN[0] * win.get(x1, i) + scale * win.around(src, i)) * inverse_e)

    win.each(3, known_out, known)


def gathered_down_kernel(
    across, down, parts_ref, power_ref, link_ref, power3, v3, v4, coarse_ref, lower_ref, out_ref,
    f, fp, ap, x1, x2, t, r, pair, y1, y2, ty, ry, pair3
):
    many, side = parts_ref.shape[0], parts_ref.shape[2]
    lines = side * side
    for p in range(many):
        px, py = p // down * side, p % down * side
        part = parts_ref[p, 0:side]
        f[px : px + side, py : py + side] = part
        fp[p * lines : (p + 1) * lines] = part.reshape(lines, 128)
        ap[:, p * lines : (p + 1) * lines] = parts_ref[p, side][:, 0:lines]
    fields, coefficients = halves(fp[...]), halves(ap[...])
    for j, x in enumerate((x1, x2)):
        value = nt(fields, power_ref[j]) + tn(coefficients, link_ref[j])
        for p in range(many):
            px, py = p // down * side, p % down * side
            x[px : px + side, py : py + side] = value[p * lines : (p + 1) * lines].reshape(side, side, 128)
    win = Window(f.shape[:2])
    smoothed_residual(win, f, x1, x2, t, r, 2)
    restrict(r, pair, coarse_ref, 0, 0)
    field = halves(flat(coarse_ref))
    lanes = field[0].shape[0]
    out_ref[0, :, 0:lanes] = nt(v3[...], field)
    y1[...] = nt(field, power3[0]).reshape(y1.shape)
    y2[...] = nt(field, power3[1]).reshape(y2.shape)
    smoothed_residual(Window(y1.shape[:2]), coarse_ref, y1, y2, ty, ry, 2)
    restrict(ry, pair3, lower_ref, 0, 0)
    value = nt(v4[...], flat(lower_ref))
    out_ref[0, :, lanes : lanes + value.shape[1]] = value
    for m in range(1, out_ref.shape[0]):
        out_ref[m] = out_ref[0]


def local_known_kernel(level, e_ref, f_ref, power_ref, known_ref, x1, x2, x3, x4, t0, t1):
    win = Window(f_ref.shape[:2])
    xs = (x1, x2, x3, x4)
    for j in range(POWERS):
        xs[j][...] = exact_nt(flat(f_ref), power_ref[j]).reshape(x1.shape)
    inverse_e = 1.0 / jnp.full((f_ref.shape[1], 128), e_ref[level], F32)
    src, scale = horner(win, xs, KNOWN, t0, t1, 4)

    def known(i):
        known_ref[i] = (KNOWN[0] * x1[i] + scale * win.around(src, i)) * inverse_e

    win.loop(0, known)


def clear_edges(pad, margin):
    x, y = pad.shape[:2]
    zero_rows = jnp.zeros((margin, y, 128), F32)
    zero_cols = jnp.zeros((x, margin, 128), F32)
    pad[0:margin] = zero_rows
    pad[x - margin : x] = zero_rows
    pad[:, 0:margin] = zero_cols
    pad[:, y - margin : y] = zero_cols


def cut(where_ref, pad, out_ref, margin):
    sx, sy = out_ref.shape[0] - 2 * margin, out_ref.shape[1] - 2 * margin
    x_at = where_ref[0] * sx
    y_at = pl.multiple_of(where_ref[1] * sy, 8)

    def one(i):
        out_ref[i] = pad[x_at + i, pl.ds(y_at, out_ref.shape[1]), :]

    rows(0, out_ref.shape[0], one)


UP_LANES = (896, 896, 512)


def place_on_region(where_ref, fine, pad, out_ref, margin):
    clear_edges(pad, margin)

    def place(i):
        pad[i + margin, margin : margin + fine.shape[1]] = fine[i]

    rows(0, fine.shape[0], place)
    cut(where_ref, pad, out_ref, margin)


def up_windows(where_ref, s0, grids, region, ext1, ext0):
    s1, s2 = (s0[0] // 2, s0[1] // 2), (s0[0] // 4, s0[1] // 4)
    wins = []
    for level, (shape, s) in enumerate(((ext0, s0), (ext1, s1), (region, s2))):
        hx, hy = (shape[0] - s[0]) // 2, (shape[1] - s[1]) // 2
        wins.append(Window(shape, (where_ref[0] * s[0] - hx, where_ref[1] * s[1] - hy), grids[level]))
    return wins


def to_level_one(src, out, win):
    prolong_odd(src, out, win, 5, 4, (out.shape[0] + 2) // 2, out.shape[1] // 2)


def to_level_zero(src, out, win):
    prolong(src, False, out, win, 3, 6, out.shape[0] // 2, out.shape[1] // 2)


def local_up_kernel(
    s0, grids, margin, where_ref, e_ref, f4_local, got_ref, om_ref, w4_ref, mix_ref, power4, link4,
    known3_local, known2, known1, power3, power2, power1, v3, v2, v1, v0, out_ref, c1_ref,
    d1, d2, d3, pair, y4, f4, known3, b1, b2, c4, w3, p1, p2, pt, c3, fine, pad, w2, q1, q2, qt, c2, w1, r1, r2, rt
):
    k = got_ref.shape[0]
    win3 = Window(d1.shape[:2])
    lanes = win3.x * win3.y
    got3 = halves(got_ref[:, 0:lanes])
    d1[...] = tn(got3, mix_ref[0, 0:k]).reshape(d1.shape)
    d2[...] = tn(got3, mix_ref[1, 0:k]).reshape(d2.shape)
    win3.each(0, d1, lambda i: win3.get(d1, i) + win3.around(d2, i))
    win3.each(0, d3, lambda i: win3.around(d1, i))
    restrict(d3, pair, y4, 0, 0)
    f4[...] = f4_local[...] + exact_nn(flat(y4), mix_ref[13]).reshape(f4.shape)
    ends = exact_nn(om_ref[:, 0:k], got_ref[:, lanes : lanes + y4.shape[0] * y4.shape[1]])
    ends = ends + exact_nt(w4_ref[...], flat(y4))

    src, buffers = d1, (d2, d3)
    d1[...] = tn(got3, mix_ref[17, 0:k]).reshape(d1.shape)
    for n, q in enumerate((2, 1, 0)):
        dst = buffers[n % 2] if n < 2 else d1
        dst[...] = tn(got3, mix_ref[14 + q, 0:k]).reshape(d1.shape)
        win3.each(0, dst, lambda i, src=src, dst=dst: win3.get(dst, i) + win3.around(src, i))
        src = dst
    inverse_e = 1.0 / jnp.full((8, 128), e_ref[3], F32)
    bases = v3[...] * inverse_e
    bases = jnp.concatenate([bases * inverse_e, jnp.zeros((120, 128), F32)], 0)
    known3[...] = known3_local[...] + exact_nn(flat(src), bases).reshape(known3.shape)

    win = Window(f4.shape[:2])
    line_powers(flat(f4), ends, power4, link4, 2, (b1, b2), exact=True)
    inverse_e = 1.0 / jnp.full((f4.shape[1], 128), e_ref[LEVELS - 1], F32)

    def one(i):
        c4[i] = (0.96 * b1[i] + 0.64 * win.around(b2, i)) * inverse_e

    win.loop(0, one)
    prolong(c4, True, w3, win3, 0, 0, win.x, win.y)
    _, win1, win2 = up_windows(where_ref, s0, grids, w2.shape[:2], w1.shape[:2], w1.shape[:2])
    at1, at2 = UP_LANES[0], UP_LANES[0] + UP_LANES[1]
    out_ref[0] = jnp.zeros(out_ref.shape[1:], F32)

    def local(win, w, known, power, x1, x2, t, c):
        field = halves(flat(w))
        x1[...] = nt(field, power[0]).reshape(x1.shape)
        x2[...] = nt(field, power[1]).reshape(x2.shape)
        c[...] = jnp.zeros_like(c)
        smoothed_residual(win, w, x1, x2, t, c, 2, masked=True, add=known)

    def words(v_ref, w, first_row, at):
        value = exact_nt(v_ref[...], flat(w))
        out_ref[0, first_row : first_row + 4, at : at + value.shape[1]] = value[0:4]

    words(v3, w3, 0, at2)
    local(win3, w3, known3, power3, p1, p2, pt, c3)
    prolong(c3, True, fine, Window(fine.shape[:2]), 0, 0, win3.x, win3.y)
    place_on_region(where_ref, fine, pad, w2, margin)
    words(v2, w2, 4, at1)
    local(win2, w2, known2, power2, q1, q2, qt, c2)
    to_level_one(c2, w1, win1)
    words(v1, w1, 0, at1)
    local(win1, w1, known1, power1, r1, r2, rt, c1_ref)
    value = exact_nt(v0[...], flat(c1_ref))
    out_ref[0, :, 0 : value.shape[1]] = value
    for m in range(1, out_ref.shape[0]):
        out_ref[m] = out_ref[0]


def finish_kernel(
    s0, grids, margin, where_ref, e_ref, got_ref, c1_local, known_ref, twice_ref, mix_ref, basis_ref,
    power_ref, link_ref, m_ref, m_link_ref, u_ref, r_ref,
    d1, d2, d3, fine, pad, y2, g1, g2, g3, y1, h1, h2, h3, c1, w, q, x1, x2, xm, t0, t1
):
    win0, win1, win2 = up_windows(where_ref, s0, grids, y2.shape[:2], y1.shape[:2], w.shape[:2])
    lines1 = y1.shape[0] * y1.shape[1]
    lines2, lines3 = y2.shape[0] * y2.shape[1], d1.shape[0] * d1.shape[1]
    at1, at2 = UP_LANES[0], UP_LANES[0] + UP_LANES[1]
    k = got_ref.shape[0]

    got3 = halves(got_ref[:, at2 : at2 + lines3])
    d1[...] = tn(got3, mix_ref[0, 0:k]).reshape(d1.shape)
    d2[...] = tn(got3, mix_ref[1, 0:k]).reshape(d2.shape)
    win3 = Window(d1.shape[:2])
    win3.each(0, d1, lambda i: win3.get(d1, i) + win3.around(d2, i))
    win3.each(0, d3, lambda i: win3.around(d1, i))
    prolong(d3, True, fine, Window(fine.shape[:2]), 0, 0, win3.x, win3.y)
    place_on_region(where_ref, fine, pad, y2, margin)

    def coefficients(win, got, y, once, twice, maps, a1, a2, a3, trim):
        y, got = halves(flat(y)), halves(got)
        a1[...] = (tn(got, once[0:k]) + nn(y, maps[1])).reshape(a1.shape)
        a2[...] = (tn(got, twice[0:k]) + nn(y, maps[2])).reshape(a2.shape)
        a3[...] = nn(y, maps[0]).reshape(a3.shape)
        win.each(trim - 1, a1, lambda i: win.get(a1, i) + win.mask(i, win.around(a2, i)))
        win.each(trim, a3, lambda i: win.mask(i, win.get(a3, i) + win.around(a1, i)))

    maps = (mix_ref[4], mix_ref[5], mix_ref[6])
    got2 = got_ref[:, at1 : at1 + lines2]
    coefficients(win2, got2, y2, mix_ref[2], mix_ref[3], maps, g1, g2, g3, 2)
    to_level_one(g3, y1, win1)
    maps = (mix_ref[7], mix_ref[8], mix_ref[9])
    got1 = got_ref[:, at1 : at1 + lines1]
    coefficients(win1, got1, y1, mix_ref[10], mix_ref[11], maps, h1, h2, h3, 2)
    c1[...] = c1_local[...] + exact_nn(flat(h3), basis_ref[...]).reshape(c1.shape)
    h3[...] = h3[...] + tn(got_ref[:, 0:lines1], mix_ref[12, 0:k]).reshape(h3.shape)
    to_level_zero(c1, w, win0)
    to_level_zero(h3, q, win0)

    hx, hy = (w.shape[0] - s0[0]) // 2, (w.shape[1] - s0[1]) // 2
    sy = s0[1]
    win = win0
    field, ends = flat(w), flat(q)
    lane_powers(field, ends, 64, power_ref, link_ref, 2, (x1, x2))
    n = field.shape[1]
    m_link = jnp.concatenate([jnp.zeros((64, n), F32), m_link_ref[...], jnp.zeros((n - 72, n), F32)], 0)
    xm[...] = (exact_nt(field, m_ref[...]) + exact_nn(ends, m_link)).reshape(xm.shape)
    e = e_ref[0]
    w_ref = w

    lo, hi = win.span(hx - 2)

    def inner(i):
        one = 0.32 * win.get(x1, i)
        two = win.mask(i, 0.64 * win.around(x2, i))
        win.put(t0, i, one + two)
        win.put(t1, i, e * (one - two))

    rows(lo, hi, inner)
    win.each(hx - 1, x2, lambda i: (0.28 * e) * win.get(w_ref, i) + win.mask(i, win.around(t1, i)))
    lo, hi = win.span(hx)
    cut_y = hy - win.lo

    def last(i):
        u = 0.04 * win.get(w_ref, i) + win.around(t0, i)
        u_ref[i - hx] = known_ref[i - hx] + u[cut_y : cut_y + sy]
        r = 0.04 * win.get(xm, i) + win.around(x2, i)
        r_ref[i - hx] = twice_ref[i - hx] - r[cut_y : cut_y + sy]

    rows(lo, hi, last)


def prolong_odd(src, out, win, x_from, y_from, count_x, count_y):
    for i in range(count_x):
        at = x_from + i
        for odd, other in ((0, at - 1), (1, at + 1)):
            row = 2 * i + odd - 1
            if row < 0 or row >= out.shape[0]:
                continue
            v = 0.75 * src[at] + 0.25 * src[other]
            low, high = shifted(v, False)
            for parity, side in ((0, low), (1, high)):
                w = 0.75 * v + 0.25 * side
                out[row, pl.ds(parity, count_y, stride=2), :] = w[y_from : y_from + count_y]
    win.each(0, out, lambda i: win.mask(i, win.get(out, i)))


def call(kernel, outs, scratch, smem, *args, flops=0):
    specs = [
        pl.BlockSpec(memory_space=pltpu.SMEM if k in smem else pltpu.VMEM) for k in range(len(args))
    ]
    out_specs = [pl.BlockSpec(memory_space=pltpu.VMEM) for _ in outs]
    return pl.pallas_call(
        kernel,
        out_shape=[jax.ShapeDtypeStruct(s, F32) for s in outs],
        in_specs=specs,
        out_specs=out_specs,
        scratch_shapes=[pltpu.VMEM(s, F32) for s in scratch],
        compiler_params=pltpu.CompilerParams(vmem_limit_bytes=VMEM_LIMIT),
        cost_estimate=pl.CostEstimate(flops=int(flops) or 1000000, bytes_accessed=1000000, transcendentals=0),
    )(*args)


def exchange(copies, axes="gz"):
    got = lax.all_to_all(copies, axes, 0, 0, tiled=True)
    return got


def stacked(copies):
    got = exchange(copies)
    return got.reshape(got.shape[0] * got.shape[1], got.shape[2])


def edges(v, axis, dim, width):
    size, length = lax.axis_size(axis), v.shape[dim]
    up = [(i, i + 1) for i in range(size - 1)]
    last = lax.slice_in_dim(v, length - width, length, axis=dim)
    first = lax.slice_in_dim(v, 0, width, axis=dim)
    return lax.ppermute(last, axis, up), lax.ppermute(first, axis, [(b, a) for a, b in up])


def halo_y(v, width):
    return edges(v, "gy", 1, width)


def halo_x(v, width):
    low, high = edges(v, "gx", 0, width)
    return jnp.concatenate([low, v, high], axis=0)


def body(right_side, z_faces, xy_coupling, block_inverse):
    part = functools.partial
    gx, gy, gz = (lax.axis_size(a) for a in ("gx", "gy", "gz"))
    n = z_faces.shape[0]
    where = jnp.stack([lax.axis_index(a) for a in ("gx", "gy", "gz")]).astype(jnp.int32)
    sx, sy = right_side.shape[0], right_side.shape[1]
    grids = [(gx * (sx >> l), gy * (sy >> l)) for l in range(LEVELS)]
    e = xy_coupling
    faces = z_faces.reshape(1, n)

    setup = call(
        powers_kernel,
        [(POWERS, n, n)] * LEVELS + [(8, n)] * LEVELS + [(POWERS, 8, n)] * LEVELS + [(8, n), (16, n), (n, n), (gz, 11, 8, n)],
        [],
        (1,),
        block_inverse, e, faces,
    )
    power, ends, link = (setup[k * LEVELS : (k + 1) * LEVELS] for k in range(3))
    ends_up, basis, basis_up, table = setup[3 * LEVELS :]
    low, high, table = lax.optimization_barrier((*halo_y(right_side, 12), table))
    f0 = halo_x(jnp.concatenate([low, right_side, high], axis=1), 12)
    table = exchange(table)
    *om, om_up, m_matrix, m_link, mix, up_mix, w2_map, w4_map = call(
        coupling_kernel,
        [(8, n)] * LEVELS + [(8, n), (n, n), (8, n), (11, n, n), (18, n, n), (8, n), (8, n)],
        [(gz, 8, 8, n), (n, n)],
        (0, 2),
        where, table, e, faces, basis, basis_up,
    )

    s0, s1, s2 = (sx, sy), (sx // 2, sy // 2), (sx // 4, sy // 4)
    ext0, ext1 = (sx + 24, sy + 24), (sx // 2 + 10, sy // 2 + 16)
    cube0, cube1 = ext0 + (n,), ext1 + (n,)
    lines0, lines1 = ext0[0] * ext0[1], ext1[0] * ext1[1]
    lanes = padded_lanes(lines0) + padded_lanes(lines1) + padded_lanes(s2[0] * s2[1])
    copies, f1_local, f2_local = call(
        part(local_down_kernel, s0, s1, grids),
        [(gz, 8, lanes), cube1, s2 + (n,)],
        [cube0] * 4 + [(ext1[0], ext0[1], n)] + [cube1] * 4 + [(s2[0], ext1[1], n)],
        (0,),
        where, f0, power[0], power[1], ends[0], ends[1], ends[2],
    )
    got = stacked(copies)
    f1, own1, parts = call(
        part(joined_down_kernel, s0, s1, ext0, grids),
        [cube1, cube1, (gy, s2[0] + 1, s2[1], n)],
        [cube0] * 3 + [(ext1[0], ext0[1], n)] + [cube1] * 4 + [(s2[0], ext1[1], n), s2 + (n,)],
        (0,),
        where, got, f1_local, f2_local, mix, om[2], w2_map,
    )
    parts = exchange(parts, "gy")
    inner0 = (sx + 8, sy + 8, n)
    known0, twice0 = call(
        part(known_zero_kernel, s0, ext0, grids[0]),
        [s0 + (n,), s0 + (n,)],
        [inner0] * 8,
        (0, 1),
        where, e, f0, got, mix, power[0], link[0],
        flops=20000000000,
    )
    (known1,) = call(
        part(known_one_kernel, s1, grids[1]),
        [cube1],
        [cube1] * 6,
        (0, 1),
        where, e, f1, own1, power[1], link[1],
        flops=10000000000,
    )
    parts, known1 = lax.optimization_barrier((parts, known1))
    parts = exchange(jnp.broadcast_to(parts[None], (gx,) + parts.shape), "gx")
    parts, known0, twice0 = lax.optimization_barrier((parts, known0, twice0))
    parts = parts.reshape((gx * gy,) + parts.shape[2:])

    cubes = [g + (n,) for g in grids]
    lines = [g[0] * g[1] for g in grids]
    margin = s2[0]
    region = (3 * s2[0], 3 * s2[1], n)
    padded = (grids[2][0] + 2 * margin, grids[2][1] + 2 * margin, n)
    f3, f4_local, copies = call(
        part(gathered_down_kernel, gx, gy),
        [cubes[3], cubes[4], (gz, 8, lines[3] + lines[4])],
        [cubes[2], (lines[2], n), (8, lines[2])]
        + [cubes[2]] * 4
        + [(grids[3][0], grids[2][1], n)]
        + [cubes[3]] * 4
        + [(grids[4][0], grids[3][1], n)],
        (),
        parts, power[2], link[2], power[3], ends[3], ends[4],
    )
    got34 = stacked(copies)
    parts, f3 = lax.optimization_barrier((parts, f3))
    (known2,) = call(
        part(known_two_kernel, gx, gy, grids[2]),
        [region],
        [(region[0] * region[1], n), (8, region[0] * region[1])] + [region] * 6,
        (0, 1),
        where, e, parts, power[2], link[2],
        flops=500000000,
    )
    (known3_local,) = call(
        part(local_known_kernel, 3),
        [cubes[3]],
        [cubes[3]] * 6,
        (0,),
        e, f3, power[3],
        flops=500000000,
    )
    got34, known2, known3_local = lax.optimization_barrier((got34, known2, known3_local))

    copies, c1_local = call(
        part(local_up_kernel, s0, grids, margin),
        [(gz, 8, sum(UP_LANES)), cube1],
        [cubes[3]] * 3 + [(grids[4][0], grids[3][1], n)] + [cubes[4]] * 2 + [cubes[3]] + [cubes[4]] * 3 + [cubes[3]] * 5 + [cubes[2], padded] + [region] * 5 + [cube1] * 4,
        (0, 1),
        where, e, f4_local, got34, om[4], w4_map, up_mix, power[4], link[4], known3_local, known2, known1,
        power[3], power[2], power[1], ends[3], ends[2], ends[1], ends_up,
    )
    u, r = call(
        part(finish_kernel, s0, grids, margin),
        [s0 + (n,), s0 + (n,)],
        [cubes[3]] * 3 + [cubes[2], padded] + [region] * 4 + [cube1] * 5 + [inner0] * 7,
        (0, 1),
        where, e, stacked(copies), c1_local, known0, twice0, up_mix, basis_up,
        power[0], link[0], m_matrix, m_link,
    )
    return u, r


def solution(mesh):
    return jax.shard_map(
        body,
        mesh=mesh,
        in_specs=(P("gx", "gy", "gz"), P("gz"), P(), P(None, "gz", None)),
        out_specs=(P("gx", "gy", "gz"), P("gx", "gy", "gz")),
        check_vma=False,
    )
```

```python
import functools

import jax
import jax.numpy as jnp
from jax import lax
from jax.experimental import pallas as pl
from jax.experimental.pallas import tpu as pltpu
from jax.sharding import PartitionSpec as P

LEVELS = 5
POWERS = 4
HIGHEST = lax.Precision.HIGHEST
F32 = jnp.float32
KNOWN = (0.9984, 0.9728, 0.8192, 0.4096)
TWICE = (0.0016, 0.0256, 0.1536, 0.4096, 0.4096)
VMEM_LIMIT = 56 * 1024 * 1024


def contract(a, b, da, db):
    return lax.dot_general(
        a, b, (((da,), (db,)), ((), ())), precision=HIGHEST, preferred_element_type=F32
    )


def exact_nn(a, b):
    return contract(a, b, 1, 0)


def exact_nt(a, b):
    return contract(a, b, 1, 1)


def exact_tn(a, b):
    return contract(a, b, 0, 0)


def halves(a):
    if isinstance(a, tuple):
        return a
    high = a.astype(jnp.bfloat16)
    return high, (a - high.astype(F32)).astype(jnp.bfloat16)


def product(a, b, da, db):
    (ah, al), (bh, bl) = halves(a), halves(b)

    def dot(x, y):
        return lax.dot_general(x, y, (((da,), (db,)), ((), ())), preferred_element_type=F32)

    return dot(ah, bh) + (dot(ah, bl) + dot(al, bh))


def nn(a, b):
    return product(a, b, 1, 0)


def nt(a, b):
    return product(a, b, 1, 1)


def tn(a, b):
    return product(a, b, 0, 0)


def rows(lo, hi, fn, step=8):
    full = (hi - lo) // step
    if full:
        def group(k, carry):
            for q in range(step):
                fn(lo + k * step + q)
            return carry

        lax.fori_loop(0, full, group, 0)
    for i in range(lo + full * step, hi):
        fn(i)


def sublane_index(length):
    return lax.broadcasted_iota(jnp.int32, (length, 128), 0)


def shifted(v, zero_ends):
    n = v.shape[0]
    low, high = pltpu.roll(v, 1, 0), pltpu.roll(v, n - 1, 0)
    if zero_ends:
        at = sublane_index(n)
        low = jnp.where(at > 0, low, 0.0)
        high = jnp.where(at < n - 1, high, 0.0)
    return low, high


class Window:
    def __init__(self, shape, origin=None, grid=None):
        self.x, self.y = shape
        self.whole = origin is None
        self.lo, self.hi = (0, self.y) if self.whole else (1, self.y - 1)
        if not self.whole:
            self.x0, y0 = origin
            self.nx, ny = grid
            at = sublane_index(self.y - 2) + (y0 + 1)
            self.in_y = jnp.where((at >= 0) & (at < ny), 1.0, 0.0).astype(F32)

    def get(self, ref, i):
        return ref[i, self.lo : self.hi]

    def put(self, ref, i, v):
        ref[i, self.lo : self.hi] = v

    def mask(self, i, v):
        if self.whole:
            return v
        at = self.x0 + i
        inside = jnp.where((at >= 0) & (at < self.nx), 1.0, 0.0).astype(F32)
        return v * (self.in_y * inside)

    def around(self, ref, i):
        if self.whole:
            low, high = shifted(ref[i], True)
            total = low + high
            if not (isinstance(i, int) and i == 0):
                total = total + ref[i - 1]
            if not (isinstance(i, int) and i == self.x - 1):
                total = total + ref[i + 1]
            return total
        y = self.y
        return (ref[i, 0 : y - 2] + ref[i, 2:y]) + (ref[i - 1, 1 : y - 1] + ref[i + 1, 1 : y - 1])

    def span(self, trim):
        return (0, self.x) if self.whole else (trim, self.x - trim)

    def loop(self, trim, fn):
        lo, hi = self.span(trim)
        if self.whole:
            fn(0)
            rows(lo + 1, hi - 1, fn)
            fn(hi - 1)
        else:
            rows(lo, hi, fn)

    def each(self, trim, out, fn):
        self.loop(trim, lambda i: self.put(out, i, fn(i)))


def line_powers(field, ends, power_ref, link_ref, count, out_refs, exact=False):
    if not exact:
        field, ends = halves(field), halves(ends)
    for j in range(count):
        if exact:
            value = exact_nt(field, power_ref[j]) + exact_tn(ends, link_ref[j])
        else:
            value = nt(field, power_ref[j]) + tn(ends, link_ref[j])
        out_refs[j][...] = value.reshape(out_refs[j].shape)


def smoothed_residual(win, field_ref, x1, x2, t, out, trim, masked=False, add=None):
    win.each(trim - 1, t, lambda i: 0.32 * win.get(x1, i) + win.mask(i, 0.64 * win.around(x2, i)))

    def outer(i):
        v = 0.04 * win.get(field_ref, i) + win.around(t, i)
        if add is not None:
            v = v + win.get(add, i)
        return win.mask(i, v) if masked else v

    win.each(trim, out, outer)


def horner(win, xs, weights, t0, t1, trim):
    src = xs[-1]
    scale = weights[-1]
    buffers = (t0, t1)
    for n, j in enumerate(range(len(xs) - 2, 0, -1)):
        dst = buffers[n % 2]

        def one(i, src=src, j=j, scale=scale):
            return weights[j] * win.get(xs[j], i) + win.mask(i, scale * win.around(src, i))

        win.each(trim - j, dst, one)
        src, scale = dst, 1.0
    return src, scale


def restrict(src, scratch, out, x_at, y_at):
    count_x, count_y = out.shape[0], out.shape[1]
    for i in range(count_x):
        scratch[i] = src[x_at + 2 * i] + src[x_at + 2 * i + 1]
    for i in range(count_x):
        even = scratch[i, pl.ds(y_at, count_y, stride=2), :]
        odd = scratch[i, pl.ds(y_at + 1, count_y, stride=2), :]
        out[i] = (even + odd) * 0.25


def prolong(src, src_whole, out, win, x_from, y_from, count_x, count_y):
    last = src.shape[0] - 1
    for i in range(count_x):
        at = x_from + i
        centre = src[at]
        below = src[at - 1] if at > 0 else jnp.zeros_like(centre)
        above = src[at + 1] if at < last else jnp.zeros_like(centre)
        for odd, other in ((0, below), (1, above)):
            v = 0.75 * centre + 0.25 * other
            low, high = shifted(v, src_whole)
            for parity, side in ((0, low), (1, high)):
                w = 0.75 * v + 0.25 * side
                out[2 * i + odd, pl.ds(parity, count_y, stride=2), :] = w[y_from : y_from + count_y]
    if not win.whole:
        win.each(0, out, lambda i: win.mask(i, win.get(out, i)))


def send(out_ref, value):
    for m in range(out_ref.shape[0]):
        out_ref[m] = value


def powers_kernel(g_ref, e_ref, zf_ref, *outs):
    levels, n = g_ref.shape[0], g_ref.shape[1]
    power_refs, ends_refs, link_refs = outs[0:levels], outs[levels : 2 * levels], outs[2 * levels : 3 * levels]
    up_ref, basis_ref, basis_up_ref, table_ref = outs[3 * levels :]
    table_ref[...] = jnp.zeros_like(table_ref)
    for level in range(levels):
        power_ref, ends_ref, link_ref = power_refs[level], ends_refs[level], link_refs[level]
        link_ref[...] = jnp.zeros_like(link_ref)
        e = e_ref[level]
        inverse_e = 1.0 / jnp.full((1, n), e, F32)
        one = g_ref[level] * e
        two = exact_nn(one, one)
        three = exact_nn(two, one)
        four = exact_nn(two, two)
        ends = []
        for j, value in enumerate((one, two, three, four)):
            power_ref[j] = value
            for s, row in enumerate((value[0:1], value[n - 1 : n])):
                ends_ref[2 * j + s : 2 * j + s + 1] = row
                table_ref[0, 2 * j + s, level : level + 1] = row
                ends.append(row)
        for j in range(POWERS):
            for i in range(j + 1):
                for t in range(2):
                    link_ref[j, 2 * i + t : 2 * i + t + 1] = ends[2 * (j - i) + t] * inverse_e
        table_ref[0, 9, level : level + 1] = inverse_e
    table_ref[0, 8] = jnp.broadcast_to(zf_ref[...], (8, n))
    def columns(level):
        return ends_refs[level][0:4] * (1.0 / jnp.full((4, n), e_ref[level], F32))

    zero = columns(0)
    basis_ref[0:4] = zero
    basis_ref[4:8] = exact_nn(zero, power_refs[1][0])
    basis_ref[8:12] = exact_nn(zero, power_refs[1][1])
    basis_ref[12:16] = columns(1)
    three = columns(3)
    two = [three, exact_nn(three, power_refs[2][0]), exact_nn(three, power_refs[2][1]), columns(2)]
    two = jnp.concatenate(two, 0)
    basis_up_ref[...] = jnp.zeros_like(basis_up_ref)
    basis_up_ref[0:16] = two
    basis_up_ref[16:32] = exact_nn(two, power_refs[1][0])
    basis_up_ref[32:48] = exact_nn(two, power_refs[1][1])
    basis_up_ref[48:52] = columns(1)
    at = lax.broadcasted_iota(jnp.int32, (1, n), 1)
    up_ref[...] = jnp.zeros_like(up_ref)
    up_ref[0:4] = ends_refs[0][0:4]
    up_ref[4:5] = jnp.where(at == 0, 1.0, 0.0).astype(F32)
    up_ref[5:6] = jnp.where(at == n - 1, 1.0, 0.0).astype(F32)


    full_basis = jnp.concatenate([basis_ref[...], jnp.zeros((n - 16, n), F32)], 0)
    at = lax.broadcasted_iota(jnp.int32, (8, n), 1)
    first = jnp.where(at < 4, exact_nt(ends_refs[1][...], full_basis), 0.0)
    second = exact_nt(ends_refs[2][...], full_basis)
    shifted_ends = jnp.concatenate([jnp.zeros((4, n), F32), ends_refs[2][0:4]], 0)
    third = jnp.where(at < 4, exact_nt(shifted_ends, basis_up_ref[...]), 0.0)
    fourth = jnp.where(at < 16, exact_nt(ends_refs[1][...], basis_up_ref[...]), 0.0)
    fifth = exact_nt(up_ref[...], basis_up_ref[...])
    total = first + pltpu.roll(second, 4, 1) + pltpu.roll(third, 20, 1)
    sixth = jnp.where(at < 4, exact_nt(ends_refs[4][...], basis_up_ref[...]), 0.0)
    total = total + pltpu.roll(fourth, 24, 1) + pltpu.roll(fifth, 40, 1)
    table_ref[0, 10] = total + pltpu.roll(sixth, 92, 1)
    for m in range(1, table_ref.shape[0]):
        table_ref[m] = table_ref[0]


def coupling_kernel(
    where_ref, table_ref, e_ref, zf_ref, basis_ref, basis_up_ref, om0, om1, om2, om3, om4, om_up_ref, m_ref, m_link_ref, mix_ref, up_mix_ref, w2_ref, w4_ref, held, full
):
    blocks, n = table_ref.shape[0], table_ref.shape[3]
    k_own = where_ref[2]
    wide = (8, n)
    lane = lax.broadcasted_iota(jnp.int32, wide, 1)
    inverse_e = table_ref[0, 9]

    def entry(m, row, column):
        at = 0 if column == 0 else n - 1
        return jnp.broadcast_to(table_ref[m, row][:, at : at + 1], wide)

    corner = [
        [
            [[entry(m, 2 * i + s, t) * inverse_e for t in range(2)] for s in range(2)]
            for m in range(blocks)
        ]
        for i in range(POWERS)
    ]
    face = [entry(m, 8, 0) for m in range(blocks)]

    gain_v, gain_d, gain_p, gain_g = [corner[0][0][1][1]], [None], [None], [None]
    for k in range(1, blocks):
        (a, b), (c, d) = corner[0][k]
        g = face[k]
        gv = g * g * gain_v[k - 1]
        dk = 1.0 / (1.0 - a * gv)
        gain_d.append(dk)
        gain_p.append(dk * b)
        gain_g.append(gv)
        gain_v.append(d + c * gv * gain_p[k])

    def solve(low, high):
        u, pu = [high[0]], [None]
        for k in range(1, blocks):
            (a, b), (c, d) = corner[0][k]
            gu = face[k] * u[k - 1]
            pu.append(gain_d[k] * (low[k] + a * gu))
            u.append(high[k] + c * (gu + gain_g[k] * pu[k]))
        zero = jnp.zeros(wide, F32)
        alpha, beta = [zero] * blocks, [zero] * blocks
        for k in range(blocks - 1, 0, -1):
            p = pu[k] + gain_p[k] * beta[k]
            beta[k - 1] = face[k] * p
            alpha[k] = face[k] * (u[k - 1] + gain_v[k - 1] * beta[k - 1])
        return alpha, beta

    unit = [
        [jnp.where(lane == 8 * m + s, 1.0, 0.0).astype(F32) for m in range(blocks)] for s in range(2)
    ]
    response = [solve(unit[0], unit[1])]
    for i in range(1, POWERS):
        source = [[None] * blocks, [None] * blocks]
        for m in range(blocks):
            for s in range(2):
                total = None
                for q in range(i):
                    c = corner[i - q][m][s]
                    term = c[0] * response[q][0][m] + c[1] * response[q][1][m]
                    total = term if total is None else total + term
                source[s][m] = total
        response.append(solve(source[0], source[1]))
    for i in range(POWERS):
        for t in range(2):
            for m in range(blocks):
                held[m, 2 * i + t] = response[i][t][m]
    om_refs = (om0, om1, om2, om3, om4)
    for i in range(POWERS):
        for t in range(2):
            total = held[k_own, 2 * i + t]
            for j in range(1, i + 1):
                total = total + pltpu.roll(held[k_own, 2 * (i - j) + t], 2 * j, 1)
            for level in range(LEVELS):
                om_refs[level][2 * i + t : 2 * i + t + 1] = total[level : level + 1]
    om_up_ref[...] = om0[...]

    lane = lane[0:1]
    om_up_ref[4:5] = jnp.where((lane == 8 * (k_own - 1) + 5) & (k_own > 0), 1.0, 0.0).astype(F32)
    om_up_ref[5:6] = jnp.where((lane == 8 * (k_own + 1) + 4) & (k_own < blocks - 1), 1.0, 0.0).astype(F32)
    om_up_ref[6:8] = jnp.zeros((2, n), F32)

    row = lax.broadcasted_iota(jnp.int32, (n, n), 0)
    column = lax.broadcasted_iota(jnp.int32, (n, n), 1)

    def every(i, t, m, offset):
        total = held[m, 2 * i + t]
        if i == 1:
            total = total + pltpu.roll(held[m, t], 2, 1)
        return pltpu.roll(total, offset, 1) if offset else total

    def matrix(level, groups, own=None, offset=0):
        full[...] = jnp.zeros_like(full)
        for start, i, scale in groups:
            for m in range(blocks):
                for t in range(2):
                    at = start + 2 * m + t
                    full[at : at + 1] = scale * every(i, t, m, offset)[level : level + 1]
        if own is not None:
            full[own : own + 8] = om_refs[level][...]
        return full[...].T

    def gathered(offset, count):
        tiles = jnp.concatenate([table_ref[m, 10] for m in range(blocks)], 0)
        at = row - offset
        place = (at >= 0) & (at < count) & (at == (column >> 4) * 2 + (column & 1))
        value = exact_nn(tiles, jnp.where(place, 1.0, 0.0).astype(F32))
        high = 8 * blocks
        value = jnp.where((row[0:high] >> 3) == ((column[0:high] >> 1) & 7), value, 0.0)
        return jnp.concatenate([value, jnp.zeros((n - high, n), F32)], 0)

    def diagonal(shift, scale):
        return jnp.where((row < 32) & (column == row + shift), scale, 0.0).astype(F32)

    def rest(slot_ref, base, level, once, twice, table):
        slot_ref[base] = once
        slot_ref[base + 1] = twice
        slot_ref[base + 2] = diagonal(0, 0.04)
        slot_ref[base + 3] = exact_nn(table, once) + diagonal(32, 0.32)
        slot_ref[base + 4] = exact_nn(table, twice) + diagonal(64, 0.64)

    mix_ref[0] = matrix(0, [(0, 0, 0.32)], 64)
    mix_ref[1] = matrix(0, [(0, 1, 0.64), (16, 0, 0.64)])
    one = gathered(0, 4).T
    rest(mix_ref, 2, 1, matrix(1, [(96, 0, 0.32)]), matrix(1, [(96, 1, 0.64), (112, 0, 0.64)]), one)
    mix_ref[7] = matrix(1, [], 0)
    mix_ref[8] = exact_nn(one, mix_ref[7])
    w2_ref[...] = exact_nn(om2[...], gathered(4, 16))
    basis = jnp.concatenate([basis_ref[...], jnp.zeros((n - 16, n), F32)], 0)
    own_rows = jnp.where(
        (row < 16) & (column == (row >> 1) * 16 + 2 * k_own + (row & 1)), 1.0, 0.0
    ).astype(F32)
    chosen = exact_tn(own_rows, basis)
    mix_ref[9] = jnp.where(row < 32, chosen, 0.0)
    mix_ref[10] = chosen

    up_mix_ref[0] = matrix(3, [(0, 0, 0.32)])
    up_mix_ref[1] = matrix(3, [(0, 1, 0.64), (16, 0, 0.64)])
    once = matrix(2, [(96, 0, 0.32)], offset=4)
    twice = matrix(2, [(96, 1, 0.64), (112, 0, 0.64)], offset=4)
    rest(up_mix_ref, 2, 2, once, twice, gathered(20, 4).T)
    both = matrix(1, [(0, 0, 1.0), (16, 1, 1.0)])
    through = exact_nn(gathered(24, 16).T, both)
    up_rows = om_up_ref[...]
    for k, scale in enumerate((0.04, 0.32, 0.64)):
        full[...] = jnp.zeros_like(full)
        full[16 * k : 16 * k + 16] = scale * own_rows[0:16]
        full[64:72] = scale * exact_nn(up_rows, gathered(40 + 16 * k, 16))
        up_mix_ref[7 + k] = full[...].T
    last = exact_nn(up_rows, gathered(88, 4))
    wide_lane = lax.broadcasted_iota(jnp.int32, (8, n), 1)
    full[...] = jnp.zeros_like(full)
    for t in range(2):
        full[48 + t : 49 + t] = jnp.where(lane == 2 * k_own + t, 0.32, 0.0).astype(F32)
    full[64:72] = jnp.where(wide_lane < 16, 0.32 * last, 0.0)
    mixed = full[...].T
    up_mix_ref[8] = up_mix_ref[8] + exact_nn(through, mixed)
    up_mix_ref[10] = exact_nn(both, mixed)
    full[...] = jnp.zeros_like(full)
    for t in range(2):
        full[48 + t : 49 + t] = jnp.where(lane == 16 + 2 * k_own + t, 0.64, 0.0).astype(F32)
        full[50 + t : 51 + t] = jnp.where(lane == 2 * k_own + t, 0.64, 0.0).astype(F32)
    swapped = jnp.where(
        wide_lane < 16,
        pltpu.roll(last, n - 16, 1),
        jnp.where(wide_lane < 32, pltpu.roll(last, 16, 1), 0.0),
    )
    full[64:72] = 0.64 * swapped
    mixed = full[...].T
    up_mix_ref[9] = up_mix_ref[9] + exact_nn(through, mixed)
    up_mix_ref[11] = exact_nn(both, mixed)
    full[...] = jnp.zeros_like(full)
    full[64:72] = up_rows
    up_mix_ref[12] = full[...].T
    up_mix_ref[13] = jnp.where(row < 32, exact_tn(own_rows, basis_up_ref[...]), 0.0)
    w4_ref[...] = exact_nn(om4[...], gathered(92, 4))
    for q in range(POWERS):
        full[...] = jnp.zeros_like(full)
        for b in range(q + 1):
            full[2 * b : 2 * b + 2] = KNOWN[q] * om3[2 * (q - b) : 2 * (q - b) + 2]
        up_mix_ref[14 + q] = full[...].T

    above = jnp.minimum(k_own + 1, blocks - 1)
    top = table_ref[above, 8][0:1, 0:1]
    top = jnp.where(jnp.full((1, 1), k_own, jnp.int32) < blocks - 1, top, 1.0)
    down = zf_ref[...]
    up = jnp.where(lane == n - 1, jnp.broadcast_to(top, (1, n)), pltpu.roll(down, n - 1, 1))
    down_all, up_all = jnp.broadcast_to(down, (n, n)), jnp.broadcast_to(up, (n, n))
    m_ref[...] = jnp.where(
        row == column,
        down_all + up_all + 4.0 * e_ref[0],
        jnp.where(row == column - 1, -down_all, jnp.where(row == column + 1, -up_all, 0.0)),
    )
    m_link_ref[...] = jnp.zeros_like(m_link_ref)
    m_link_ref[4:5] = jnp.where(lane == 0, -down, 0.0)
    m_link_ref[5:6] = jnp.where(lane == n - 1, -up, 0.0)


def flat(ref):
    return ref[...].reshape(ref.shape[0] * ref.shape[1], ref.shape[2])


def ends_from(om_ref, got_ref):
    return exact_nn(om_ref[:, : got_ref.shape[0]], got_ref[...])


def restrict_into(src, scratch, out, x_at, y_at, count_y, y_to):
    for i in range(out.shape[0]):
        scratch[i] = src[x_at + 2 * i] + src[x_at + 2 * i + 1]
    for i in range(out.shape[0]):
        even = scratch[i, pl.ds(y_at, count_y, stride=2), :]
        odd = scratch[i, pl.ds(y_at + 1, count_y, stride=2), :]
        out[i, y_to : y_to + count_y] = (even + odd) * 0.25


def padded_lanes(count):
    return (count + 127) // 128 * 128


def split_lanes(ext):
    count = next(r for r in range(ext[0] // 2, ext[0] + 1) if r * ext[1] % 128 == 0)
    return count * ext[1], count


def part_maps(matrix):
    low = (lax.broadcasted_iota(jnp.int32, matrix.shape, 0) & 7) < 4
    first, second = jnp.where(low, matrix, 0.0), jnp.where(low, 0.0, matrix)
    count = matrix.shape[0]
    return (first, pltpu.roll(first, 4, 0)), (pltpu.roll(second, count - 4, 0), second)


def late_words_kernel(inner, f_ref, v_ref, out_ref):
    cx, cy = (f_ref.shape[0] - inner[0]) // 2, (f_ref.shape[1] - inner[1]) // 2
    half = inner[0] // 2
    out_ref[0] = jnp.zeros(out_ref.shape[1:], F32)
    for p in range(2):
        field = f_ref[cx + p * half : cx + (p + 1) * half, cy : cy + inner[1]]
        value = nt(v_ref[...], field.reshape(half * inner[1], 128))
        out_ref[0, 4 * p : 4 * p + 4, 0 : half * inner[1]] = value[4:8]
    for m in range(1, out_ref.shape[0]):
        out_ref[m] = out_ref[0]


def windows(where_ref, s0, s1, ext0, ext1, grids):
    h0 = tuple((a - b) // 2 for a, b in zip(ext0, s0))
    h1 = tuple((a - b) // 2 for a, b in zip(ext1, s1))
    ix, iy = where_ref[0], where_ref[1]
    win0 = Window(ext0, (ix * s0[0] - h0[0], iy * s0[1] - h0[1]), grids[0])
    win1 = Window(ext1, (ix * s1[0] - h1[0], iy * s1[1] - h1[1]), grids[1])
    return win0, win1, h0, h1


def local_down_kernel(
    s0, s1, grids, where_ref, f_ref, power0, power1, v0, v1, v2, out_ref, f1_ref, f2_ref,
    x1, x2, t, r, pair, y1, y2, t1, r1, pair1
):
    ext0, ext1 = f_ref.shape[:2], f1_ref.shape[:2]
    win0, win1, h0, h1 = windows(where_ref, s0, s1, ext0, ext1, grids)
    field = halves(flat(f_ref))
    lanes0 = ext0[0] * ext0[1]
    lanes1 = ext1[0] * ext1[1]
    at1 = split_lanes(ext0)[0]
    at2 = at1 + padded_lanes(lanes1)
    many = out_ref.shape[0]
    out_ref[0, :, 0:at1] = jnp.zeros((8, at1), F32)
    out_ref[0, :, at2 - 128 : at2] = jnp.zeros((8, 128), F32)
    out_ref[0, :, at2 : at2 + 128] = jnp.zeros((8, 128), F32)
    value = nt(v0[...], field)
    out_ref[0, 0:4, 0:at1] = value[0:4, 0:at1]
    out_ref[0, 4:8, 0 : lanes0 - at1] = value[0:4, at1:lanes0]
    x1[...] = nt(field, power0[0]).reshape(x1.shape)
    x2[...] = nt(field, power0[1]).reshape(x2.shape)
    smoothed_residual(win0, f_ref, x1, x2, t, r, 2, masked=True)
    f1_ref[...] = jnp.zeros_like(f1_ref)
    count = (ext0[1] - 4) // 2
    restrict_into(r, pair, f1_ref, 2, 2, count, (ext1[1] - count) // 2)
    field = halves(flat(f1_ref))
    out_ref[0, :, at1 : at1 + lanes1] = nt(v1[...], field)
    y1[...] = nt(field, power1[0]).reshape(y1.shape)
    y2[...] = nt(field, power1[1]).reshape(y2.shape)
    smoothed_residual(win1, f1_ref, y1, y2, t1, r1, h1[0])
    restrict(r1, pair1, f2_ref, h1[0], h1[1])
    lines2 = f2_ref.shape[0] * f2_ref.shape[1]
    out_ref[0, :, at2 : at2 + lines2] = nt(v2[...], flat(f2_ref))
    for m in range(1, many):
        out_ref[m] = out_ref[0]


def joined_down_kernel(
    s0, s1, ext0, grids, where_ref, got_ref, f1_local, f2_local, mix_ref, om2_ref, w2_ref,
    f1_ref, own1_ref, parts_ref, d1, d2, f, pair, y, h1s, h2s, f2s, pair1, z
):
    ext1 = f1_local.shape[:2]
    win0, win1, h0, h1 = windows(where_ref, s0, s1, ext0, ext1, grids)
    lanes0 = ext0[0] * ext0[1]
    lanes1 = ext1[0] * ext1[1]
    at1, cut_x = split_lanes(ext0)
    at2 = at1 + padded_lanes(lanes1)
    rows_in = got_ref.shape[0]
    spans = ((0, cut_x, at1), (cut_x, ext0[0], lanes0 - at1))
    for p, (lo, hi, count) in enumerate(spans):
        got0 = halves(got_ref[:, 0:count])
        for d, slot in ((d1, 0), (d2, 1)):
            matrix = part_maps(mix_ref[slot, 0:rows_in])[0][p]
            d[lo:hi] = tn(got0, matrix).reshape(hi - lo, ext0[1], 128)

    win0.each(1, d1, lambda i: win0.get(d1, i) + win0.mask(i, win0.around(d2, i)))
    win0.each(2, f, lambda i: win0.mask(i, win0.around(d1, i)))
    y[...] = jnp.zeros_like(y)
    count = (ext0[1] - 4) // 2
    restrict_into(f, pair, y, 2, 2, count, (ext1[1] - count) // 2)
    yf = halves(flat(y))
    f1_ref[...] = f1_local[...] + nn(yf, mix_ref[9]).reshape(f1_ref.shape)
    got1 = halves(got_ref[:, at1 : at1 + lanes1])
    own1_ref[...] = (tn(got1, mix_ref[7, 0:rows_in]) + nn(yf, mix_ref[8])).reshape(own1_ref.shape)
    h1s[...] = (tn(got1, mix_ref[2, 0:rows_in]) + nn(yf, mix_ref[5])).reshape(h1s.shape)
    h2s[...] = (tn(got1, mix_ref[3, 0:rows_in]) + nn(yf, mix_ref[6])).reshape(h2s.shape)
    f2s[...] = nn(yf, mix_ref[4]).reshape(f2s.shape)
    trim = h1[0]
    win1.each(trim - 1, h1s, lambda i: win1.get(h1s, i) + win1.mask(i, win1.around(h2s, i)))
    win1.each(trim, f2s, lambda i: win1.get(f2s, i) + win1.around(h1s, i))
    restrict(f2s, pair1, z, h1[0], h1[1])
    zf = flat(z)
    lines2 = zf.shape[0]
    side = z.shape[0]
    parts_ref[0, 0:side] = f2_local[...] + nn(zf, mix_ref[10]).reshape(z.shape)
    own2 = nn(om2_ref[:, 0:rows_in], got_ref[:, at2 : at2 + lines2]) + nt(w2_ref[...], zf)
    parts_ref[0, side] = jnp.zeros((8, 128), F32)
    parts_ref[0, side, :, 0:lines2] = own2
    for m in range(1, parts_ref.shape[0]):
        parts_ref[m] = parts_ref[0]


def lane_powers(field, coefficients, lane0, power_ref, link_ref, count, out_refs, exact=False):
    n = field.shape[1]
    if not exact:
        field, coefficients = halves(field), halves(coefficients)
    one, two = (exact_nt, exact_nn) if exact else (nt, nn)
    for j in range(count):
        pieces = [link_ref[j], jnp.zeros((n - 8 - lane0, n), F32)]
        if lane0:
            pieces = [jnp.zeros((lane0, n), F32)] + pieces
        value = one(field, power_ref[j]) + two(coefficients, jnp.concatenate(pieces, 0))
        out_refs[j][...] = value.reshape(out_refs[j].shape)


def known_zero_kernel(
    s0, ext0, late_at, grid, where_ref, e_ref, f_ref, got_ref, late_ref, mix_ref, power_ref, link_ref,
    known_out, twice_out, wide, own, f, x1, x2, x3, x4, t0, t1
):
    hx, hy = (f.shape[0] - s0[0]) // 2, (f.shape[1] - s0[1]) // 2
    cx, cy = (ext0[0] - f.shape[0]) // 2, (ext0[1] - f.shape[1]) // 2
    win = Window(f.shape[:2], (where_ref[0] * s0[0] - hx, where_ref[1] * s0[1] - hy), grid)
    early, late = part_maps(mix_ref[0, 0 : got_ref.shape[0]])
    at1, cut_x = split_lanes(ext0)
    spans = ((0, cut_x, at1), (cut_x, ext0[0], ext0[0] * ext0[1] - at1))
    for p, (lo, hi, count) in enumerate(spans):
        wide[lo:hi] = tn(got_ref[:, 0:count], early[p]).reshape(hi - lo, ext0[1], 128)
    own[...] = wide[cx : cx + f.shape[0], cy : cy + f.shape[1]]
    half = f.shape[0] // 2
    words = late_ref[:, late_at : late_at + half * f.shape[1]]
    for p in range(2):
        part = slice(p * half, (p + 1) * half)
        own[part] = own[part] + tn(words, late[p]).reshape(half, f.shape[1], 128)
    f[...] = f_ref[cx : cx + f.shape[0], cy : cy + f.shape[1]]
    xs = (x1, x2, x3, x4)
    lane_powers(flat(f), flat(own), 64, power_ref, link_ref, POWERS, xs)
    inverse_e = 1.0 / jnp.full((win.hi - win.lo, 128), e_ref[0], F32)
    at = hy - win.lo
    src, scale = horner(win, xs, KNOWN, t0, t1, hx)
    lo, hi = win.span(hx)

    def known(i):
        v = (KNOWN[0] * win.get(x1, i) + scale * win.around(src, i)) * inverse_e
        known_out[i - hx] = v[at : at + s0[1]]

    rows(lo, hi, known)
    src2, scale2 = horner(win, (f,) + xs, TWICE, t0, t1, hx)

    def again(i):
        v = TWICE[0] * win.get(f, i) + scale2 * win.around(src2, i)
        twice_out[i - hx] = v[at : at + s0[1]]

    rows(lo, hi, again)


def known_one_kernel(
    s1, grid, where_ref, e_ref, f_ref, own_ref, power_ref, link_ref, known_out, x1, x2, x3, x4, t0, t1
):
    hx, hy = (f_ref.shape[0] - s1[0]) // 2, (f_ref.shape[1] - s1[1]) // 2
    win = Window(f_ref.shape[:2], (where_ref[0] * s1[0] - hx, where_ref[1] * s1[1] - hy), grid)
    xs = (x1, x2, x3, x4)
    lane_powers(flat(f_ref), flat(own_ref), 0, power_ref, link_ref, POWERS, xs, exact=True)
    inverse_e = 1.0 / jnp.full((win.hi - win.lo, 128), e_ref[1], F32)
    src, scale = horner(win, xs, KNOWN, t0, t1, 3)
    known_out[...] = jnp.zeros_like(known_out)

    def known(i):
        return win.mask(i, (KNOWN[0] * win.get(x1, i) + scale * win.around(src, i)) * inverse_e)

    win.each(3, known_out, known)


def known_two_kernel(
    across, down, grid, where_ref, e_ref, parts_ref, power_ref, link_ref, known_out,
    fp, ap, x1, x2, x3, x4, t0, t1
):
    side = parts_ref.shape[2]
    lines = side * side
    ix, iy = where_ref[0], where_ref[1]
    for p in range(9):
        jx, jy = ix + p // 3 - 1, iy + p % 3 - 1
        inside = (jx >= 0) & (jx < across) & (jy >= 0) & (jy < down)
        at = jnp.clip(jx, 0, across - 1) * down + jnp.clip(jy, 0, down - 1)
        scale = jnp.where(inside, 1.0, 0.0).astype(F32)
        fp[p * lines : (p + 1) * lines] = (parts_ref[at, 0:side] * scale).reshape(lines, 128)
        ap[:, p * lines : (p + 1) * lines] = (parts_ref[at, side] * scale)[:, 0:lines]
    xs = (x1, x2, x3, x4)
    for j in range(POWERS):
        value = exact_nt(fp[...], power_ref[j]) + exact_tn(ap[...], link_ref[j])
        for p in range(9):
            px, py = p // 3 * side, p % 3 * side
            piece = value[p * lines : (p + 1) * lines].reshape(side, side, 128)
            xs[j][px : px + side, py : py + side] = piece
    win = Window(x1.shape[:2], ((ix - 1) * side, (iy - 1) * side), grid)
    inverse_e = 1.0 / jnp.full((win.hi - win.lo, 128), e_ref[2], F32)
    src, scale = horner(win, xs, KNOWN, t0, t1, 3)
    known_out[...] = jnp.zeros_like(known_out)

    def known(i):
        return win.mask(i, (KNOWN[0] * win.get(x1, i) + scale * win.around(src, i)) * inverse_e)

    win.each(3, known_out, known)


def gathered_down_kernel(
    across, down, parts_ref, late_ref, power_ref, link_ref, power3, v3, v4, coarse_ref, lower_ref, out_ref,
    f, fp, ap, x1, x2, t, r, pair, y1, y2, ty, ry, pair3
):
    many, side = parts_ref.shape[0], parts_ref.shape[2]
    lines = side * side
    for p in range(many):
        px, py = p // down * side, p % down * side
        part = parts_ref[p, 0:side]
        f[px : px + side, py : py + side] = part
        fp[p * lines : (p + 1) * lines] = part.reshape(lines, 128)
        ap[:, p * lines : (p + 1) * lines] = parts_ref[p, side][:, 0:lines]
    fields, coefficients = halves(fp[...]), halves(ap[...])
    for j, x in enumerate((x1, x2)):
        value = nt(fields, power_ref[j]) + tn(coefficients, link_ref[j])
        for p in range(many):
            px, py = p // down * side, p % down * side
            x[px : px + side, py : py + side] = value[p * lines : (p + 1) * lines].reshape(side, side, 128)
    win = Window(f.shape[:2])
    smoothed_residual(win, f, x1, x2, t, r, 2)
    restrict(r, pair, coarse_ref, 0, 0)
    field = halves(flat(coarse_ref))
    lanes = field[0].shape[0]
    out_ref[0, :, 0:lanes] = nt(v3[...], field)
    y1[...] = nt(field, power3[0]).reshape(y1.shape)
    y2[...] = nt(field, power3[1]).reshape(y2.shape)
    smoothed_residual(Window(y1.shape[:2]), coarse_ref, y1, y2, ty, ry, 2)
    restrict(ry, pair3, lower_ref, 0, 0)
    value = nt(v4[...], flat(lower_ref))
    out_ref[0, :, lanes : lanes + value.shape[1]] = value
    out_ref[0, :, lanes + value.shape[1] :] = late_ref[0]
    for m in range(1, out_ref.shape[0]):
        out_ref[m] = out_ref[0]


def local_known_kernel(level, e_ref, f_ref, power_ref, known_ref, x1, x2, x3, x4, t0, t1):
    win = Window(f_ref.shape[:2])
    xs = (x1, x2, x3, x4)
    for j in range(POWERS):
        xs[j][...] = exact_nt(flat(f_ref), power_ref[j]).reshape(x1.shape)
    inverse_e = 1.0 / jnp.full((f_ref.shape[1], 128), e_ref[level], F32)
    src, scale = horner(win, xs, KNOWN, t0, t1, 4)

    def known(i):
        known_ref[i] = (KNOWN[0] * x1[i] + scale * win.around(src, i)) * inverse_e

    win.loop(0, known)


def clear_edges(pad, margin):
    x, y = pad.shape[:2]
    zero_rows = jnp.zeros((margin, y, 128), F32)
    zero_cols = jnp.zeros((x, margin, 128), F32)
    pad[0:margin] = zero_rows
    pad[x - margin : x] = zero_rows
    pad[:, 0:margin] = zero_cols
    pad[:, y - margin : y] = zero_cols


def cut(where_ref, pad, out_ref, margin):
    sx, sy = out_ref.shape[0] - 2 * margin, out_ref.shape[1] - 2 * margin
    x_at = where_ref[0] * sx
    y_at = pl.multiple_of(where_ref[1] * sy, 8)

    def one(i):
        out_ref[i] = pad[x_at + i, pl.ds(y_at, out_ref.shape[1]), :]

    rows(0, out_ref.shape[0], one)


UP_LANES = (896, 896, 512)


def place_on_region(where_ref, fine, pad, out_ref, margin):
    clear_edges(pad, margin)

    def place(i):
        pad[i + margin, margin : margin + fine.shape[1]] = fine[i]

    rows(0, fine.shape[0], place)
    cut(where_ref, pad, out_ref, margin)


def up_windows(where_ref, s0, grids, region, ext1, ext0):
    s1, s2 = (s0[0] // 2, s0[1] // 2), (s0[0] // 4, s0[1] // 4)
    wins = []
    for level, (shape, s) in enumerate(((ext0, s0), (ext1, s1), (region, s2))):
        hx, hy = (shape[0] - s[0]) // 2, (shape[1] - s[1]) // 2
        wins.append(Window(shape, (where_ref[0] * s[0] - hx, where_ref[1] * s[1] - hy), grids[level]))
    return wins


def to_level_one(src, out, win):
    prolong_odd(src, out, win, 5, 4, (out.shape[0] + 2) // 2, out.shape[1] // 2)


def to_level_zero(src, out, win):
    prolong(src, False, out, win, 3, 6, out.shape[0] // 2, out.shape[1] // 2)


def local_up_kernel(
    s0, grids, margin, where_ref, e_ref, f4_local, got_ref, om_ref, w4_ref, mix_ref, power4, link4,
    known3_local, known2, known1, power3, power2, power1, v3, v2, v1, v0, out_ref, c1_ref,
    d1, d2, d3, pair, y4, f4, known3, b1, b2, c4, w3, p1, p2, pt, c3, fine, pad, w2, q1, q2, qt, c2, w1, r1, r2, rt
):
    k = got_ref.shape[0]
    win3 = Window(d1.shape[:2])
    lanes = win3.x * win3.y
    got3 = halves(got_ref[:, 0:lanes])
    d1[...] = tn(got3, mix_ref[0, 0:k]).reshape(d1.shape)
    d2[...] = tn(got3, mix_ref[1, 0:k]).reshape(d2.shape)
    win3.each(0, d1, lambda i: win3.get(d1, i) + win3.around(d2, i))
    win3.each(0, d3, lambda i: win3.around(d1, i))
    restrict(d3, pair, y4, 0, 0)
    f4[...] = f4_local[...] + exact_nn(flat(y4), mix_ref[13]).reshape(f4.shape)
    ends = exact_nn(om_ref[:, 0:k], got_ref[:, lanes : lanes + y4.shape[0] * y4.shape[1]])
    ends = ends + exact_nt(w4_ref[...], flat(y4))

    src, buffers = d1, (d2, d3)
    d1[...] = tn(got3, mix_ref[17, 0:k]).reshape(d1.shape)
    for n, q in enumerate((2, 1, 0)):
        dst = buffers[n % 2] if n < 2 else d1
        dst[...] = tn(got3, mix_ref[14 + q, 0:k]).reshape(d1.shape)
        win3.each(0, dst, lambda i, src=src, dst=dst: win3.get(dst, i) + win3.around(src, i))
        src = dst
    inverse_e = 1.0 / jnp.full((8, 128), e_ref[3], F32)
    bases = v3[...] * inverse_e
    bases = jnp.concatenate([bases * inverse_e, jnp.zeros((120, 128), F32)], 0)
    known3[...] = known3_local[...] + exact_nn(flat(src), bases).reshape(known3.shape)

    win = Window(f4.shape[:2])
    line_powers(flat(f4), ends, power4, link4, 2, (b1, b2), exact=True)
    inverse_e = 1.0 / jnp.full((f4.shape[1], 128), e_ref[LEVELS - 1], F32)

    def one(i):
        c4[i] = (0.96 * b1[i] + 0.64 * win.around(b2, i)) * inverse_e

    win.loop(0, one)
    prolong(c4, True, w3, win3, 0, 0, win.x, win.y)
    _, win1, win2 = up_windows(where_ref, s0, grids, w2.shape[:2], w1.shape[:2], w1.shape[:2])
    at1, at2 = UP_LANES[0], UP_LANES[0] + UP_LANES[1]
    out_ref[0] = jnp.zeros(out_ref.shape[1:], F32)

    def local(win, w, known, power, x1, x2, t, c):
        field = halves(flat(w))
        x1[...] = nt(field, power[0]).reshape(x1.shape)
        x2[...] = nt(field, power[1]).reshape(x2.shape)
        c[...] = jnp.zeros_like(c)
        smoothed_residual(win, w, x1, x2, t, c, 2, masked=True, add=known)

    def words(v_ref, w, first_row, at):
        value = exact_nt(v_ref[...], flat(w))
        out_ref[0, first_row : first_row + 4, at : at + value.shape[1]] = value[0:4]

    words(v3, w3, 0, at2)
    local(win3, w3, known3, power3, p1, p2, pt, c3)
    prolong(c3, True, fine, Window(fine.shape[:2]), 0, 0, win3.x, win3.y)
    place_on_region(where_ref, fine, pad, w2, margin)
    words(v2, w2, 4, at1)
    local(win2, w2, known2, power2, q1, q2, qt, c2)
    to_level_one(c2, w1, win1)
    words(v1, w1, 0, at1)
    local(win1, w1, known1, power1, r1, r2, rt, c1_ref)
    value = exact_nt(v0[...], flat(c1_ref))
    out_ref[0, :, 0 : value.shape[1]] = value
    for m in range(1, out_ref.shape[0]):
        out_ref[m] = out_ref[0]


def finish_kernel(
    s0, grids, margin, where_ref, e_ref, got_ref, c1_local, known_ref, twice_ref, mix_ref, basis_ref,
    power_ref, link_ref, m_ref, m_link_ref, u_ref, r_ref,
    d1, d2, d3, fine, pad, y2, g1, g2, g3, y1, h1, h2, h3, c1, w, q, x1, x2, xm, t0, t1
):
    win0, win1, win2 = up_windows(where_ref, s0, grids, y2.shape[:2], y1.shape[:2], w.shape[:2])
    lines1 = y1.shape[0] * y1.shape[1]
    lines2, lines3 = y2.shape[0] * y2.shape[1], d1.shape[0] * d1.shape[1]
    at1, at2 = UP_LANES[0], UP_LANES[0] + UP_LANES[1]
    k = got_ref.shape[0]

    got3 = halves(got_ref[:, at2 : at2 + lines3])
    d1[...] = tn(got3, mix_ref[0, 0:k]).reshape(d1.shape)
    d2[...] = tn(got3, mix_ref[1, 0:k]).reshape(d2.shape)
    win3 = Window(d1.shape[:2])
    win3.each(0, d1, lambda i: win3.get(d1, i) + win3.around(d2, i))
    win3.each(0, d3, lambda i: win3.around(d1, i))
    prolong(d3, True, fine, Window(fine.shape[:2]), 0, 0, win3.x, win3.y)
    place_on_region(where_ref, fine, pad, y2, margin)

    def coefficients(win, got, y, once, twice, maps, a1, a2, a3, trim):
        y, got = halves(flat(y)), halves(got)
        a1[...] = (tn(got, once[0:k]) + nn(y, maps[1])).reshape(a1.shape)
        a2[...] = (tn(got, twice[0:k]) + nn(y, maps[2])).reshape(a2.shape)
        a3[...] = nn(y, maps[0]).reshape(a3.shape)
        win.each(trim - 1, a1, lambda i: win.get(a1, i) + win.mask(i, win.around(a2, i)))
        win.each(trim, a3, lambda i: win.mask(i, win.get(a3, i) + win.around(a1, i)))

    maps = (mix_ref[4], mix_ref[5], mix_ref[6])
    got2 = got_ref[:, at1 : at1 + lines2]
    coefficients(win2, got2, y2, mix_ref[2], mix_ref[3], maps, g1, g2, g3, 2)
    to_level_one(g3, y1, win1)
    maps = (mix_ref[7], mix_ref[8], mix_ref[9])
    got1 = got_ref[:, at1 : at1 + lines1]
    coefficients(win1, got1, y1, mix_ref[10], mix_ref[11], maps, h1, h2, h3, 2)
    c1[...] = c1_local[...] + exact_nn(flat(h3), basis_ref[...]).reshape(c1.shape)
    h3[...] = h3[...] + tn(got_ref[:, 0:lines1], mix_ref[12, 0:k]).reshape(h3.shape)
    to_level_zero(c1, w, win0)
    to_level_zero(h3, q, win0)

    hx, hy = (w.shape[0] - s0[0]) // 2, (w.shape[1] - s0[1]) // 2
    sy = s0[1]
    win = win0
    field, ends = flat(w), flat(q)
    lane_powers(field, ends, 64, power_ref, link_ref, 2, (x1, x2))
    xm[...] = exact_nt(field, m_ref[...]).reshape(xm.shape)
    below, above = m_link_ref[4:5], m_link_ref[5:6]

    def link_ends(i):
        a = q[i]
        xm[i] = xm[i] + (pltpu.roll(a, 128 - 68, 1) * below + pltpu.roll(a, 127 - 69, 1) * above)

    rows(0, q.shape[0], link_ends)
    e = e_ref[0]
    w_ref = w

    lo, hi = win.span(hx - 2)

    def inner(i):
        one = 0.32 * win.get(x1, i)
        two = win.mask(i, 0.64 * win.around(x2, i))
        win.put(t0, i, one + two)
        win.put(t1, i, e * (one - two))

    rows(lo, hi, inner)
    win.each(hx - 1, x2, lambda i: (0.28 * e) * win.get(w_ref, i) + win.mask(i, win.around(t1, i)))
    lo, hi = win.span(hx)
    cut_y = hy - win.lo

    def last(i):
        u = 0.04 * win.get(w_ref, i) + win.around(t0, i)
        u_ref[i - hx] = known_ref[i - hx] + u[cut_y : cut_y + sy]
        r = 0.04 * win.get(xm, i) + win.around(x2, i)
        r_ref[i - hx] = twice_ref[i - hx] - r[cut_y : cut_y + sy]

    rows(lo, hi, last)


def prolong_odd(src, out, win, x_from, y_from, count_x, count_y):
    for i in range(count_x):
        at = x_from + i
        for odd, other in ((0, at - 1), (1, at + 1)):
            row = 2 * i + odd - 1
            if row < 0 or row >= out.shape[0]:
                continue
            v = 0.75 * src[at] + 0.25 * src[other]
            low, high = shifted(v, False)
            for parity, side in ((0, low), (1, high)):
                w = 0.75 * v + 0.25 * side
                out[row, pl.ds(parity, count_y, stride=2), :] = w[y_from : y_from + count_y]
    win.each(0, out, lambda i: win.mask(i, win.get(out, i)))


def call(kernel, outs, scratch, smem, *args, flops=0):
    specs = [
        pl.BlockSpec(memory_space=pltpu.SMEM if k in smem else pltpu.VMEM) for k in range(len(args))
    ]
    out_specs = [pl.BlockSpec(memory_space=pltpu.VMEM) for _ in outs]
    return pl.pallas_call(
        kernel,
        out_shape=[jax.ShapeDtypeStruct(s, F32) for s in outs],
        in_specs=specs,
        out_specs=out_specs,
        scratch_shapes=[pltpu.VMEM(s, F32) for s in scratch],
        compiler_params=pltpu.CompilerParams(vmem_limit_bytes=VMEM_LIMIT),
        cost_estimate=pl.CostEstimate(flops=int(flops) or 1000000, bytes_accessed=1000000, transcendentals=0),
    )(*args)


def exchange(copies, axes="gz"):
    got = lax.all_to_all(copies, axes, 0, 0, tiled=True)
    return got


def stacked(copies):
    got = exchange(copies)
    return got.reshape(got.shape[0] * got.shape[1], got.shape[2])


def edges(v, axis, dim, width):
    size, length = lax.axis_size(axis), v.shape[dim]
    up = [(i, i + 1) for i in range(size - 1)]
    last = lax.slice_in_dim(v, length - width, length, axis=dim)
    first = lax.slice_in_dim(v, 0, width, axis=dim)
    return lax.ppermute(last, axis, up), lax.ppermute(first, axis, [(b, a) for a, b in up])


def halo_y(v, width):
    return edges(v, "gy", 1, width)


def halo_x(v, width):
    low, high = edges(v, "gx", 0, width)
    return jnp.concatenate([low, v, high], axis=0)


def body(right_side, z_faces, xy_coupling, block_inverse):
    part = functools.partial
    gx, gy, gz = (lax.axis_size(a) for a in ("gx", "gy", "gz"))
    n = z_faces.shape[0]
    where = jnp.stack([lax.axis_index(a) for a in ("gx", "gy", "gz")]).astype(jnp.int32)
    sx, sy = right_side.shape[0], right_side.shape[1]
    grids = [(gx * (sx >> l), gy * (sy >> l)) for l in range(LEVELS)]
    e = xy_coupling
    faces = z_faces.reshape(1, n)

    setup = call(
        powers_kernel,
        [(POWERS, n, n)] * LEVELS + [(8, n)] * LEVELS + [(POWERS, 8, n)] * LEVELS + [(8, n), (16, n), (n, n), (gz, 11, 8, n)],
        [],
        (1,),
        block_inverse, e, faces,
    )
    power, ends, link = (setup[k * LEVELS : (k + 1) * LEVELS] for k in range(3))
    ends_up, basis, basis_up, table = setup[3 * LEVELS :]
    low, high, table = lax.optimization_barrier((*halo_y(right_side, 12), table))
    f0 = halo_x(jnp.concatenate([low, right_side, high], axis=1), 12)
    table = exchange(table)
    *om, om_up, m_matrix, m_link, mix, up_mix, w2_map, w4_map = call(
        coupling_kernel,
        [(8, n)] * LEVELS + [(8, n), (n, n), (8, n), (11, n, n), (18, n, n), (8, n), (8, n)],
        [(gz, 8, 8, n), (n, n)],
        (0, 2),
        where, table, e, faces, basis, basis_up,
    )

    s0, s1, s2 = (sx, sy), (sx // 2, sy // 2), (sx // 4, sy // 4)
    ext0, ext1 = (sx + 24, sy + 24), (sx // 2 + 10, sy // 2 + 16)
    cube0, cube1 = ext0 + (n,), ext1 + (n,)
    lines0, lines1 = ext0[0] * ext0[1], ext1[0] * ext1[1]
    lanes = split_lanes(ext0)[0] + padded_lanes(lines1) + padded_lanes(s2[0] * s2[1])
    copies, f1_local, f2_local = call(
        part(local_down_kernel, s0, s1, grids),
        [(gz, 8, lanes), cube1, s2 + (n,)],
        [cube0] * 4 + [(ext1[0], ext0[1], n)] + [cube1] * 4 + [(s2[0], ext1[1], n)],
        (0,),
        where, f0, power[0], power[1], ends[0], ends[1], ends[2],
    )
    got = stacked(copies)
    inner0 = (sx + 8, sy + 8, n)
    late_lanes = padded_lanes(inner0[0] * inner0[1] // 2)
    (late,) = call(
        part(late_words_kernel, inner0[:2]), [(1, 8, late_lanes)], [], (), f0, ends[0], flops=500000000
    )
    got, late = lax.optimization_barrier((got, late))
    f1, own1, parts = call(
        part(joined_down_kernel, s0, s1, ext0, grids),
        [cube1, cube1, (gy, s2[0] + 1, s2[1], n)],
        [cube0] * 3 + [(ext1[0], ext0[1], n)] + [cube1] * 4 + [(s2[0], ext1[1], n), s2 + (n,)],
        (0,),
        where, got, f1_local, f2_local, mix, om[2], w2_map,
    )
    parts = exchange(parts, "gy")
    (known1,) = call(
        part(known_one_kernel, s1, grids[1]),
        [cube1],
        [cube1] * 6,
        (0, 1),
        where, e, f1, own1, power[1], link[1],
        flops=10000000000,
    )
    parts = exchange(jnp.broadcast_to(parts[None], (gx,) + parts.shape), "gx")
    parts, known1 = lax.optimization_barrier((parts, known1))
    parts = parts.reshape((gx * gy,) + parts.shape[2:])

    cubes = [g + (n,) for g in grids]
    lines = [g[0] * g[1] for g in grids]
    margin = s2[0]
    region = (3 * s2[0], 3 * s2[1], n)
    padded = (grids[2][0] + 2 * margin, grids[2][1] + 2 * margin, n)
    f3, f4_local, copies = call(
        part(gathered_down_kernel, gx, gy),
        [cubes[3], cubes[4], (gz, 8, lines[3] + lines[4] + late_lanes)],
        [cubes[2], (lines[2], n), (8, lines[2])]
        + [cubes[2]] * 4
        + [(grids[3][0], grids[2][1], n)]
        + [cubes[3]] * 4
        + [(grids[4][0], grids[3][1], n)],
        (),
        parts, late, power[2], link[2], power[3], ends[3], ends[4],
    )
    got34 = stacked(copies)
    parts, f3 = lax.optimization_barrier((parts, f3))
    (known2,) = call(
        part(known_two_kernel, gx, gy, grids[2]),
        [region],
        [(region[0] * region[1], n), (8, region[0] * region[1])] + [region] * 6,
        (0, 1),
        where, e, parts, power[2], link[2],
        flops=500000000,
    )
    (known3_local,) = call(
        part(local_known_kernel, 3),
        [cubes[3]],
        [cubes[3]] * 6,
        (0,),
        e, f3, power[3],
        flops=500000000,
    )
    got34, known2, known3_local = lax.optimization_barrier((got34, known2, known3_local))

    copies, c1_local = call(
        part(local_up_kernel, s0, grids, margin),
        [(gz, 8, sum(UP_LANES)), cube1],
        [cubes[3]] * 3 + [(grids[4][0], grids[3][1], n)] + [cubes[4]] * 2 + [cubes[3]] + [cubes[4]] * 3 + [cubes[3]] * 5 + [cubes[2], padded] + [region] * 5 + [cube1] * 4,
        (0, 1),
        where, e, f4_local, got34, om[4], w4_map, up_mix, power[4], link[4], known3_local, known2, known1,
        power[3], power[2], power[1], ends[3], ends[2], ends[1], ends_up,
    )
    got_up = stacked(copies)
    got, c1_local = lax.optimization_barrier((got, c1_local))
    known0, twice0 = call(
        part(known_zero_kernel, s0, ext0, lines[3] + lines[4], grids[0]),
        [s0 + (n,), s0 + (n,)],
        [ext0 + (n,)] + [inner0] * 8,
        (0, 1),
        where, e, f0, got, got34, mix, power[0], link[0],
        flops=500000000,
    )
    got_up, known0, twice0 = lax.optimization_barrier((got_up, known0, twice0))
    u, r = call(
        part(finish_kernel, s0, grids, margin),
        [s0 + (n,), s0 + (n,)],
        [cubes[3]] * 3 + [cubes[2], padded] + [region] * 4 + [cube1] * 5 + [inner0] * 7,
        (0, 1),
        where, e, got_up, c1_local, known0, twice0, up_mix, basis_up,
        power[0], link[0], m_matrix, m_link,
    )
    return u, r


def solution(mesh):
    return jax.shard_map(
        body,
        mesh=mesh,
        in_specs=(P("gx", "gy", "gz"), P("gz"), P(), P(None, "gz", None)),
        out_specs=(P("gx", "gy", "gz"), P("gx", "gy", "gz")),
        check_vma=False,
    )
```
